32 devices in a mesh: data: 1 (over z), dap: 32 (over y, x, core).
Axes of the slice: x: 4, y: 4, z: 1, core: 2. Of those that a mesh axis runs over, the one named last changes fastest.
The devices are a block of a 4x4x8 slice.
Arguments:
- msa_act: bfloat16 [4096, 128, 64], P(('data', 'dap'))
- pair_act: bfloat16 [128, 128, 128], P(('data', 'dap'))
- msa_mask: int32 [4096, 128], P('data')
- res_mask: int32 [128], P('data')
- row_bias_w: bfloat16 [128, 8], replicated
- row_qkvg_w: bfloat16 [64, 4, 8, 8], replicated
- row_out_w: bfloat16 [8, 8, 64], replicated
- col_query_w: bfloat16 [64, 8, 8], replicated
- col_kv_w: bfloat16 [64, 2, 8], replicated
- col_gate_w: bfloat16 [64, 8, 8], replicated
- col_out_w: bfloat16 [8, 8, 64], replicated
- opm_proj_w: bfloat16 [64, 2, 32], replicated
- opm_out_w: bfloat16 [32, 32, 128], replicated
- start_bias_w: bfloat16 [128, 4], replicated
- start_qkvg_w: bfloat16 [128, 4, 4, 32], replicated
- start_out_w: bfloat16 [4, 32, 128], replicated
- end_bias_w: bfloat16 [128, 4], replicated
- end_qkvg_w: bfloat16 [128, 4, 4, 32], replicated
- end_out_w: bfloat16 [4, 32, 128], replicated
Outputs:
- output 1: bfloat16 [4096, 128, 64], P(('data', 'dap'))
- output 2: bfloat16 [128, 128, 128], P(('data', 'dap'))
All inputs are finite; a program needn't handle non-finite values.
Results may differ from the reference program's by a relative error of at most 0.0149318.
Values are sent between devices in bfloat16 or wider.
A program may use at most 768 MiB of HBM per device.

```python
import jax
import jax.numpy as jnp
from jax import lax

NUM_SEQ = 4096
NUM_RES = 128
MSA_DIM = 64
PAIR_DIM = 128
MSA_HEADS = 8
MSA_HEAD_DIM = 8
TRI_HEADS = 4
TRI_HEAD_DIM = 32
OPM_DIM = 32


def draw_weight(rng_key, arr_shape, fan_in, gain_val):
    return (jax.random.normal(rng_key, arr_shape, jnp.float32) * (gain_val * fan_in ** -0.5)).astype(jnp.bfloat16)


def setup_inputs(seed: int = 0, part: int = 0) -> dict:
    part_key = jax.random.fold_in(jax.random.key(seed), part)
    part_keys = jax.random.split(part_key, 6)
    common = jax.random.normal(part_keys[0], (NUM_RES, MSA_DIM), jnp.float32)
    seq_noise = jax.random.normal(part_keys[1], (NUM_SEQ, NUM_RES, MSA_DIM), jnp.float32)
    msa_act = (0.8 * common[None] + 0.6 * seq_noise).astype(jnp.bfloat16)
    pair_act = jax.random.normal(part_keys[2], (NUM_RES, NUM_RES, PAIR_DIM), jnp.float32).astype(jnp.bfloat16)
    msa_mask = (jax.random.randint(part_keys[3], (NUM_SEQ, NUM_RES), 0, 5) != 0).astype(jnp.int32)
    res_mask = (jax.random.randint(part_keys[4], (NUM_RES,), 0, 4) != 0).astype(jnp.int32)
    weight_keys = jax.random.split(jax.random.key(seed + 1), 15)
    msa_width = MSA_HEADS * MSA_HEAD_DIM
    tri_width = TRI_HEADS * TRI_HEAD_DIM
    return {
        'msa_act': msa_act,
        'pair_act': pair_act,
        'msa_mask': msa_mask,
        'res_mask': res_mask,
        'row_bias_w': draw_weight(weight_keys[0], (PAIR_DIM, MSA_HEADS), PAIR_DIM, 1.5),
        'row_qkvg_w': draw_weight(weight_keys[1], (MSA_DIM, 4, MSA_HEADS, MSA_HEAD_DIM), MSA_DIM, 1.25),
        'row_out_w': draw_weight(weight_keys[2], (MSA_HEADS, MSA_HEAD_DIM, MSA_DIM), msa_width, 1.0),
        'col_query_w': draw_weight(weight_keys[3], (MSA_DIM, MSA_HEADS, MSA_HEAD_DIM), MSA_DIM, 2.0),
        'col_kv_w': draw_weight(weight_keys[4], (MSA_DIM, 2, MSA_HEAD_DIM), MSA_DIM, 1.25),
        'col_gate_w': draw_weight(weight_keys[5], (MSA_DIM, MSA_HEADS, MSA_HEAD_DIM), MSA_DIM, 1.0),
        'col_out_w': draw_weight(weight_keys[6], (MSA_HEADS, MSA_HEAD_DIM, MSA_DIM), msa_width, 1.0),
        'opm_proj_w': draw_weight(weight_keys[7], (MSA_DIM, 2, OPM_DIM), MSA_DIM, 1.0),
        'opm_out_w': draw_weight(weight_keys[8], (OPM_DIM, OPM_DIM, PAIR_DIM), OPM_DIM * OPM_DIM, 0.5),
        'start_bias_w': draw_weight(weight_keys[9], (PAIR_DIM, TRI_HEADS), PAIR_DIM, 1.5),
        'start_qkvg_w': draw_weight(weight_keys[10], (PAIR_DIM, 4, TRI_HEADS, TRI_HEAD_DIM), PAIR_DIM, 1.25),
        'start_out_w': draw_weight(weight_keys[11], (TRI_HEADS, TRI_HEAD_DIM, PAIR_DIM), tri_width, 1.0),
        'end_bias_w': draw_weight(weight_keys[12], (PAIR_DIM, TRI_HEADS), PAIR_DIM, 1.5),
        'end_qkvg_w': draw_weight(weight_keys[13], (PAIR_DIM, 4, TRI_HEADS, TRI_HEAD_DIM), PAIR_DIM, 1.25),
        'end_out_w': draw_weight(weight_keys[14], (TRI_HEADS, TRI_HEAD_DIM, PAIR_DIM), tri_width, 1.0),
    }


def layer_norm(values):
    widened = values.astype(jnp.float32)
    mean_val = jnp.mean(widened, axis=-1, keepdims=True)
    centered = widened - mean_val
    variance = jnp.mean(centered * centered, axis=-1, keepdims=True)
    return (centered * lax.rsqrt(variance + 1e-5)).astype(jnp.bfloat16)


def project(einsum_form, activations, weight):
    return jnp.einsum(einsum_form, activations.astype(jnp.float32), weight.astype(jnp.float32)).astype(jnp.bfloat16)


def mask_bias(mask_vals):
    return (mask_vals.astype(jnp.float32) - 1.0) * 1e4


def gated_out(einsum_form, gate_proj, attended, out_w):
    gated_vals = (jax.nn.sigmoid(gate_proj.astype(jnp.float32)) * attended).astype(jnp.bfloat16)
    return jnp.einsum(einsum_form, gated_vals.astype(jnp.float32), out_w.astype(jnp.float32))


def row_attention(msa_act, pair_act, msa_mask, row_bias_w, row_qkvg_w, row_out_w):
    pair_bias = project('ijc,ch->hij', layer_norm(pair_act), row_bias_w).astype(jnp.float32)
    logit_scale = MSA_HEAD_DIM ** -0.5

    def one_seq(seq_inputs):
        seq_ln, seq_mask = seq_inputs
        projected = project('ic,cahd->aihd', seq_ln, row_qkvg_w)
        logits = jnp.einsum('ihd,jhd->hij', projected[0].astype(jnp.float32), projected[1].astype(jnp.float32)) * logit_scale + pair_bias + mask_bias(seq_mask)[None, None, :]
        attn_probs = jax.nn.softmax(logits, axis=-1).astype(jnp.bfloat16)
        attended = jnp.einsum('hij,jhd->ihd', attn_probs.astype(jnp.float32), projected[2].astype(jnp.float32))
        return gated_out('ihd,hdc->ic', projected[3], attended, row_out_w)

    updates = lax.map(one_seq, (layer_norm(msa_act), msa_mask))
    return (msa_act.astype(jnp.float32) + updates).astype(jnp.bfloat16)


def column_attention(msa_act, msa_mask, col_query_w, col_kv_w, col_gate_w, col_out_w):
    msa_ln = layer_norm(msa_act)
    mask_f = msa_mask.astype(jnp.float32)
    mask_count = jnp.sum(mask_f, axis=0) + 1e-10
    mean_query = (jnp.einsum('sr,src->rc', mask_f, msa_ln.astype(jnp.float32)) / mask_count[:, None]).astype(jnp.bfloat16)
    query_proj = project('rc,chd->rhd', mean_query, col_query_w)
    key_val = project('src,cad->asrd', msa_ln, col_kv_w)
    gate_proj = project('src,chd->srhd', msa_ln, col_gate_w)
    logits = jnp.einsum('rhd,srd->rhs', query_proj.astype(jnp.float32), key_val[0].astype(jnp.float32)) * (MSA_HEAD_DIM ** -0.5) + mask_bias(msa_mask).T[:, None, :]
    attn_probs = jax.nn.softmax(logits, axis=-1).astype(jnp.bfloat16)
    attended = jnp.einsum('rhs,srd->rhd', attn_probs.astype(jnp.float32), key_val[1].astype(jnp.float32))
    update = gated_out('srhd,hdc->src', gate_proj, attended[None], col_out_w)
    return (msa_act.astype(jnp.float32) + update).astype(jnp.bfloat16)


def outer_product_mean(msa_act, pair_act, msa_mask, opm_proj_w, opm_out_w):
    mask_f = msa_mask.astype(jnp.float32)
    projected = project('src,cae->asre', layer_norm(msa_act), opm_proj_w) * msa_mask.astype(jnp.bfloat16)[None, :, :, None]
    counts = jnp.einsum('si,sj->ij', mask_f, mask_f)
    right_proj = projected[1].astype(jnp.float32)
    out_f = opm_out_w.astype(jnp.float32)

    def one_row(row_inputs):
        left_row, count_row = row_inputs
        outer_sum = jnp.einsum('se,sjf->jef', left_row.astype(jnp.float32), right_proj).astype(jnp.bfloat16)
        return jnp.einsum('jef,efc->jc', outer_sum.astype(jnp.float32), out_f) / (1e-3 + count_row)[:, None]

    updates = lax.map(one_row, (jnp.swapaxes(projected[0], 0, 1), counts))
    return (pair_act.astype(jnp.float32) + updates).astype(jnp.bfloat16)


def triangle_start(pair_act, res_mask, bias_w, qkvg_w, out_w):
    pair_ln = layer_norm(pair_act)
    tri_bias = project('jkc,ch->hjk', pair_ln, bias_w).astype(jnp.float32)
    key_bias = mask_bias(res_mask)[None, None, :]
    logit_scale = TRI_HEAD_DIM ** -0.5

    def one_row(row_ln):
        projected = project('jc,cahd->ajhd', row_ln, qkvg_w)
        logits = jnp.einsum('jhd,khd->hjk', projected[0].astype(jnp.float32), projected[1].astype(jnp.float32)) * logit_scale + tri_bias + key_bias
        attn_probs = jax.nn.softmax(logits, axis=-1).astype(jnp.bfloat16)
        attended = jnp.einsum('hjk,khd->jhd', attn_probs.astype(jnp.float32), projected[2].astype(jnp.float32))
        return gated_out('jhd,hdc->jc', projected[3], attended, out_w)

    updates = lax.map(one_row, pair_ln)
    return (pair_act.astype(jnp.float32) + updates).astype(jnp.bfloat16)


def reference(msa_act, pair_act, msa_mask, res_mask, row_bias_w, row_qkvg_w, row_out_w, col_query_w, col_kv_w, col_gate_w, col_out_w, opm_proj_w, opm_out_w, start_bias_w, start_qkvg_w, start_out_w, end_bias_w, end_qkvg_w, end_out_w):
    msa_act = row_attention(msa_act, pair_act, msa_mask, row_bias_w, row_qkvg_w, row_out_w)
    msa_act = column_attention(msa_act, msa_mask, col_query_w, col_kv_w, col_gate_w, col_out_w)
    pair_act = outer_product_mean(msa_act, pair_act, msa_mask, opm_proj_w, opm_out_w)
    pair_act = triangle_start(pair_act, res_mask, start_bias_w, start_qkvg_w, start_out_w)
    pair_act = jnp.swapaxes(triangle_start(jnp.swapaxes(pair_act, 0, 1), res_mask, end_bias_w, end_qkvg_w, end_out_w), 0, 1)
    return (msa_act, pair_act)
```

```python
import functools
import math

import jax
import jax.numpy as jnp
from jax import lax
from jax.experimental import pallas as pl
from jax.experimental.pallas import tpu as pltpu
from jax.sharding import PartitionSpec as P

MESH = pl.DeviceIdType.MESH
F32 = jnp.float32
BF16 = jnp.bfloat16


def layer_norm(values):
    widened = values.astype(F32)
    mean_val = jnp.mean(widened, axis=-1, keepdims=True)
    centered = widened - mean_val
    variance = jnp.mean(centered * centered, axis=-1, keepdims=True)
    return (centered * lax.rsqrt(variance + 1e-5)).astype(BF16)


def mask_bias(mask_vals):
    return (mask_vals.astype(F32) - 1.0) * 1e4


def matmul_bf(einsum_form, left_arr, right_arr):
    return jnp.einsum(einsum_form, left_arr, right_arr, preferred_element_type=F32).astype(BF16)


def gated_out(einsum_form, gate_proj, attended, out_w):
    gated_vals = (jax.nn.sigmoid(gate_proj.astype(F32)) * attended).astype(BF16)
    return jnp.einsum(einsum_form, gated_vals, out_w, preferred_element_type=F32)


def row_attention(msa, bias_full, seq_mask, qkvg_w, out_w):
    projected = matmul_bf('sic,cahd->asihd', layer_norm(msa), qkvg_w)
    logits = jnp.einsum('sihd,sjhd->shij', projected[0], projected[1], preferred_element_type=F32) * (qkvg_w.shape[-1] ** -0.5) + bias_full[None] + mask_bias(seq_mask)[:, None, None, :]
    attn_probs = jax.nn.softmax(logits, axis=-1).astype(BF16)
    attended = jnp.einsum('shij,sjhd->sihd', attn_probs, projected[2], preferred_element_type=F32)
    return (msa + gated_out('sihd,hdc->sic', projected[3], attended, out_w)).astype(BF16)


def triangle_rows(pair_act, pair_ln, bias_full, res_mask, qkvg_w, out_w):
    projected = matmul_bf('ijc,cahd->aijhd', pair_ln, qkvg_w)
    logits = jnp.einsum('ijhd,ikhd->ihjk', projected[0], projected[1], preferred_element_type=F32) * (qkvg_w.shape[-1] ** -0.5) + bias_full[None] + mask_bias(res_mask)[None, None, None, :]
    attn_probs = jax.nn.softmax(logits, axis=-1).astype(BF16)
    attended = jnp.einsum('ihjk,ikhd->ijhd', attn_probs, projected[2], preferred_element_type=F32)
    return (pair_act + gated_out('ijhd,hdc->ijc', projected[3], attended, out_w)).astype(BF16)


def remote(src, dst, send_sem, recv_sem, dev):
    return pltpu.make_async_remote_copy(src_ref=src, dst_ref=dst, send_sem=send_sem, recv_sem=recv_sem,
                                        device_id={'dap': dev}, device_id_type=MESH)


def greet_all(me, n):
    barrier = pltpu.get_barrier_semaphore()
    for k in range(1, n):
        pl.semaphore_signal(barrier, inc=1, device_id={'dap': lax.rem(me + k, n)}, device_id_type=MESH)
    pl.semaphore_wait(barrier, n - 1)


def vmem():
    return pl.BlockSpec(memory_space=pltpu.VMEM)


def params(cid, limit=None):
    return pltpu.CompilerParams(collective_id=cid, has_side_effects=True, vmem_limit_bytes=limit)


def position(me, side):
    return me // (2 * side), (me // 2) % side, me % 2


def rows_to_block(me, side, rows_ref, block_ref, send_sem, recv_sem):
    y, x, c = position(me, side)
    half = side // 2
    slot = (x % half) * 2 + c
    core = x // half
    for t in range(side):
        dst = y * 2 * side + t * 2 + core

        @pl.when(dst != me)
        def _():
            remote(rows_ref.at[:, t], block_ref.at[slot], send_sem.at[t], recv_sem.at[slot], dst).start()

        @pl.when(dst == me)
        def _():
            block_ref[slot] = rows_ref[:, t]


def rows_to_block_wait(me, side, rows_ref, block_ref, send_sem, recv_sem):
    y, x, c = position(me, side)
    half = side // 2
    core = x // half
    for t in range(side):
        dst = y * 2 * side + t * 2 + core
        src = y * 2 * side + (c * half + t // 2) * 2 + t % 2

        @pl.when(dst != me)
        def _():
            remote(rows_ref.at[:, t], block_ref.at[t], send_sem.at[t], recv_sem.at[t], dst).wait_send()

        @pl.when(src != me)
        def _():
            remote(rows_ref.at[:, 0], block_ref.at[t], send_sem.at[t], recv_sem.at[t], dst).wait_recv()


def entry_kernel(n, side, bias_ref, rows_ref, bias_out, block_out, send_sem, recv_sem, bsend, brecv):
    me = lax.axis_index('dap')
    greet_all(me, n)
    copies = []
    for k in range(1, n):
        cp = remote(bias_ref, bias_out.at[me], send_sem.at[k], recv_sem.at[k], lax.rem(me + k, n))
        cp.start()
        copies.append(cp)
    rows_to_block(me, side, rows_ref, block_out, bsend, brecv)
    bias_out[me] = bias_ref[...]
    rows_to_block_wait(me, side, rows_ref, block_out, bsend, brecv)
    for cp in copies:
        cp.wait()


def entry_exchange(n, side, bias, rows):
    r, sides, w, ch = rows.shape
    return pl.pallas_call(
        functools.partial(entry_kernel, n, side),
        out_shape=[jax.ShapeDtypeStruct((n,) + bias.shape, bias.dtype),
                   jax.ShapeDtypeStruct((side, r, w, ch), rows.dtype)],
        in_specs=[vmem(), vmem()], out_specs=[vmem(), vmem()],
        scratch_shapes=[pltpu.SemaphoreType.DMA((n,)), pltpu.SemaphoreType.DMA((n,)),
                        pltpu.SemaphoreType.DMA((side,)), pltpu.SemaphoreType.DMA((side,))],
        compiler_params=params(0), name='entry_exchange')(bias, rows)


def reduce_kernel(n, combine, part_ref, out_ref, got, mine, send_sem, recv_sem, send2, recv2):
    me = lax.axis_index('dap')
    greet_all(me, n)
    copies = []
    for k in range(1, n):
        dst = lax.rem(me + k, n)
        cp = remote(part_ref.at[dst], got.at[me], send_sem.at[k], recv_sem.at[k], dst)
        cp.start()
        copies.append(cp)
    got[me] = part_ref[me]
    for cp in copies:
        cp.wait()
    total = combine(got[...])
    mine[...] = total
    out_ref[me] = total
    copies = []
    for k in range(1, n):
        cp = remote(mine, out_ref.at[me], send2.at[k], recv2.at[k], lax.rem(me + k, n))
        cp.start()
        copies.append(cp)
    for cp in copies:
        cp.wait()


def all_reduce(n, cid, combine, part, out_block):
    return pl.pallas_call(
        functools.partial(reduce_kernel, n, combine),
        out_shape=jax.ShapeDtypeStruct((n,) + out_block, F32),
        in_specs=[vmem()], out_specs=vmem(),
        scratch_shapes=[pltpu.VMEM(part.shape, F32), pltpu.VMEM(out_block, F32)]
        + [pltpu.SemaphoreType.DMA((n,))] * 4,
        compiler_params=params(cid), name=f'all_reduce{cid}')(part)


def combine_sum(got):
    return jnp.sum(got, axis=0)


def combine_softmax(got):
    acc, top, den = got[:, 0], got[:, 1], got[:, 2]
    scale = jnp.exp(top - jnp.max(top, axis=0, keepdims=True))
    return jnp.sum(acc * scale, axis=0) / jnp.sum(den * scale, axis=0)


def opm_kernel(side, a_ref, c_ref, o_ref, a_buf, c_buf, acc, got, s1, r1, s2, r2, s3, r3):
    me = lax.axis_index('dap')
    y, x, c = position(me, side)
    seq = a_ref.shape[-1]
    half = side // 2
    blk = a_ref.shape[1]

    def dev(yy, xx, cc):
        return (yy * side + xx) * 2 + cc

    barrier = pltpu.get_barrier_semaphore()
    peers = [dev(y, x, 1 - c)]
    for k in range(1, side):
        peers.append(dev(lax.rem(y + k, side), x, c))
        peers.append(dev(y, lax.rem(x + k, side), c))
    for p in peers:
        pl.semaphore_signal(barrier, inc=1, device_id={'dap': p}, device_id_type=MESH)
    pl.semaphore_wait(barrier, len(peers))

    def slot(buf, yy, xx):
        return buf.at[yy, xx // 2, :, pl.ds(pl.multiple_of((xx % 2) * seq, seq), seq)]

    first = []
    for k in range(1, side):
        ty = lax.rem(y + k, side)
        cp = remote(a_ref.at[ty], slot(a_buf, y, x), s1.at[0, k], r1.at[0, k], dev(ty, x, c))
        cp.start()
        tx = lax.rem(x + k, side)
        cq = remote(c_ref.at[tx], slot(c_buf, y, x), s1.at[1, k], r1.at[1, k], dev(y, tx, c))
        cq.start()
        first.append((cp, cq))
    second = []
    for k in range(1, side):
        cp = remote(a_ref.at[y], slot(a_buf, y, x), s2.at[0, 0, k], r2.at[0, 0, k], dev(y, lax.rem(x + k, side), c))
        cp.start()
        cq = remote(c_ref.at[x], slot(c_buf, y, x), s2.at[1, 0, k], r2.at[1, 0, k], dev(lax.rem(y + k, side), x, c))
        cq.start()
        second += [cp, cq]
    lanes = pl.ds(pl.multiple_of((x % 2) * seq, seq), seq)
    a_buf[y, x // 2, :, lanes] = a_ref[y]
    c_buf[y, x // 2, :, lanes] = c_ref[x]
    order = [1, side - 1] + list(range(2, side - 1))
    for k in order:
        cp, cq = first[k - 1]
        cp.wait_recv()
        sy = lax.rem(y - k + side, side)
        for q in range(1, side):
            f = remote(slot(a_buf, sy, x), slot(a_buf, sy, x), s2.at[0, k, q], r2.at[0, k, q], dev(y, lax.rem(x + q, side), c))
            f.start()
            second.append(f)
        cq.wait_recv()
        sx = lax.rem(x - k + side, side)
        for q in range(1, side):
            f = remote(slot(c_buf, y, sx), slot(c_buf, y, sx), s2.at[1, k, q], r2.at[1, k, q], dev(lax.rem(y + q, side), x, c))
            f.start()
            second.append(f)
    for cp, cq in first:
        cp.wait_send()
        cq.wait_send()
    for f in second:
        f.wait()
    rows = blk // 2

    def product(base, dst):
        def tile(t, _):
            r0 = pl.multiple_of(base + t * 128, 128)
            total = jnp.zeros((128, blk), F32)
            for yy in range(side):
                for xx in range(half):
                    total += lax.dot_general(a_buf[yy, xx, pl.ds(r0, 128), :], c_buf[yy, xx], (((1,), (1,)), ((), ())),
                                             preferred_element_type=F32)
            dst[pl.ds(pl.multiple_of(t * 128, 128), 128), :] = total
            return 0
        lax.fori_loop(0, rows // 128, tile, 0)

    product((1 - c) * rows, acc.at[0])
    swap = remote(acc.at[0], got, s3, r3, dev(y, x, 1 - c))
    swap.start()
    product(c * rows, acc.at[1])
    swap.wait()
    o_ref[...] = (acc[1] + got[...]).astype(BF16)


def opm_exchange(side, a, c):
    blk, seq = a.shape[1:]
    buf = pltpu.VMEM((side, side // 2, blk, 2 * seq), BF16)
    dma = pltpu.SemaphoreType.DMA
    return pl.pallas_call(
        functools.partial(opm_kernel, side),
        out_shape=jax.ShapeDtypeStruct((blk // 2, blk), BF16),
        in_specs=[vmem(), vmem()], out_specs=vmem(),
        scratch_shapes=[buf, buf, pltpu.VMEM((2, blk // 2, blk), F32), pltpu.VMEM((blk // 2, blk), F32),
                        dma((2, side)), dma((2, side)), dma((2, side, side)), dma((2, side, side)), dma, dma],
        compiler_params=params(3, 60 * 1024 * 1024), name='opm_exchange')(a, c)


def block_to_rows_kernel(side, block_ref, rows_out, send_sem, recv_sem):
    me = lax.axis_index('dap')
    y, x, c = position(me, side)
    half = side // 2
    core = x // half
    my_slot = (x % half) * 2 + c
    barrier = pltpu.get_barrier_semaphore()
    for t in range(2 * side):
        peer = y * 2 * side + t

        @pl.when(peer != me)
        def _():
            pl.semaphore_signal(barrier, inc=1, device_id={'dap': peer}, device_id_type=MESH)
    pl.semaphore_wait(barrier, 2 * side - 1)
    for t in range(side):
        dst = y * 2 * side + (c * half + t // 2) * 2 + t % 2

        @pl.when(dst != me)
        def _():
            remote(block_ref.at[t], rows_out.at[x], send_sem.at[t], recv_sem.at[x], dst).start()

        @pl.when(dst == me)
        def _():
            rows_out[x] = block_ref[t]
    for t in range(side):
        dst = y * 2 * side + (c * half + t // 2) * 2 + t % 2
        src = y * 2 * side + t * 2 + core

        @pl.when(dst != me)
        def _():
            remote(block_ref.at[t], rows_out.at[x], send_sem.at[t], recv_sem.at[x], dst).wait_send()

        @pl.when(src != me)
        def _():
            remote(block_ref.at[t], rows_out.at[t], send_sem.at[t], recv_sem.at[t], dst).wait_recv()


def block_to_rows(side, block):
    slots, r, w, ch = block.shape
    return pl.pallas_call(
        functools.partial(block_to_rows_kernel, side),
        out_shape=jax.ShapeDtypeStruct((side, r, w, ch), block.dtype),
        in_specs=[vmem()], out_specs=vmem(),
        scratch_shapes=[pltpu.SemaphoreType.DMA((side,)), pltpu.SemaphoreType.DMA((side,))],
        compiler_params=params(4), name='block_to_rows')(block)


def exchange_kernel(n, n_gather, n_swap, *refs):
    k_in = n_gather + n_swap
    ins, outs, (send_sem, recv_sem) = refs[:k_in], refs[k_in:2 * k_in], refs[2 * k_in:]
    me = lax.axis_index('dap')
    greet_all(me, n)
    copies = []
    for k in range(1, n):
        dst = lax.rem(me + k, n)
        for a in range(k_in):
            src = ins[a] if a < n_gather else ins[a].at[dst]
            cp = remote(src, outs[a].at[me], send_sem.at[a, k], recv_sem.at[a, k], dst)
            cp.start()
            copies.append(cp)
    for a in range(k_in):
        outs[a][me] = ins[a][...] if a < n_gather else ins[a][me]
    for cp in copies:
        cp.wait()


def exchange(n, cid, gathers, swaps):
    ops = list(gathers) + list(swaps)
    shapes = [jax.ShapeDtypeStruct((n,) + g.shape, g.dtype) for g in gathers] + [jax.ShapeDtypeStruct(s.shape, s.dtype) for s in swaps]
    return pl.pallas_call(
        functools.partial(exchange_kernel, n, len(gathers), len(swaps)),
        out_shape=shapes, in_specs=[vmem()] * len(ops), out_specs=[vmem()] * len(ops),
        scratch_shapes=[pltpu.SemaphoreType.DMA((len(ops), n))] * 2,
        compiler_params=params(cid), name=f'exchange{cid}')(*ops)


def solution(mesh):
    n = mesh.shape['dap']
    side = math.isqrt(n // 2)
    assert 2 * side * side == n

    def block(msa, pair, mask_full, res_mask, row_bias_w, row_qkvg_w, row_out_w, col_query_w, col_kv_w, col_gate_w, col_out_w, opm_proj_w, opm_out_w, start_bias_w, start_qkvg_w, start_out_w, end_bias_w, end_qkvg_w, end_out_w):
        seq, res, ch = msa.shape
        r = pair.shape[0]
        pc = pair.shape[-1]
        w = res // side
        heads, hd = col_gate_w.shape[1:]
        dev_index = lax.axis_index('dap')
        y, x, core = position(dev_index, side)
        seq_mask = lax.dynamic_slice_in_dim(mask_full, dev_index * seq, seq, axis=0)

        row_bias = matmul_bf('ijc,ch->hij', layer_norm(pair), row_bias_w)
        bias_all, pair_blk = entry_exchange(n, side, row_bias, pair.reshape(r, side, w, pc))
        bias_full = bias_all.transpose(1, 0, 2, 3).reshape(row_bias.shape[0], res, res)
        msa = row_attention(msa, bias_full, seq_mask, row_qkvg_w, row_out_w)

        msa_ln = layer_norm(msa)
        part = jnp.einsum('sr,src->rc', seq_mask.astype(BF16), msa_ln, preferred_element_type=F32)
        qsum = all_reduce(n, 1, combine_sum, part.reshape(n, r, ch), (r, ch)).reshape(res, ch)
        mask_count = jnp.sum(mask_full, axis=0).astype(F32) + 1e-10
        query = matmul_bf('rc,chd->rhd', (qsum / mask_count[:, None]).astype(BF16), col_query_w)
        key_val = matmul_bf('src,cad->asrd', msa_ln, col_kv_w)
        gate = matmul_bf('src,chd->srhd', msa_ln, col_gate_w)
        logits = jnp.einsum('rhd,srd->rhs', query, key_val[0], preferred_element_type=F32) * (hd ** -0.5) + mask_bias(seq_mask).T[:, None, :]
        top = jnp.max(logits, axis=-1, keepdims=True)
        weights = jnp.exp(logits - top)
        den = jnp.sum(weights, axis=-1, keepdims=True)
        acc = jnp.einsum('rhs,srd->rhd', weights.astype(BF16), key_val[1], preferred_element_type=F32)
        part = jnp.stack([acc, jnp.broadcast_to(top, acc.shape), jnp.broadcast_to(den, acc.shape)], axis=0)
        part = part.reshape(3, n, r, heads * hd).transpose(1, 0, 2, 3)
        attended = all_reduce(n, 2, combine_softmax, part, (r, heads * hd)).reshape(res, heads, hd)
        msa = (msa + gated_out('srhd,hdc->src', gate, attended[None], col_out_w)).astype(BF16)

        msa_ln = layer_norm(msa)
        proj = matmul_bf('src,cae->ares', msa_ln, opm_proj_w) * seq_mask.astype(BF16).T[None, :, None, :]
        e = opm_proj_w.shape[-1]
        outer = opm_exchange(side, proj[0].reshape(side, w * e, seq), proj[1].reshape(side, w * e, seq))
        rows0 = y * w + core * (w // 2)
        mask_bf = mask_full.astype(BF16)
        mask_i = lax.dynamic_slice_in_dim(mask_bf, rows0, w // 2, axis=1)
        mask_j = lax.dynamic_slice_in_dim(mask_bf, x * w, w, axis=1)
        counts = jnp.einsum('si,sj->ij', mask_i, mask_j, preferred_element_type=F32)
        update = jnp.einsum('iejf,efc->ijc', outer.reshape(w // 2, e, w, e), opm_out_w, preferred_element_type=F32) / (1e-3 + counts)[:, :, None]
        pair_blk = (pair_blk.reshape(w // 2, w, pc) + update).astype(BF16)
        rows = block_to_rows(side, pair_blk.reshape(side, r, w, pc))
        pair = rows.transpose(1, 0, 2, 3).reshape(r, res, pc)

        pair_ln = layer_norm(pair)
        start_all, = exchange(n, 5, [matmul_bf('ijc,ch->hij', pair_ln, start_bias_w)], [])
        start_full = start_all.transpose(1, 0, 2, 3).reshape(-1, res, res)
        pair = triangle_rows(pair, pair_ln, start_full, res_mask, start_qkvg_w, start_out_w)

        end_bias = matmul_bf('ijc,ch->hij', layer_norm(pair), end_bias_w)
        end_all, cols = exchange(n, 6, [end_bias], [pair.reshape(r, n, r, pc).transpose(1, 2, 0, 3)])
        end_full = end_all.transpose(1, 3, 0, 2).reshape(-1, res, res)
        cols = cols.transpose(1, 0, 2, 3).reshape(r, res, pc)
        cols = triangle_rows(cols, layer_norm(cols), end_full, res_mask, end_qkvg_w, end_out_w)
        back, = exchange(n, 7, [], [cols.reshape(r, n, r, pc).transpose(1, 2, 0, 3)])
        pair_out = back.transpose(1, 0, 2, 3).reshape(r, res, pc)
        return msa, pair_out

    row_spec = P(('data', 'dap'), None, None)
    in_specs = (row_spec, row_spec, P('data', None), P('data')) + (P(),) * 15
    return jax.shard_map(block, mesh=mesh, in_specs=in_specs, out_specs=(row_spec, row_spec), check_vma=False)
```

```python
import functools
import math

import jax
import jax.numpy as jnp
from jax import lax
from jax.experimental import pallas as pl
from jax.experimental.pallas import tpu as pltpu
from jax.sharding import PartitionSpec as P

MESH = pl.DeviceIdType.MESH
F32 = jnp.float32
BF16 = jnp.bfloat16


def layer_norm(values):
    widened = values.astype(F32)
    mean_val = jnp.mean(widened, axis=-1, keepdims=True)
    centered = widened - mean_val
    variance = jnp.mean(centered * centered, axis=-1, keepdims=True)
    return (centered * lax.rsqrt(variance + 1e-5)).astype(BF16)


def mask_bias(mask_vals):
    return (mask_vals.astype(F32) - 1.0) * 1e4


def matmul_bf(einsum_form, left_arr, right_arr):
    return jnp.einsum(einsum_form, left_arr, right_arr, preferred_element_type=F32).astype(BF16)


def gated_out(einsum_form, gate_proj, attended, out_w):
    gated_vals = (jax.nn.sigmoid(gate_proj.astype(F32)) * attended).astype(BF16)
    return jnp.einsum(einsum_form, gated_vals, out_w, preferred_element_type=F32)


def triangle_rows(pair_act, pair_ln, bias_full, res_mask, qkvg_w, out_w):
    projected = matmul_bf('ijc,cahd->aijhd', pair_ln, qkvg_w)
    logits = jnp.einsum('ijhd,ikhd->ihjk', projected[0], projected[1], preferred_element_type=F32) * (qkvg_w.shape[-1] ** -0.5) + bias_full[None] + mask_bias(res_mask)[None, None, None, :]
    attn_probs = jax.nn.softmax(logits, axis=-1).astype(BF16)
    attended = jnp.einsum('ihjk,ikhd->ijhd', attn_probs, projected[2], preferred_element_type=F32)
    return (pair_act + gated_out('ijhd,hdc->ijc', projected[3], attended, out_w)).astype(BF16)


LOG2E = 1.4426950408889634

def norm_cols(x):
    mean = jnp.mean(x, axis=0, keepdims=True)
    cen = x - mean
    var = jnp.mean(cen * cen, axis=0, keepdims=True)
    return (cen * lax.rsqrt(var + 1e-5)).astype(BF16)


def row_kernel(heads, hd, m_ref, bias_ref, maskc_ref, maskl_ref, pick_ref, wt_ref, wo_ref, m_out, ln_out, q_out,
               x_buf, q_buf, v_buf, g_buf, k_buf, att_buf):
    @pl.when(pl.program_id(0) == 0)
    def _():
        q_out[...] = jnp.zeros_like(q_out)
    seqs, ch, res = m_ref.shape
    width = heads * hd
    scale = LOG2E * hd ** -0.5
    for s in range(seqs):
        x_buf[:, s * res:(s + 1) * res] = m_ref[s].astype(F32)
    ln = norm_cols(x_buf[...])
    proj = jnp.dot(wt_ref[...], ln, preferred_element_type=F32)
    q_buf[...] = proj[:width].astype(BF16)
    v_buf[...] = proj[2 * width:3 * width].astype(BF16)
    g_buf[...] = proj[3 * width:].astype(BF16)
    for s in range(seqs):
        k_buf[s] = proj[width:2 * width, s * res:(s + 1) * res].T.astype(BF16)

    units = [(s, p) for s in range(seqs) for p in range(heads // 2)]

    def logits_of(u):
        s, p = u
        qt = q_buf[:, s * res:(s + 1) * res]
        return jnp.dot(k_buf[s], jnp.concatenate([qt, qt], axis=1) * pick_ref[p], preferred_element_type=F32)

    def weights_of(u, raw):
        s, p = u
        mcol = jnp.broadcast_to(maskc_ref[0, :, s:s + 1], (res, 2 * res))
        t = raw * scale + bias_ref[p] + mcol
        w = jnp.exp2(t - jnp.max(t, axis=0, keepdims=True))
        return w.astype(BF16), 1.0 / jnp.sum(w, axis=0, keepdims=True)

    def attend(u, w, den):
        s, p = u
        o = jnp.dot(v_buf[2 * p * hd:2 * (p + 1) * hd, s * res:(s + 1) * res], w, preferred_element_type=F32) * den
        lo = 2 * p * hd
        att_buf[lo:lo + hd, s * res:(s + 1) * res] = o[:hd, :res]
        att_buf[lo + hd:lo + 2 * hd, s * res:(s + 1) * res] = o[hd:, res:]

    raws = [logits_of(units[0]), logits_of(units[1])]
    prev = None
    for i, u in enumerate(units):
        if i + 2 < len(units):
            raws.append(logits_of(units[i + 2]))
        cur = weights_of(u, raws.pop(0))
        if prev is not None:
            attend(*prev)
        prev = (u,) + cur
    attend(*prev)
    y = (jax.nn.sigmoid(g_buf[...].astype(F32)) * att_buf[...]).astype(BF16)
    new = (x_buf[...] + jnp.dot(wo_ref[...], y, preferred_element_type=F32)).astype(BF16)
    m_out[0] = new
    ln2 = norm_cols(new.astype(F32))
    ln_out[0] = ln2
    masked = ln2.astype(F32) * maskl_ref[0]
    total = masked[:, :res]
    for s in range(1, seqs):
        total += masked[:, s * res:(s + 1) * res]
    q_out[...] += total


def row_attention(msa, bias_full, seq_mask, qkvg_w, out_w, block=8):
    seq, res, ch = msa.shape
    heads, hd = out_w.shape[:2]
    pairs = heads // 2
    steps = seq // block
    bias = (bias_full.astype(F32) * LOG2E).transpose(0, 2, 1).reshape(pairs, 2, res, res).transpose(0, 2, 1, 3).reshape(pairs, res, 2 * res)
    maskf = seq_mask.astype(F32)
    maskc = ((maskf - 1.0) * (1e4 * LOG2E)).reshape(steps, block, res).transpose(0, 2, 1)
    maskl = maskf.reshape(steps, 1, block * res)
    row_head = jnp.arange(heads * hd) // hd
    lane_head = jnp.arange(2 * res) // res
    pick = (row_head[None, :, None] == (2 * jnp.arange(pairs)[:, None, None] + lane_head[None, None, :])).astype(BF16)
    wt = qkvg_w.reshape(ch, -1).T
    wo = out_w.reshape(heads * hd, ch).T
    full = lambda a: pl.BlockSpec(a.shape, lambda g: (0,) * a.ndim)
    wide = jax.ShapeDtypeStruct((steps, ch, block * res), BF16)
    lanes = block * res
    return pl.pallas_call(
        functools.partial(row_kernel, heads, hd),
        grid=(steps,),
        out_shape=[wide, wide, jax.ShapeDtypeStruct((ch, res), F32)],
        in_specs=[pl.BlockSpec((block, ch, res), lambda g: (g, 0, 0)), full(bias), pl.BlockSpec((1, res, block), lambda g: (g, 0, 0)),
                  pl.BlockSpec((1, 1, lanes), lambda g: (g, 0, 0)), full(pick), full(wt), full(wo)],
        out_specs=[pl.BlockSpec((1, ch, lanes), lambda g: (g, 0, 0))] * 2 + [pl.BlockSpec((ch, res), lambda g: (0, 0))],
        scratch_shapes=[pltpu.VMEM((ch, lanes), F32), pltpu.VMEM((heads * hd, lanes), BF16), pltpu.VMEM((heads * hd, lanes), BF16),
                        pltpu.VMEM((heads * hd, lanes), BF16), pltpu.VMEM((block, res, heads * hd), BF16), pltpu.VMEM((heads * hd, lanes), F32)],
        compiler_params=pltpu.CompilerParams(dimension_semantics=("arbitrary",), vmem_limit_bytes=48 * 1024 * 1024),
        name='row_attention')(msa.transpose(0, 2, 1), bias, maskc, maskl, pick, wt, wo)


def col_sums_kernel(heads, hd, ln_ref, q_ref, maskb_ref, wkv_ref, part_out, logit_buf, val_buf):
    steps, ch, lanes = ln_ref.shape
    res = q_ref.shape[-1]
    block = lanes // res
    scale = hd ** -0.5
    qd = [q_ref[d] for d in range(hd)]

    def first(g, top):
        kv = jnp.dot(wkv_ref[...], ln_ref[g], preferred_element_type=F32).astype(BF16).astype(F32)
        bias = maskb_ref[g]
        for u in range(block):
            k = kv[:hd, u * res:(u + 1) * res]
            logit = qd[0] * k[0:1]
            for d in range(1, hd):
                logit += qd[d] * k[d:d + 1]
            logit = logit * scale + bias[u:u + 1]
            logit_buf[g * block + u] = logit
            val_buf[g * block + u] = kv[hd:, u * res:(u + 1) * res]
            top = jnp.maximum(top, logit)
        return top
    top = lax.fori_loop(0, steps, first, jnp.full((heads, res), -jnp.inf, F32))

    def second(g, carry):
        den, acc = carry
        acc = list(acc)
        for u in range(block):
            s = g * block + u
            w = jnp.exp(logit_buf[s] - top)
            den = den + w
            wb = w.astype(BF16).astype(F32)
            val = val_buf[s]
            for d in range(hd):
                acc[d] = acc[d] + wb * val[d:d + 1]
        return den, tuple(acc)
    zero = jnp.zeros((heads, res), F32)
    den, acc = lax.fori_loop(0, steps, second, (zero, (zero,) * hd))
    for d in range(hd):
        rows = slice(d * heads, (d + 1) * heads)
        part_out[0, rows] = acc[d]
        part_out[1, rows] = top
        part_out[2, rows] = den


def col_sums(ln, query, seq_mask, kv_w, heads, hd):
    steps, ch, lanes = ln.shape
    seq, res = seq_mask.shape
    vm = pl.BlockSpec(memory_space=pltpu.VMEM)
    maskb = ((seq_mask.astype(F32) - 1.0) * 1e4).reshape(steps, seq // steps, res)
    return pl.pallas_call(
        functools.partial(col_sums_kernel, heads, hd),
        out_shape=jax.ShapeDtypeStruct((3, hd * heads, res), F32),
        in_specs=[vm] * 4, out_specs=vm,
        scratch_shapes=[pltpu.VMEM((seq, heads, res), F32), pltpu.VMEM((seq, hd, res), F32)],
        compiler_params=pltpu.CompilerParams(vmem_limit_bytes=48 * 1024 * 1024),
        name='col_sums')(ln, query, maskb, kv_w.reshape(ch, -1).T)


def col_out_kernel(m_ref, ln_ref, att_ref, maskl_ref, wg_ref, wo_ref, wp_ref, m_out, p_out):
    seqs, ch, res = m_out.shape
    att = jnp.concatenate([att_ref[...]] * seqs, axis=1)
    gate = jnp.dot(wg_ref[...], ln_ref[0], preferred_element_type=F32).astype(BF16).astype(F32)
    y = (jax.nn.sigmoid(gate) * att).astype(BF16)
    new = (m_ref[0].astype(F32) + jnp.dot(wo_ref[...], y, preferred_element_type=F32)).astype(BF16)
    newf = new.astype(F32)
    for s in range(seqs):
        m_out[s] = new[:, s * res:(s + 1) * res]
    proj = jnp.dot(wp_ref[...], norm_cols(newf), preferred_element_type=F32).astype(BF16)
    proj = (proj.astype(F32) * maskl_ref[0]).astype(BF16)
    for s in range(seqs):
        p_out[s] = proj[:, s * res:(s + 1) * res]


def col_out(m, ln, att, seq_mask, gate_w, out_w, proj_w):
    steps, ch, lanes = m.shape
    seq, res = seq_mask.shape
    block = seq // steps
    wg, wo = gate_w.transpose(2, 1, 0).reshape(-1, ch), out_w.transpose(2, 1, 0).reshape(ch, -1)
    wp = proj_w.reshape(ch, -1).T
    maskl = seq_mask.astype(F32).reshape(steps, 1, lanes)
    full = lambda a: pl.BlockSpec(a.shape, lambda g: (0,) * a.ndim)
    blk = pl.BlockSpec((1, ch, lanes), lambda g: (g, 0, 0))
    m_new, proj = pl.pallas_call(
        col_out_kernel, grid=(steps,),
        out_shape=[jax.ShapeDtypeStruct((seq, ch, res), BF16), jax.ShapeDtypeStruct((seq, wp.shape[0], res), BF16)],
        in_specs=[blk, blk, full(att), pl.BlockSpec((1, 1, lanes), lambda g: (g, 0, 0)), full(wg), full(wo), full(wp)],
        out_specs=[pl.BlockSpec((block, ch, res), lambda g: (g, 0, 0)), pl.BlockSpec((block, wp.shape[0], res), lambda g: (g, 0, 0))],
        compiler_params=pltpu.CompilerParams(dimension_semantics=("arbitrary",), vmem_limit_bytes=48 * 1024 * 1024),
        name='col_out')(m, ln, att, maskl, wg, wo, wp)
    return m_new.transpose(0, 2, 1), proj


def remote(src, dst, send_sem, recv_sem, dev):
    return pltpu.make_async_remote_copy(src_ref=src, dst_ref=dst, send_sem=send_sem, recv_sem=recv_sem,
                                        device_id={'dap': dev}, device_id_type=MESH)


def greet_all(me, n):
    barrier = pltpu.get_barrier_semaphore()
    for k in range(1, n):
        pl.semaphore_signal(barrier, inc=1, device_id={'dap': lax.rem(me + k, n)}, device_id_type=MESH)
    pl.semaphore_wait(barrier, n - 1)


def vmem():
    return pl.BlockSpec(memory_space=pltpu.VMEM)


def params(cid, limit=None):
    return pltpu.CompilerParams(collective_id=cid, has_side_effects=True, vmem_limit_bytes=limit)


def position(me, side):
    return me // (2 * side), (me // 2) % side, me % 2


def rows_to_block(me, side, rows_ref, block_ref, send_sem, recv_sem):
    y, x, c = position(me, side)
    half = side // 2
    slot = (x % half) * 2 + c
    core = x // half
    for t in range(side):
        dst = y * 2 * side + t * 2 + core

        @pl.when(dst != me)
        def _():
            remote(rows_ref.at[:, t], block_ref.at[slot], send_sem.at[t], recv_sem.at[slot], dst).start()

        @pl.when(dst == me)
        def _():
            block_ref[slot] = rows_ref[:, t]


def rows_to_block_wait(me, side, rows_ref, block_ref, send_sem, recv_sem):
    y, x, c = position(me, side)
    half = side // 2
    core = x // half
    for t in range(side):
        dst = y * 2 * side + t * 2 + core
        src = y * 2 * side + (c * half + t // 2) * 2 + t % 2

        @pl.when(dst != me)
        def _():
            remote(rows_ref.at[:, t], block_ref.at[t], send_sem.at[t], recv_sem.at[t], dst).wait_send()

        @pl.when(src != me)
        def _():
            remote(rows_ref.at[:, 0], block_ref.at[t], send_sem.at[t], recv_sem.at[t], dst).wait_recv()


def entry_kernel(n, side, bias_ref, rows_ref, bias_out, block_out, send_sem, recv_sem, bsend, brecv):
    me = lax.axis_index('dap')
    greet_all(me, n)
    copies = []
    for k in range(1, n):
        cp = remote(bias_ref, bias_out.at[me], send_sem.at[k], recv_sem.at[k], lax.rem(me + k, n))
        cp.start()
        copies.append(cp)
    rows_to_block(me, side, rows_ref, block_out, bsend, brecv)
    bias_out[me] = bias_ref[...]
    rows_to_block_wait(me, side, rows_ref, block_out, bsend, brecv)
    for cp in copies:
        cp.wait()


def entry_exchange(n, side, bias, rows):
    r, sides, w, ch = rows.shape
    return pl.pallas_call(
        functools.partial(entry_kernel, n, side),
        out_shape=[jax.ShapeDtypeStruct((n,) + bias.shape, bias.dtype),
                   jax.ShapeDtypeStruct((side, r, w, ch), rows.dtype)],
        in_specs=[vmem(), vmem()], out_specs=[vmem(), vmem()],
        scratch_shapes=[pltpu.SemaphoreType.DMA((n,)), pltpu.SemaphoreType.DMA((n,)),
                        pltpu.SemaphoreType.DMA((side,)), pltpu.SemaphoreType.DMA((side,))],
        compiler_params=params(0), name='entry_exchange')(bias, rows)


def reduce_kernel(n, combine, finish, n_extra, *refs):
    part_ref, extra, out_ref = refs[0], refs[1:1 + n_extra], refs[1 + n_extra]
    cut, got, mine, back, send_sem, recv_sem, send2, recv2 = refs[2 + n_extra:]
    me = lax.axis_index('dap')
    terms, width, res = part_ref.shape
    own = res // n
    for t in range(terms):
        flat = part_ref[t].T
        for p in range(n):
            cut[p, t] = flat[p * own:(p + 1) * own]
    greet_all(me, n)
    copies = []
    for k in range(1, n):
        dst = lax.rem(me + k, n)
        cp = remote(cut.at[dst], got.at[me], send_sem.at[k], recv_sem.at[k], dst)
        cp.start()
        copies.append(cp)
    got[me] = cut[me]
    for cp in copies:
        cp.wait()
    total = combine(got[...])
    mine[...] = total
    back[me] = total
    copies = []
    for k in range(1, n):
        cp = remote(mine, back.at[me], send2.at[k], recv2.at[k], lax.rem(me + k, n))
        cp.start()
        copies.append(cp)
    for cp in copies:
        cp.wait()
    whole = jnp.concatenate([back[p] for p in range(n)], axis=0)
    finish(whole.T, extra, out_ref)


def all_reduce(n, cid, combine, finish, part, extra, out_shape):
    terms, width, res = part.shape
    own = res // n
    return pl.pallas_call(
        functools.partial(reduce_kernel, n, combine, finish, len(extra)),
        out_shape=jax.ShapeDtypeStruct(out_shape, F32),
        in_specs=[vmem()] * (1 + len(extra)), out_specs=vmem(),
        scratch_shapes=[pltpu.VMEM((n, terms, own, width), F32)] * 2 + [pltpu.VMEM((own, width), F32), pltpu.VMEM((n, own, width), F32)]
        + [pltpu.SemaphoreType.DMA((n,))] * 4,
        compiler_params=params(cid), name=f'all_reduce{cid}')(part, *extra)


def combine_sum(got):
    return jnp.sum(got[:, 0], axis=0)


def combine_softmax(got):
    acc, top, den = got[:, 0], got[:, 1], got[:, 2]
    scale = jnp.exp(top - jnp.max(top, axis=0, keepdims=True))
    return jnp.sum(acc * scale, axis=0) / jnp.sum(den * scale, axis=0)


def finish_query(total, extra, out_ref):
    count_ref, w_ref = extra
    hd, heads, res = out_ref.shape
    mean = (total / count_ref[...]).astype(BF16)
    query = jnp.dot(w_ref[...], mean, preferred_element_type=F32).astype(BF16).astype(F32)
    for d in range(hd):
        out_ref[d] = query[d * heads:(d + 1) * heads]


def finish_plain(total, extra, out_ref):
    out_ref[...] = total


def opm_kernel(side, a_ref, c_ref, o_ref, a_buf, c_buf, acc, got, s1, r1, s2, r2, s3, r3):
    me = lax.axis_index('dap')
    y, x, c = position(me, side)
    seq = a_ref.shape[-1]
    half = side // 2
    blk = a_ref.shape[1]

    def dev(yy, xx, cc):
        return (yy * side + xx) * 2 + cc

    barrier = pltpu.get_barrier_semaphore()
    peers = [dev(y, x, 1 - c)]
    for k in range(1, side):
        peers.append(dev(lax.rem(y + k, side), x, c))
        peers.append(dev(y, lax.rem(x + k, side), c))
    for p in peers:
        pl.semaphore_signal(barrier, inc=1, device_id={'dap': p}, device_id_type=MESH)
    pl.semaphore_wait(barrier, len(peers))

    def slot(buf, yy, xx):
        return buf.at[yy, xx // 2, :, pl.ds(pl.multiple_of((xx % 2) * seq, seq), seq)]

    first = []
    for k in range(1, side):
        ty = lax.rem(y + k, side)
        cp = remote(a_ref.at[ty], slot(a_buf, y, x), s1.at[0, k], r1.at[0, k], dev(ty, x, c))
        cp.start()
        tx = lax.rem(x + k, side)
        cq = remote(c_ref.at[tx], slot(c_buf, y, x), s1.at[1, k], r1.at[1, k], dev(y, tx, c))
        cq.start()
        first.append((cp, cq))
    second = []
    for k in range(1, side):
        cp = remote(a_ref.at[y], slot(a_buf, y, x), s2.at[0, 0, k], r2.at[0, 0, k], dev(y, lax.rem(x + k, side), c))
        cp.start()
        cq = remote(c_ref.at[x], slot(c_buf, y, x), s2.at[1, 0, k], r2.at[1, 0, k], dev(lax.rem(y + k, side), x, c))
        cq.start()
        second += [cp, cq]
    lanes = pl.ds(pl.multiple_of((x % 2) * seq, seq), seq)
    a_buf[y, x // 2, :, lanes] = a_ref[y]
    c_buf[y, x // 2, :, lanes] = c_ref[x]
    order = [1, side - 1] + list(range(2, side - 1))
    for k in order:
        cp, cq = first[k - 1]
        cp.wait_recv()
        sy = lax.rem(y - k + side, side)
        for q in range(1, side):
            f = remote(slot(a_buf, sy, x), slot(a_buf, sy, x), s2.at[0, k, q], r2.at[0, k, q], dev(y, lax.rem(x + q, side), c))
            f.start()
            second.append(f)
        cq.wait_recv()
        sx = lax.rem(x - k + side, side)
        for q in range(1, side):
            f = remote(slot(c_buf, y, sx), slot(c_buf, y, sx), s2.at[1, k, q], r2.at[1, k, q], dev(lax.rem(y + q, side), x, c))
            f.start()
            second.append(f)
    for cp, cq in first:
        cp.wait_send()
        cq.wait_send()
    for f in second:
        f.wait()
    rows = blk // 2

    def product(base, dst):
        def tile(t, _):
            r0 = pl.multiple_of(base + t * 128, 128)
            total = jnp.zeros((128, blk), F32)
            for yy in range(side):
                for xx in range(half):
                    total += lax.dot_general(a_buf[yy, xx, pl.ds(r0, 128), :], c_buf[yy, xx], (((1,), (1,)), ((), ())),
                                             preferred_element_type=F32)
            dst[pl.ds(pl.multiple_of(t * 128, 128), 128), :] = total
            return 0
        lax.fori_loop(0, rows // 128, tile, 0)

    product((1 - c) * rows, acc.at[0])
    swap = remote(acc.at[0], got, s3, r3, dev(y, x, 1 - c))
    swap.start()
    product(c * rows, acc.at[1])
    swap.wait()
    o_ref[...] = (acc[1] + got[...]).astype(BF16)


def opm_exchange(side, a, c):
    blk, seq = a.shape[1:]
    buf = pltpu.VMEM((side, side // 2, blk, 2 * seq), BF16)
    dma = pltpu.SemaphoreType.DMA
    return pl.pallas_call(
        functools.partial(opm_kernel, side),
        out_shape=jax.ShapeDtypeStruct((blk // 2, blk), BF16),
        in_specs=[vmem(), vmem()], out_specs=vmem(),
        scratch_shapes=[buf, buf, pltpu.VMEM((2, blk // 2, blk), F32), pltpu.VMEM((blk // 2, blk), F32),
                        dma((2, side)), dma((2, side)), dma((2, side, side)), dma((2, side, side)), dma, dma],
        compiler_params=params(3, 60 * 1024 * 1024), name='opm_exchange')(a, c)


def block_to_rows_kernel(side, block_ref, rows_out, send_sem, recv_sem):
    me = lax.axis_index('dap')
    y, x, c = position(me, side)
    half = side // 2
    core = x // half
    my_slot = (x % half) * 2 + c
    barrier = pltpu.get_barrier_semaphore()
    for t in range(2 * side):
        peer = y * 2 * side + t

        @pl.when(peer != me)
        def _():
            pl.semaphore_signal(barrier, inc=1, device_id={'dap': peer}, device_id_type=MESH)
    pl.semaphore_wait(barrier, 2 * side - 1)
    for t in range(side):
        dst = y * 2 * side + (c * half + t // 2) * 2 + t % 2

        @pl.when(dst != me)
        def _():
            remote(block_ref.at[t], rows_out.at[x], send_sem.at[t], recv_sem.at[x], dst).start()

        @pl.when(dst == me)
        def _():
            rows_out[x] = block_ref[t]
    for t in range(side):
        dst = y * 2 * side + (c * half + t // 2) * 2 + t % 2
        src = y * 2 * side + t * 2 + core

        @pl.when(dst != me)
        def _():
            remote(block_ref.at[t], rows_out.at[x], send_sem.at[t], recv_sem.at[x], dst).wait_send()

        @pl.when(src != me)
        def _():
            remote(block_ref.at[t], rows_out.at[t], send_sem.at[t], recv_sem.at[t], dst).wait_recv()


def block_to_rows(side, block):
    slots, r, w, ch = block.shape
    return pl.pallas_call(
        functools.partial(block_to_rows_kernel, side),
        out_shape=jax.ShapeDtypeStruct((side, r, w, ch), block.dtype),
        in_specs=[vmem()], out_specs=vmem(),
        scratch_shapes=[pltpu.SemaphoreType.DMA((side,)), pltpu.SemaphoreType.DMA((side,))],
        compiler_params=params(4), name='block_to_rows')(block)


def exchange_kernel(n, n_gather, n_swap, *refs):
    k_in = n_gather + n_swap
    ins, outs, (send_sem, recv_sem) = refs[:k_in], refs[k_in:2 * k_in], refs[2 * k_in:]
    me = lax.axis_index('dap')
    greet_all(me, n)
    copies = []
    for k in range(1, n):
        dst = lax.rem(me + k, n)
        for a in range(k_in):
            src = ins[a] if a < n_gather else ins[a].at[dst]
            cp = remote(src, outs[a].at[me], send_sem.at[a, k], recv_sem.at[a, k], dst)
            cp.start()
            copies.append(cp)
    for a in range(k_in):
        outs[a][me] = ins[a][...] if a < n_gather else ins[a][me]
    for cp in copies:
        cp.wait()


def exchange(n, cid, gathers, swaps):
    ops = list(gathers) + list(swaps)
    shapes = [jax.ShapeDtypeStruct((n,) + g.shape, g.dtype) for g in gathers] + [jax.ShapeDtypeStruct(s.shape, s.dtype) for s in swaps]
    return pl.pallas_call(
        functools.partial(exchange_kernel, n, len(gathers), len(swaps)),
        out_shape=shapes, in_specs=[vmem()] * len(ops), out_specs=[vmem()] * len(ops),
        scratch_shapes=[pltpu.SemaphoreType.DMA((len(ops), n))] * 2,
        compiler_params=params(cid), name=f'exchange{cid}')(*ops)


def solution(mesh):
    n = mesh.shape['dap']
    side = math.isqrt(n // 2)
    assert 2 * side * side == n

    def block(msa, pair, mask_full, res_mask, row_bias_w, row_qkvg_w, row_out_w, col_query_w, col_kv_w, col_gate_w, col_out_w, opm_proj_w, opm_out_w, start_bias_w, start_qkvg_w, start_out_w, end_bias_w, end_qkvg_w, end_out_w):
        seq, res, ch = msa.shape
        r = pair.shape[0]
        pc = pair.shape[-1]
        w = res // side
        heads, hd = col_gate_w.shape[1:]
        dev_index = lax.axis_index('dap')
        y, x, core = position(dev_index, side)
        seq_mask = lax.dynamic_slice_in_dim(mask_full, dev_index * seq, seq, axis=0)

        row_bias = matmul_bf('ijc,ch->hij', layer_norm(pair), row_bias_w)
        bias_all, pair_blk = entry_exchange(n, side, row_bias, pair.reshape(r, side, w, pc))
        bias_full = bias_all.transpose(1, 0, 2, 3).reshape(row_bias.shape[0], res, res)
        msa_t, ln_t, qsum = row_attention(msa, bias_full, seq_mask, row_qkvg_w, row_out_w)

        count = (jnp.sum(mask_full, axis=0).astype(F32) + 1e-10)[None, :]
        query = all_reduce(n, 1, combine_sum, finish_query, qsum[None], [count, col_query_w.transpose(2, 1, 0).reshape(-1, ch)], (hd, heads, res))
        part = col_sums(ln_t, query, seq_mask, col_kv_w, heads, hd)
        attended = all_reduce(n, 2, combine_softmax, finish_plain, part, [], part.shape[1:])
        msa, proj = col_out(msa_t, ln_t, attended, seq_mask, col_gate_w, col_out_w, opm_proj_w)

        e = opm_proj_w.shape[-1]
        proj = proj.reshape(seq, 2, e, res).transpose(1, 3, 2, 0)
        outer = opm_exchange(side, proj[0].reshape(side, w * e, seq), proj[1].reshape(side, w * e, seq))
        rows0 = y * w + core * (w // 2)
        mask_bf = mask_full.astype(BF16)
        mask_i = lax.dynamic_slice_in_dim(mask_bf, rows0, w // 2, axis=1)
        mask_j = lax.dynamic_slice_in_dim(mask_bf, x * w, w, axis=1)
        counts = jnp.einsum('si,sj->ij', mask_i, mask_j, preferred_element_type=F32)
        update = jnp.einsum('iejf,efc->ijc', outer.reshape(w // 2, e, w, e), opm_out_w, preferred_element_type=F32) / (1e-3 + counts)[:, :, None]
        pair_blk = (pair_blk.reshape(w // 2, w, pc) + update).astype(BF16)
        rows = block_to_rows(side, pair_blk.reshape(side, r, w, pc))
        pair = rows.transpose(1, 0, 2, 3).reshape(r, res, pc)

        pair_ln = layer_norm(pair)
        start_all, = exchange(n, 5, [matmul_bf('ijc,ch->hij', pair_ln, start_bias_w)], [])
        start_full = start_all.transpose(1, 0, 2, 3).reshape(-1, res, res)
        pair = triangle_rows(pair, pair_ln, start_full, res_mask, start_qkvg_w, start_out_w)

        end_bias = matmul_bf('ijc,ch->hij', layer_norm(pair), end_bias_w)
        end_all, cols = exchange(n, 6, [end_bias], [pair.reshape(r, n, r, pc).transpose(1, 2, 0, 3)])
        end_full = end_all.transpose(1, 3, 0, 2).reshape(-1, res, res)
        cols = cols.transpose(1, 0, 2, 3).reshape(r, res, pc)
        cols = triangle_rows(cols, layer_norm(cols), end_full, res_mask, end_qkvg_w, end_out_w)
        back, = exchange(n, 7, [], [cols.reshape(r, n, r, pc).transpose(1, 2, 0, 3)])
        pair_out = back.transpose(1, 0, 2, 3).reshape(r, res, pc)
        return msa, pair_out

    row_spec = P(('data', 'dap'), None, None)
    in_specs = (row_spec, row_spec, P('data', None), P('data')) + (P(),) * 15
    return jax.shard_map(block, mesh=mesh, in_specs=in_specs, out_specs=(row_spec, row_spec), check_vma=False)
```

```python
import functools
import math

import jax
import jax.numpy as jnp
from jax import lax
from jax.experimental import pallas as pl
from jax.experimental.pallas import tpu as pltpu
from jax.sharding import PartitionSpec as P

MESH = pl.DeviceIdType.MESH
F32 = jnp.float32
BF16 = jnp.bfloat16


def layer_norm(values):
    widened = values.astype(F32)
    mean_val = jnp.mean(widened, axis=-1, keepdims=True)
    centered = widened - mean_val
    variance = jnp.mean(centered * centered, axis=-1, keepdims=True)
    return (centered * lax.rsqrt(variance + 1e-5)).astype(BF16)


def mask_bias(mask_vals):
    return (mask_vals.astype(F32) - 1.0) * 1e4


def matmul_bf(einsum_form, left_arr, right_arr):
    return jnp.einsum(einsum_form, left_arr, right_arr, preferred_element_type=F32).astype(BF16)


def gated_out(einsum_form, gate_proj, attended, out_w):
    gated_vals = (jax.nn.sigmoid(gate_proj.astype(F32)) * attended).astype(BF16)
    return jnp.einsum(einsum_form, gated_vals, out_w, preferred_element_type=F32)


LOG2E = 1.4426950408889634

def norm_cols(x):
    mean = jnp.mean(x, axis=0, keepdims=True)
    cen = x - mean
    var = jnp.mean(cen * cen, axis=0, keepdims=True)
    return (cen * lax.rsqrt(var + 1e-5)).astype(BF16)


def row_kernel(heads, hd, m_ref, bias_ref, maskc_ref, maskl_ref, pick_ref, wt_ref, wo_ref, m_out, ln_out, q_out,
               x_buf, q_buf, v_buf, g_buf, k_buf, att_buf):
    @pl.when(pl.program_id(0) == 0)
    def _():
        q_out[...] = jnp.zeros_like(q_out)
    seqs, ch, res = m_ref.shape
    width = heads * hd
    scale = LOG2E * hd ** -0.5
    for s in range(seqs):
        x_buf[:, s * res:(s + 1) * res] = m_ref[s].astype(F32)
    ln = norm_cols(x_buf[...])
    proj = jnp.dot(wt_ref[...], ln, preferred_element_type=F32)
    q_buf[...] = proj[:width].astype(BF16)
    v_buf[...] = proj[2 * width:3 * width].astype(BF16)
    g_buf[...] = proj[3 * width:].astype(BF16)
    for s in range(seqs):
        k_buf[s] = proj[width:2 * width, s * res:(s + 1) * res].T.astype(BF16)

    units = [(s, p) for s in range(seqs) for p in range(heads // 2)]

    def logits_of(u):
        s, p = u
        qt = q_buf[:, s * res:(s + 1) * res]
        return jnp.dot(k_buf[s], jnp.concatenate([qt, qt], axis=1) * pick_ref[p], preferred_element_type=F32)

    def weights_of(u, raw):
        s, p = u
        mcol = jnp.broadcast_to(maskc_ref[0, :, s:s + 1], (res, 2 * res))
        t = raw * scale + bias_ref[p] + mcol
        w = jnp.exp2(t - jnp.max(t, axis=0, keepdims=True))
        return w.astype(BF16), 1.0 / jnp.sum(w, axis=0, keepdims=True)

    def attend(u, w, den):
        s, p = u
        o = jnp.dot(v_buf[2 * p * hd:2 * (p + 1) * hd, s * res:(s + 1) * res], w, preferred_element_type=F32) * den
        lo = 2 * p * hd
        att_buf[lo:lo + hd, s * res:(s + 1) * res] = o[:hd, :res]
        att_buf[lo + hd:lo + 2 * hd, s * res:(s + 1) * res] = o[hd:, res:]

    raws = [logits_of(units[0]), logits_of(units[1])]
    prev = None
    for i, u in enumerate(units):
        if i + 2 < len(units):
            raws.append(logits_of(units[i + 2]))
        cur = weights_of(u, raws.pop(0))
        if prev is not None:
            attend(*prev)
        prev = (u,) + cur
    attend(*prev)
    y = (jax.nn.sigmoid(g_buf[...].astype(F32)) * att_buf[...]).astype(BF16)
    new = (x_buf[...] + jnp.dot(wo_ref[...], y, preferred_element_type=F32)).astype(BF16)
    m_out[0] = new
    ln2 = norm_cols(new.astype(F32))
    ln_out[0] = ln2
    masked = ln2.astype(F32) * maskl_ref[0]
    total = masked[:, :res]
    for s in range(1, seqs):
        total += masked[:, s * res:(s + 1) * res]
    q_out[...] += total


def row_attention(msa, bias_full, seq_mask, qkvg_w, out_w, block=8):
    seq, res, ch = msa.shape
    heads, hd = out_w.shape[:2]
    pairs = heads // 2
    steps = seq // block
    bias = (bias_full.astype(F32) * LOG2E).transpose(0, 2, 1).reshape(pairs, 2, res, res).transpose(0, 2, 1, 3).reshape(pairs, res, 2 * res)
    maskf = seq_mask.astype(F32)
    maskc = ((maskf - 1.0) * (1e4 * LOG2E)).reshape(steps, block, res).transpose(0, 2, 1)
    maskl = maskf.reshape(steps, 1, block * res)
    row_head = jnp.arange(heads * hd) // hd
    lane_head = jnp.arange(2 * res) // res
    pick = (row_head[None, :, None] == (2 * jnp.arange(pairs)[:, None, None] + lane_head[None, None, :])).astype(BF16)
    wt = qkvg_w.reshape(ch, -1).T
    wo = out_w.reshape(heads * hd, ch).T
    full = lambda a: pl.BlockSpec(a.shape, lambda g: (0,) * a.ndim)
    wide = jax.ShapeDtypeStruct((steps, ch, block * res), BF16)
    lanes = block * res
    return pl.pallas_call(
        functools.partial(row_kernel, heads, hd),
        grid=(steps,),
        out_shape=[wide, wide, jax.ShapeDtypeStruct((ch, res), F32)],
        in_specs=[pl.BlockSpec((block, ch, res), lambda g: (g, 0, 0)), full(bias), pl.BlockSpec((1, res, block), lambda g: (g, 0, 0)),
                  pl.BlockSpec((1, 1, lanes), lambda g: (g, 0, 0)), full(pick), full(wt), full(wo)],
        out_specs=[pl.BlockSpec((1, ch, lanes), lambda g: (g, 0, 0))] * 2 + [pl.BlockSpec((ch, res), lambda g: (0, 0))],
        scratch_shapes=[pltpu.VMEM((ch, lanes), F32), pltpu.VMEM((heads * hd, lanes), BF16), pltpu.VMEM((heads * hd, lanes), BF16),
                        pltpu.VMEM((heads * hd, lanes), BF16), pltpu.VMEM((block, res, heads * hd), BF16), pltpu.VMEM((heads * hd, lanes), F32)],
        compiler_params=pltpu.CompilerParams(dimension_semantics=("arbitrary",), vmem_limit_bytes=48 * 1024 * 1024),
        name='row_attention')(msa.transpose(0, 2, 1), bias, maskc, maskl, pick, wt, wo)


def col_sums_kernel(heads, hd, ln_ref, q_ref, maskb_ref, wkv_ref, part_out, logit_buf, val_buf):
    steps, ch, lanes = ln_ref.shape
    res = q_ref.shape[-1]
    block = lanes // res
    scale = hd ** -0.5
    qd = [q_ref[d] for d in range(hd)]

    def first(g, top):
        kv = jnp.dot(wkv_ref[...], ln_ref[g], preferred_element_type=F32).astype(BF16).astype(F32)
        bias = maskb_ref[g]
        for u in range(block):
            k = kv[:hd, u * res:(u + 1) * res]
            logit = qd[0] * k[0:1]
            for d in range(1, hd):
                logit += qd[d] * k[d:d + 1]
            logit = logit * scale + bias[u:u + 1]
            logit_buf[g * block + u] = logit
            val_buf[g * block + u] = kv[hd:, u * res:(u + 1) * res]
            top = jnp.maximum(top, logit)
        return top
    top = lax.fori_loop(0, steps, first, jnp.full((heads, res), -jnp.inf, F32))

    def second(g, carry):
        den, acc = carry
        acc = list(acc)
        for u in range(block):
            s = g * block + u
            w = jnp.exp(logit_buf[s] - top)
            den = den + w
            wb = w.astype(BF16).astype(F32)
            val = val_buf[s]
            for d in range(hd):
                acc[d] = acc[d] + wb * val[d:d + 1]
        return den, tuple(acc)
    zero = jnp.zeros((heads, res), F32)
    den, acc = lax.fori_loop(0, steps, second, (zero, (zero,) * hd))
    for d in range(hd):
        rows = slice(d * heads, (d + 1) * heads)
        part_out[0, rows] = acc[d]
        part_out[1, rows] = top
        part_out[2, rows] = den


def col_sums(ln, query, seq_mask, kv_w, heads, hd):
    steps, ch, lanes = ln.shape
    seq, res = seq_mask.shape
    vm = pl.BlockSpec(memory_space=pltpu.VMEM)
    maskb = ((seq_mask.astype(F32) - 1.0) * 1e4).reshape(steps, seq // steps, res)
    return pl.pallas_call(
        functools.partial(col_sums_kernel, heads, hd),
        out_shape=jax.ShapeDtypeStruct((3, hd * heads, res), F32),
        in_specs=[vm] * 4, out_specs=vm,
        scratch_shapes=[pltpu.VMEM((seq, heads, res), F32), pltpu.VMEM((seq, hd, res), F32)],
        compiler_params=pltpu.CompilerParams(vmem_limit_bytes=48 * 1024 * 1024),
        name='col_sums')(ln, query, maskb, kv_w.reshape(ch, -1).T)


def col_out_kernel(m_ref, ln_ref, att_ref, maskl_ref, wg_ref, wo_ref, wp_ref, m_out, p_out):
    seqs, ch, res = m_out.shape
    att = jnp.concatenate([att_ref[...]] * seqs, axis=1)
    gate = jnp.dot(wg_ref[...], ln_ref[0], preferred_element_type=F32).astype(BF16).astype(F32)
    y = (jax.nn.sigmoid(gate) * att).astype(BF16)
    new = (m_ref[0].astype(F32) + jnp.dot(wo_ref[...], y, preferred_element_type=F32)).astype(BF16)
    newf = new.astype(F32)
    for s in range(seqs):
        m_out[s] = new[:, s * res:(s + 1) * res]
    proj = jnp.dot(wp_ref[...], norm_cols(newf), preferred_element_type=F32).astype(BF16)
    proj = (proj.astype(F32) * maskl_ref[0]).astype(BF16)
    for s in range(seqs):
        p_out[s] = proj[:, s * res:(s + 1) * res]


def col_out(m, ln, att, seq_mask, gate_w, out_w, proj_w):
    steps, ch, lanes = m.shape
    seq, res = seq_mask.shape
    block = seq // steps
    wg, wo = gate_w.transpose(2, 1, 0).reshape(-1, ch), out_w.transpose(2, 1, 0).reshape(ch, -1)
    wp = proj_w.reshape(ch, -1).T
    maskl = seq_mask.astype(F32).reshape(steps, 1, lanes)
    full = lambda a: pl.BlockSpec(a.shape, lambda g: (0,) * a.ndim)
    blk = pl.BlockSpec((1, ch, lanes), lambda g: (g, 0, 0))
    m_new, proj = pl.pallas_call(
        col_out_kernel, grid=(steps,),
        out_shape=[jax.ShapeDtypeStruct((seq, ch, res), BF16), jax.ShapeDtypeStruct((seq, wp.shape[0], res), BF16)],
        in_specs=[blk, blk, full(att), pl.BlockSpec((1, 1, lanes), lambda g: (g, 0, 0)), full(wg), full(wo), full(wp)],
        out_specs=[pl.BlockSpec((block, ch, res), lambda g: (g, 0, 0)), pl.BlockSpec((block, wp.shape[0], res), lambda g: (g, 0, 0))],
        compiler_params=pltpu.CompilerParams(dimension_semantics=("arbitrary",), vmem_limit_bytes=48 * 1024 * 1024),
        name='col_out')(m, ln, att, maskl, wg, wo, wp)
    return m_new.transpose(0, 2, 1), proj


def remote(src, dst, send_sem, recv_sem, dev):
    return pltpu.make_async_remote_copy(src_ref=src, dst_ref=dst, send_sem=send_sem, recv_sem=recv_sem,
                                        device_id={'dap': dev}, device_id_type=MESH)


def greet_all(me, n):
    barrier = pltpu.get_barrier_semaphore()
    for k in range(1, n):
        pl.semaphore_signal(barrier, inc=1, device_id={'dap': lax.rem(me + k, n)}, device_id_type=MESH)
    pl.semaphore_wait(barrier, n - 1)


def vmem():
    return pl.BlockSpec(memory_space=pltpu.VMEM)


def params(cid, limit=None):
    return pltpu.CompilerParams(collective_id=cid, has_side_effects=True, vmem_limit_bytes=limit)


def position(me, side):
    return me // (2 * side), (me // 2) % side, me % 2


def rows_to_block(me, side, rows_ref, block_ref, send_sem, recv_sem):
    y, x, c = position(me, side)
    half = side // 2
    slot = (x % half) * 2 + c
    core = x // half
    for t in range(side):
        dst = y * 2 * side + t * 2 + core

        @pl.when(dst != me)
        def _():
            remote(rows_ref.at[:, t], block_ref.at[slot], send_sem.at[t], recv_sem.at[slot], dst).start()

        @pl.when(dst == me)
        def _():
            block_ref[slot] = rows_ref[:, t]


def rows_to_block_wait(me, side, rows_ref, block_ref, send_sem, recv_sem):
    y, x, c = position(me, side)
    half = side // 2
    core = x // half
    for t in range(side):
        dst = y * 2 * side + t * 2 + core
        src = y * 2 * side + (c * half + t // 2) * 2 + t % 2

        @pl.when(dst != me)
        def _():
            remote(rows_ref.at[:, t], block_ref.at[t], send_sem.at[t], recv_sem.at[t], dst).wait_send()

        @pl.when(src != me)
        def _():
            remote(rows_ref.at[:, 0], block_ref.at[t], send_sem.at[t], recv_sem.at[t], dst).wait_recv()


def entry_kernel(n, side, bias_ref, rows_ref, bias_out, block_out, send_sem, recv_sem, bsend, brecv):
    me = lax.axis_index('dap')
    greet_all(me, n)
    copies = []
    for k in range(1, n):
        cp = remote(bias_ref, bias_out.at[me], send_sem.at[k], recv_sem.at[k], lax.rem(me + k, n))
        cp.start()
        copies.append(cp)
    rows_to_block(me, side, rows_ref, block_out, bsend, brecv)
    bias_out[me] = bias_ref[...]
    rows_to_block_wait(me, side, rows_ref, block_out, bsend, brecv)
    for cp in copies:
        cp.wait()


def entry_exchange(n, side, bias, rows):
    r, sides, w, ch = rows.shape
    return pl.pallas_call(
        functools.partial(entry_kernel, n, side),
        out_shape=[jax.ShapeDtypeStruct((n,) + bias.shape, bias.dtype),
                   jax.ShapeDtypeStruct((side, r, w, ch), rows.dtype)],
        in_specs=[vmem(), vmem()], out_specs=[vmem(), vmem()],
        scratch_shapes=[pltpu.SemaphoreType.DMA((n,)), pltpu.SemaphoreType.DMA((n,)),
                        pltpu.SemaphoreType.DMA((side,)), pltpu.SemaphoreType.DMA((side,))],
        compiler_params=params(0), name='entry_exchange')(bias, rows)


def reduce_kernel(n, combine, finish, n_extra, *refs):
    part_ref, extra, out_ref = refs[0], refs[1:1 + n_extra], refs[1 + n_extra]
    cut, got, mine, back, send_sem, recv_sem, send2, recv2 = refs[2 + n_extra:]
    me = lax.axis_index('dap')
    terms, width, res = part_ref.shape
    own = res // n
    for t in range(terms):
        flat = part_ref[t].T
        for p in range(n):
            cut[p, t] = flat[p * own:(p + 1) * own]
    greet_all(me, n)
    copies = []
    for k in range(1, n):
        dst = lax.rem(me + k, n)
        cp = remote(cut.at[dst], got.at[me], send_sem.at[k], recv_sem.at[k], dst)
        cp.start()
        copies.append(cp)
    got[me] = cut[me]
    for cp in copies:
        cp.wait()
    total = combine(got[...])
    mine[...] = total
    back[me] = total
    copies = []
    for k in range(1, n):
        cp = remote(mine, back.at[me], send2.at[k], recv2.at[k], lax.rem(me + k, n))
        cp.start()
        copies.append(cp)
    for cp in copies:
        cp.wait()
    whole = jnp.concatenate([back[p] for p in range(n)], axis=0)
    finish(whole.T, extra, out_ref)


def all_reduce(n, cid, combine, finish, part, extra, out_shape):
    terms, width, res = part.shape
    own = res // n
    return pl.pallas_call(
        functools.partial(reduce_kernel, n, combine, finish, len(extra)),
        out_shape=jax.ShapeDtypeStruct(out_shape, F32),
        in_specs=[vmem()] * (1 + len(extra)), out_specs=vmem(),
        scratch_shapes=[pltpu.VMEM((n, terms, own, width), F32)] * 2 + [pltpu.VMEM((own, width), F32), pltpu.VMEM((n, own, width), F32)]
        + [pltpu.SemaphoreType.DMA((n,))] * 4,
        compiler_params=params(cid), name=f'all_reduce{cid}')(part, *extra)


def combine_sum(got):
    return jnp.sum(got[:, 0], axis=0)


def combine_softmax(got):
    acc, top, den = got[:, 0], got[:, 1], got[:, 2]
    scale = jnp.exp(top - jnp.max(top, axis=0, keepdims=True))
    return jnp.sum(acc * scale, axis=0) / jnp.sum(den * scale, axis=0)


def finish_query(total, extra, out_ref):
    count_ref, w_ref = extra
    hd, heads, res = out_ref.shape
    mean = (total / count_ref[...]).astype(BF16)
    query = jnp.dot(w_ref[...], mean, preferred_element_type=F32).astype(BF16).astype(F32)
    for d in range(hd):
        out_ref[d] = query[d * heads:(d + 1) * heads]


def finish_plain(total, extra, out_ref):
    out_ref[...] = total


def norm_rows(x):
    mean = jnp.mean(x, axis=-1, keepdims=True)
    cen = x - mean
    var = jnp.mean(cen * cen, axis=-1, keepdims=True)
    return (cen * lax.rsqrt(var + 1e-5)).astype(BF16)


def triangle(z_ref, bias_ref, maskb, qkvg_ref, out_w_ref, heads):
    rows, res, ch = z_ref.shape
    width = qkvg_ref.shape[-1] // 4
    hd = width // heads
    lane_head = lax.broadcasted_iota(jnp.int32, (res, width), 1) // hd
    picks = [(lane_head == h).astype(F32) for h in range(heads)]
    pick_bf = jnp.concatenate(picks, axis=0).astype(BF16)
    bias = bias_ref[...].reshape(heads * res, res) + maskb
    projs = [jnp.dot(norm_rows(z_ref[i]), qkvg_ref[...], preferred_element_type=F32) for i in range(rows)]
    raws = []
    for i in range(rows):
        q = projs[i][:, :width].astype(BF16)
        k = projs[i][:, width:2 * width].astype(BF16)
        raws.append(lax.dot_general(jnp.concatenate([q] * heads, axis=0) * pick_bf, k, (((1,), (1,)), ((), ())), preferred_element_type=F32))
    outs = []
    for i in range(rows):
        t = raws[i] * hd ** -0.5 + bias
        w = jnp.exp(t - jnp.max(t, axis=-1, keepdims=True))
        den = 1.0 / jnp.sum(w, axis=-1, keepdims=True)
        v = projs[i][:, 2 * width:3 * width].astype(BF16)
        outs.append(jnp.dot(w.astype(BF16), v, preferred_element_type=F32) * den)
    for i in range(rows):
        att = outs[i][:res] * picks[0]
        for h in range(1, heads):
            att += outs[i][h * res:(h + 1) * res] * picks[h]
        gate = projs[i][:, 3 * width:].astype(BF16).astype(F32)
        y = (jax.nn.sigmoid(gate) * att).astype(BF16)
        z_ref[i] = (z_ref[i] + jnp.dot(y, out_w_ref[...], preferred_element_type=F32)).astype(BF16).astype(F32)


def pair_kernel(n, side, heads, a_ref, c_ref, zblk_ref, count_ref, w_ref, maskb_ref, sb_ref, sq_ref, so_ref, eb_ref, eq_ref, eo_ref, z_out,
                a_buf, c_buf, acc, got, terms, zsend, zrows, z_f, bias, msg, inbox, flat,
                s1, r1, s2, r2, s3, r3, s4, r4, s5, r5, s6, r6, s7, r7, s8, r8):
    me = lax.axis_index('dap')
    y, x, c = position(me, side)
    seq = a_ref.shape[-1]
    half = side // 2
    blk = a_ref.shape[1]

    def dev(yy, xx, cc):
        return (yy * side + xx) * 2 + cc

    def slot(buf, yy, xx, rows=None):
        rows = pl.ds(0, blk) if rows is None else rows
        return buf.at[yy, xx // 2, rows, pl.ds(pl.multiple_of((xx % 2) * seq, seq), seq)]

    greet_all(me, n)
    order = [0, 1, side - 1] + list(range(2, side - 1))
    first = {}
    for k in [1, side - 1] + list(range(2, side - 1)):
        ty, tx = lax.rem(y + k, side), lax.rem(x + k, side)
        cp = remote(a_ref.at[ty], slot(a_buf, y, x), s1.at[0, k], r1.at[0, k], dev(ty, x, c))
        cq = remote(c_ref.at[tx], slot(c_buf, y, x), s1.at[1, k], r1.at[1, k], dev(y, tx, c))
        cp.start()
        cq.start()
        first[k] = (cp, cq)
    started = []
    hop = {}
    halves = [pl.ds(0, blk // 2), pl.ds(blk // 2, blk // 2)]
    xn, yn = [lax.rem(x + 1, side), lax.rem(x + side - 1, side)], [lax.rem(y + 1, side), lax.rem(y + side - 1, side)]

    def spread(k):
        sy, sx = lax.rem(y - k + side, side), lax.rem(x - k + side, side)
        for d in range(2):
            src = a_ref.at[y] if k == 0 else slot(a_buf, sy, x)
            cp = remote(src, slot(a_buf, sy, x), s2.at[0, k, d], r2.at[0, k, d], dev(y, xn[d], c))
            src = c_ref.at[x] if k == 0 else slot(c_buf, y, sx)
            cq = remote(src, slot(c_buf, y, sx), s2.at[1, k, d], r2.at[1, k, d], dev(yn[d], x, c))
            cp.start()
            cq.start()
            hop[k, d] = (cp, cq)

    def relay(k):
        sy, sx = lax.rem(y - k + side, side), lax.rem(x - k + side, side)
        for d in range(2):
            hop[k, d][0].wait_recv()
            fx = xn[1 - d]
            f = remote(slot(a_buf, sy, fx, halves[d]), slot(a_buf, sy, fx, halves[d]), s3.at[0, k, d], r3.at[0, k, d], dev(y, xn[d], c))
            f.start()
            hop[k, d][1].wait_recv()
            fy = yn[1 - d]
            g = remote(slot(c_buf, fy, sx, halves[d]), slot(c_buf, fy, sx, halves[d]), s3.at[1, k, d], r3.at[1, k, d], dev(yn[d], x, c))
            g.start()
            started.extend([f, g])

    lanes = pl.ds(pl.multiple_of((x % 2) * seq, seq), seq)
    for pos, k in enumerate(order):
        if k:
            first[k][0].wait_recv()
            first[k][1].wait_recv()
        spread(k)
        if pos == 0:
            a_buf[y, x // 2, :, lanes] = a_ref[y]
            c_buf[y, x // 2, :, lanes] = c_ref[x]
        else:
            relay(order[pos - 1])
    relay(order[-1])
    for k in order[1:]:
        first[k][0].wait_send()
        first[k][1].wait_send()
    for pair in hop.values():
        pair[0].wait_send()
        pair[1].wait_send()
    for f in started:
        f.wait()

    cols = blk // 2

    def product(base, dst):
        def chunk(t, _):
            yy, xx = t // half, t % half
            part = lax.dot_general(c_buf[yy, xx], a_buf[yy, xx, pl.ds(pl.multiple_of(base, cols), cols), :], (((1,), (1,)), ((), ())),
                                   preferred_element_type=F32)

            @pl.when(t == 0)
            def _():
                dst[...] = part

            @pl.when(t > 0)
            def _():
                dst[...] += part
            return 0
        lax.fori_loop(0, side * half, chunk, 0)

    product((1 - c) * cols, acc.at[0])
    swap = remote(acc.at[0], got, s4, r4, dev(y, x, 1 - c))
    swap.start()
    product(c * cols, acc.at[1])
    swap.wait()

    w = zblk_ref.shape[2]
    e = blk // w
    per = 128 // e
    lane_i = lax.broadcasted_iota(jnp.int32, (w, 128), 1) // e
    keep = [(lane_i == i).astype(F32) for i in range(per)]

    def place(f, _):
        for g in range(cols // 128):
            rows = pl.ds(pl.multiple_of(f * w, w), w)
            both = acc[1, rows, g * 128:(g + 1) * 128] + got[rows, g * 128:(g + 1) * 128]
            for i in range(per):
                r0 = (g * per + i) * w
                terms[r0:r0 + w, pl.ds(pl.multiple_of(f * 128, 128), 128)] = (both * keep[i]).astype(BF16)
        return 0
    lax.fori_loop(0, blk // w, place, 0)
    update = jnp.dot(terms[...], w_ref[...], preferred_element_type=F32) / count_ref[...]
    slots, r, _, ch = zblk_ref.shape
    fresh = (zblk_ref[...].reshape(slots * r * w, ch).astype(F32) + update).astype(BF16)
    zsend[...] = fresh.reshape(slots, r, w, ch)

    my_core = x // half
    for t in range(side):
        dst = y * 2 * side + (c * half + t // 2) * 2 + t % 2

        @pl.when(dst != me)
        def _():
            remote(zsend.at[t], zrows.at[x], s5.at[t], r5.at[x], dst).start()

        @pl.when(dst == me)
        def _():
            zrows[x] = zsend[t]
    for t in range(side):
        dst = y * 2 * side + (c * half + t // 2) * 2 + t % 2
        src = y * 2 * side + t * 2 + my_core

        @pl.when(dst != me)
        def _():
            remote(zsend.at[t], zrows.at[x], s5.at[t], r5.at[x], dst).wait_send()

        @pl.when(src != me)
        def _():
            remote(zsend.at[t], zrows.at[t], s5.at[t], r5.at[t], dst).wait_recv()
    for t in range(side):
        z_f[:, t * w:(t + 1) * w, :] = zrows[t].astype(F32)

    res = side * w
    nh = r * heads

    def bias_rows(wb_ref):
        parts = [lax.dot_general(wb_ref[...], norm_rows(z_f[i]), (((1,), (1,)), ((), ())), preferred_element_type=F32)[:heads] for i in range(r)]
        return jnp.concatenate(parts, axis=0).astype(BF16)

    def gather_bias(turn):
        for h in range(heads):
            plane = flat[pl.ds(h, res, stride=heads), :]
            bias[h] = plane.T if turn else plane

    def exchange_all(box, src_of, send_sem, recv_sem):
        copies = []
        for k in range(1, n):
            dst = lax.rem(me + k, n)
            cp = remote(src_of(dst), box.at[me], send_sem.at[k], recv_sem.at[k], dst)
            cp.start()
            copies.append(cp)
        box[me] = src_of(me)[...]
        for cp in copies:
            cp.wait()

    msg[0, 0, :nh] = bias_rows(sb_ref)
    exchange_all(inbox.at[0, :, :nh], lambda p: msg.at[0, 0, :nh], s6, r6)
    flat[...] = inbox[0, :, :nh].astype(F32).reshape(n * nh, res)
    gather_bias(False)
    triangle(z_f, bias, maskb_ref[...], sq_ref, so_ref, heads)

    rr = r * r

    def pack(slot_id):
        for p in range(n):
            msg[slot_id, p, :rr] = jnp.concatenate([z_f[i, p * r:(p + 1) * r, :] for i in range(r)], axis=0).astype(BF16)

    def unpack(slot_id):
        flat[...] = inbox[slot_id, :, :rr].astype(F32).reshape(n * rr, ch)
        for i in range(r):
            z_f[i] = flat[pl.ds(i, res, stride=r), :]

    pack(1)
    rows_b = bias_rows(eb_ref)
    for p in range(n):
        msg[1, p, rr:] = rows_b
    exchange_all(inbox.at[1], lambda p: msg.at[1, p], s7, r7)
    flat[...] = inbox[1, :, rr:].astype(F32).reshape(n * nh, res)
    gather_bias(True)
    unpack(1)
    triangle(z_f, bias, maskb_ref[...], eq_ref, eo_ref, heads)
    pack(2)
    exchange_all(inbox.at[2, :, :rr], lambda p: msg.at[2, p, :rr], s8, r8)
    unpack(2)
    z_out[...] = z_f[...].astype(BF16)


def pair_steps(n, side, heads, a, c, zblk, count, w, maskb, weights):
    blk, seq = a.shape[1:]
    slots, r, wd, ch = zblk.shape
    res = side * wd
    assert r * r == r * heads and res == 128 and seq == 128
    buf = pltpu.VMEM((side, side // 2, blk, 2 * seq), BF16)
    dma = pltpu.SemaphoreType.DMA
    box = pltpu.VMEM((3, n, 2 * r * r, ch), BF16)
    half = pltpu.VMEM((blk, blk // 2), F32)
    ops = [a, c, zblk, count, w, maskb] + weights
    return pl.pallas_call(
        functools.partial(pair_kernel, n, side, heads),
        out_shape=jax.ShapeDtypeStruct((r, res, ch), BF16),
        in_specs=[vmem()] * len(ops), out_specs=vmem(),
        scratch_shapes=[buf, buf, pltpu.VMEM((2, blk, blk // 2), F32), half, pltpu.VMEM((slots * r * wd, blk * 128 // wd), BF16),
                        pltpu.VMEM(zblk.shape, BF16), pltpu.VMEM((side, r, wd, ch), BF16), pltpu.VMEM((r, res, ch), F32),
                        pltpu.VMEM((heads, res, res), F32), box, box, pltpu.VMEM((n * r * r, ch), F32),
                        dma((2, side)), dma((2, side)), dma((2, side, 2)), dma((2, side, 2)), dma((2, side, 2)), dma((2, side, 2)),
                        dma, dma, dma((side,)), dma((side,))] + [dma((n,))] * 6,
        compiler_params=params(3, 60 * 1024 * 1024), name='pair_steps')(*ops)


def solution(mesh):
    n = mesh.shape['dap']
    side = math.isqrt(n // 2)
    assert 2 * side * side == n

    def block(msa, pair, mask_full, res_mask, row_bias_w, row_qkvg_w, row_out_w, col_query_w, col_kv_w, col_gate_w, col_out_w, opm_proj_w, opm_out_w, start_bias_w, start_qkvg_w, start_out_w, end_bias_w, end_qkvg_w, end_out_w):
        seq, res, ch = msa.shape
        r = pair.shape[0]
        pc = pair.shape[-1]
        w = res // side
        heads, hd = col_gate_w.shape[1:]
        dev_index = lax.axis_index('dap')
        y, x, core = position(dev_index, side)
        seq_mask = lax.dynamic_slice_in_dim(mask_full, dev_index * seq, seq, axis=0)

        row_bias = matmul_bf('ijc,ch->hij', layer_norm(pair), row_bias_w)
        bias_all, pair_blk = entry_exchange(n, side, row_bias, pair.reshape(r, side, w, pc))
        bias_full = bias_all.transpose(1, 0, 2, 3).reshape(row_bias.shape[0], res, res)
        msa_t, ln_t, qsum = row_attention(msa, bias_full, seq_mask, row_qkvg_w, row_out_w)

        count = (jnp.sum(mask_full, axis=0).astype(F32) + 1e-10)[None, :]
        query = all_reduce(n, 1, combine_sum, finish_query, qsum[None], [count, col_query_w.transpose(2, 1, 0).reshape(-1, ch)], (hd, heads, res))
        part = col_sums(ln_t, query, seq_mask, col_kv_w, heads, hd)
        attended = all_reduce(n, 2, combine_softmax, finish_plain, part, [], part.shape[1:])
        msa, proj = col_out(msa_t, ln_t, attended, seq_mask, col_gate_w, col_out_w, opm_proj_w)

        e = opm_proj_w.shape[-1]
        a = proj[:, :e].transpose(2, 1, 0).reshape(side, w * e, seq)
        c = proj[:, e:].reshape(seq, e, side, w).transpose(2, 1, 3, 0).reshape(side, e * w, seq)
        rows0 = y * w + core * (w // 2)
        mask_bf = mask_full.astype(BF16)
        mask_i = lax.dynamic_slice_in_dim(mask_bf, rows0, w // 2, axis=1)
        mask_j = lax.dynamic_slice_in_dim(mask_bf, x * w, w, axis=1)
        counts = 1e-3 + jnp.einsum('si,sj->ij', mask_i, mask_j, preferred_element_type=F32)
        counts = jnp.broadcast_to(counts[:, :, None], (w // 2, w, pc)).reshape(-1, pc)
        spread_w = jnp.broadcast_to(opm_out_w.transpose(1, 0, 2)[:, None], (e, 128 // e, e, pc)).reshape(-1, pc)
        tri_heads = start_bias_w.shape[-1]
        maskb = mask_bias(res_mask)[None, :]
        weights = [start_bias_w.T, start_qkvg_w.reshape(pc, -1), start_out_w.reshape(-1, pc), end_bias_w.T, end_qkvg_w.reshape(pc, -1), end_out_w.reshape(-1, pc)]
        pair_out = pair_steps(n, side, tri_heads, a, c, pair_blk, counts, spread_w, maskb, weights)
        return msa, pair_out

    row_spec = P(('data', 'dap'), None, None)
    in_specs = (row_spec, row_spec, P('data', None), P('data')) + (P(),) * 15
    return jax.shard_map(block, mesh=mesh, in_specs=in_specs, out_specs=(row_spec, row_spec), check_vma=False)
```

```python
import functools
import math

import jax
import jax.numpy as jnp
from jax import lax
from jax.experimental import pallas as pl
from jax.experimental.pallas import tpu as pltpu
from jax.sharding import PartitionSpec as P

MESH = pl.DeviceIdType.MESH
F32 = jnp.float32
BF16 = jnp.bfloat16
NT = (((1,), (1,)), ((), ()))


def dot(a, b):
    return jnp.dot(a, b, preferred_element_type=F32)


def dot_nt(a, b):
    return lax.dot_general(a, b, NT, preferred_element_type=F32)


LOG2E = 1.4426950408889634
BLOCK = 16


def norm_cols(x):
    mean = jnp.mean(x, axis=0, keepdims=True)
    cen = x - mean
    var = jnp.mean(cen * cen, axis=0, keepdims=True)
    return (cen * lax.rsqrt(var + 1e-5)).astype(BF16)


def wide(ref, g):
    return jnp.concatenate([ref[g * BLOCK + u] for u in range(BLOCK)], axis=1)


def put(ref, g, value):
    res = ref.shape[-1]
    for u in range(BLOCK):
        ref[g * BLOCK + u] = value[:, u * res:(u + 1) * res]


def split_mask(hd):
    whole = jnp.float32(-1e4 * hd ** 0.5)
    high = whole.astype(BF16).astype(F32)
    mid = (whole - high).astype(BF16).astype(F32)
    return high, mid, whole - high - mid


def row_project(heads, hd, m_ref, mask_ref, wt_ref, q_buf, k_buf, v_buf, g_buf):
    seq, ch, res = m_ref.shape
    width = heads * hd
    terms = split_mask(hd)

    def step(g, _):
        proj = jnp.dot(wt_ref[...], norm_cols(wide(m_ref, g).astype(F32)), preferred_element_type=F32)
        put(q_buf, g, proj[:width].astype(BF16))
        put(v_buf, g, proj[2 * width:3 * width].astype(BF16))
        put(g_buf, g, proj[3 * width:].astype(BF16))
        for u in range(BLOCK):
            s = g * BLOCK + u
            off = 1.0 - mask_ref[pl.ds(s, 1), :]
            row = lax.broadcasted_iota(jnp.int32, (16, res), 0)
            extra = jnp.where(row == 0, terms[0], jnp.where(row == 1, terms[1], jnp.where(row == 2, terms[2], 0.0))) * off
            k_buf[s] = jnp.concatenate([proj[width:2 * width, u * res:(u + 1) * res], extra], axis=0).T.astype(BF16)
        return 0
    lax.fori_loop(0, seq // BLOCK, step, 0)


def row_attend(heads, hd, bias_ref, pick_ref, q_buf, k_buf, v_buf, att_buf, raw_buf, w_buf, den_buf):
    seq, width, res = q_buf.shape
    pairs = heads // 2
    scale = LOG2E * hd ** -0.5
    row = lax.broadcasted_iota(jnp.int32, (16, 2 * res), 0)
    ones = jnp.where(row < 3, 1.0, 0.0).astype(BF16)

    def logits(s, b):
        qt = q_buf[s]
        q2 = jnp.concatenate([qt, qt], axis=1)
        keys = k_buf[s]
        for p in range(pairs):
            raw_buf[b, p] = jnp.dot(keys, jnp.concatenate([q2 * pick_ref[p], ones], axis=0), preferred_element_type=F32)

    def weigh(b):
        for p in range(pairs):
            t = raw_buf[b, p] * scale + bias_ref[p]
            w = jnp.exp2(t - jnp.max(t, axis=0, keepdims=True))
            w_buf[b, p] = w.astype(BF16)
            den_buf[b, p] = jnp.broadcast_to(1.0 / jnp.sum(w, axis=0, keepdims=True), (8, 2 * res))

    def values(s, b):
        for p in range(pairs):
            lo = 2 * p * hd
            o = jnp.dot(v_buf[s, lo:lo + 2 * hd], w_buf[b, p], preferred_element_type=F32) * den_buf[b, p, 0:1]
            att_buf[s, lo:lo + hd] = o[:hd, :res]
            att_buf[s, lo + hd:lo + 2 * hd] = o[hd:, res:]

    logits(0, 0)
    logits(1, 1)
    weigh(0)

    def step(t, _):
        s = 2 * t
        logits(jnp.minimum(s + 2, seq - 1), 0)
        weigh(1)
        values(s, 0)
        logits(jnp.minimum(s + 3, seq - 1), 1)
        weigh(0)
        values(s + 1, 1)
        return 0
    lax.fori_loop(0, seq // 2, step, 0)


def row_finish(m_ref, mask_ref, wo_ref, g_buf, att_buf, new_ref, ln_ref):
    seq, ch, res = m_ref.shape

    def step(g, total):
        y = (jax.nn.sigmoid(wide(g_buf, g).astype(F32)) * wide(att_buf, g)).astype(BF16)
        new = (wide(m_ref, g).astype(F32) + jnp.dot(wo_ref[...], y, preferred_element_type=F32)).astype(BF16)
        put(new_ref, g, new)
        ln = norm_cols(new.astype(F32))
        put(ln_ref, g, ln)
        for u in range(BLOCK):
            total += ln[:, u * res:(u + 1) * res].astype(F32) * mask_ref[pl.ds(g * BLOCK + u, 1), :]
        return total
    return lax.fori_loop(0, seq // BLOCK, step, jnp.zeros((ch, res), F32))


def col_sums(query, ln_ref, mask_ref, wkv_ref, logit_buf, val_buf):
    seq, ch, res = ln_ref.shape
    hd, heads = len(query), query[0].shape[0]
    scale = hd ** -0.5

    def first(g, top):
        kv = jnp.dot(wkv_ref[...], wide(ln_ref, g), preferred_element_type=F32).astype(BF16).astype(F32)
        for u in range(BLOCK):
            s = g * BLOCK + u
            k = kv[:hd, u * res:(u + 1) * res]
            logit = query[0] * k[0:1]
            for d in range(1, hd):
                logit += query[d] * k[d:d + 1]
            logit = logit * scale + (mask_ref[pl.ds(s, 1), :] - 1.0) * 1e4
            logit_buf[s] = logit
            val_buf[s] = kv[hd:, u * res:(u + 1) * res]
            top = jnp.maximum(top, logit)
        return top
    top = lax.fori_loop(0, seq // BLOCK, first, jnp.full((heads, res), -jnp.inf, F32))

    def second(g, carry):
        den, acc = carry
        acc = list(acc)
        for u in range(BLOCK):
            s = g * BLOCK + u
            w = jnp.exp(logit_buf[s] - top)
            den = den + w
            wb = w.astype(BF16).astype(F32)
            val = val_buf[s]
            for d in range(hd):
                acc[d] = acc[d] + wb * val[d:d + 1]
        return den, tuple(acc)
    zero = jnp.zeros((heads, res), F32)
    den, acc = lax.fori_loop(0, seq // BLOCK, second, (zero, (zero,) * hd))
    return acc, top, den


def col_finish(att, m_ref, ln_ref, mask_ref, wg_ref, wo_ref, wp_ref, out_ref, proj_ref):
    seq, ch, res = m_ref.shape

    def step(g, _):
        tiled = jnp.concatenate([att] * BLOCK, axis=1)
        gate = jnp.dot(wg_ref[...], wide(ln_ref, g), preferred_element_type=F32).astype(BF16).astype(F32)
        y = (jax.nn.sigmoid(gate) * tiled).astype(BF16)
        new = (wide(m_ref, g).astype(F32) + jnp.dot(wo_ref[...], y, preferred_element_type=F32)).astype(BF16)
        put(out_ref, g, new)
        proj = jnp.dot(wp_ref[...], norm_cols(new.astype(F32)), preferred_element_type=F32).astype(BF16)
        for u in range(BLOCK):
            s = g * BLOCK + u
            proj_ref[s] = (proj[:, u * res:(u + 1) * res].astype(F32) * mask_ref[pl.ds(s, 1), :]).astype(proj_ref.dtype)
        return 0
    lax.fori_loop(0, seq // BLOCK, step, 0)


def remote(src, dst, send_sem, recv_sem, dev):
    return pltpu.make_async_remote_copy(src_ref=src, dst_ref=dst, send_sem=send_sem, recv_sem=recv_sem,
                                        device_id={'dap': dev}, device_id_type=MESH)


def vmem():
    return pl.BlockSpec(memory_space=pltpu.VMEM)


def position(me, side):
    return me // (2 * side), (me // 2) % side, me % 2


def rows_to_block(me, side, rows_ref, block_ref, send_sem, recv_sem):
    y, x, c = position(me, side)
    half = side // 2
    slot = (x % half) * 2 + c
    core = x // half
    for t in range(side):
        dst = y * 2 * side + t * 2 + core

        @pl.when(dst != me)
        def _():
            remote(rows_ref.at[:, t], block_ref.at[slot], send_sem.at[t], recv_sem.at[slot], dst).start()

        @pl.when(dst == me)
        def _():
            block_ref[slot] = rows_ref[:, t]


def rows_to_block_wait(me, side, rows_ref, block_ref, send_sem, recv_sem):
    y, x, c = position(me, side)
    half = side // 2
    core = x // half
    for t in range(side):
        dst = y * 2 * side + t * 2 + core
        src = y * 2 * side + (c * half + t // 2) * 2 + t % 2

        @pl.when(dst != me)
        def _():
            remote(rows_ref.at[:, t], block_ref.at[t], send_sem.at[t], recv_sem.at[t], dst).wait_send()

        @pl.when(src != me)
        def _():
            remote(rows_ref.at[:, 0], block_ref.at[t], send_sem.at[t], recv_sem.at[t], dst).wait_recv()


def norm_rows(x):
    mean = jnp.mean(x, axis=-1, keepdims=True)
    cen = x - mean
    var = jnp.mean(cen * cen, axis=-1, keepdims=True)
    return (cen * lax.rsqrt(var + 1e-5)).astype(BF16)


def triangle(z_ref, bias_ref, maskb, qkvg_ref, out_w_ref, heads):
    rows, res, ch = z_ref.shape
    width = qkvg_ref.shape[0] // 4
    hd = width // heads
    lane_head = lax.broadcasted_iota(jnp.int32, (res, width), 1) // hd
    picks = [(lane_head == h).astype(F32) for h in range(heads)]
    pick_bf = jnp.concatenate(picks, axis=0).astype(BF16)
    bias = bias_ref[...].reshape(heads * res, res) + maskb
    projs = [dot_nt(norm_rows(z_ref[i]), qkvg_ref[...]) for i in range(rows)]
    raws = []
    for i in range(rows):
        q = projs[i][:, :width].astype(BF16)
        k = projs[i][:, width:2 * width].astype(BF16)
        raws.append(lax.dot_general(jnp.concatenate([q] * heads, axis=0) * pick_bf, k, (((1,), (1,)), ((), ())), preferred_element_type=F32))
    outs = []
    for i in range(rows):
        t = raws[i] * hd ** -0.5 + bias
        w = jnp.exp(t - jnp.max(t, axis=-1, keepdims=True))
        den = 1.0 / jnp.sum(w, axis=-1, keepdims=True)
        v = projs[i][:, 2 * width:3 * width].astype(BF16)
        outs.append(jnp.dot(w.astype(BF16), v, preferred_element_type=F32) * den)
    for i in range(rows):
        att = outs[i][:res] * picks[0]
        for h in range(1, heads):
            att += outs[i][h * res:(h + 1) * res] * picks[h]
        gate = projs[i][:, 3 * width:].astype(BF16).astype(F32)
        y = (jax.nn.sigmoid(gate) * att).astype(BF16)
        z_ref[i] = (z_ref[i] + jnp.dot(y, out_w_ref[...], preferred_element_type=F32)).astype(BF16).astype(F32)


def bias_rows(z_f, wb_ref, heads):
    parts = [dot_nt(wb_ref[...], norm_rows(z_f[i]))[:heads] for i in range(z_f.shape[0])]
    return jnp.concatenate(parts, axis=0).astype(BF16)


def combine_sum(got):
    return jnp.sum(got[:, 0], axis=0)


def combine_softmax(got):
    acc, top, den = got[:, 0], got[:, 1], got[:, 2]
    scale = jnp.exp(top - jnp.max(top, axis=0, keepdims=True))
    return jnp.sum(acc * scale, axis=0) / jnp.sum(den * scale, axis=0)


def block_kernel(n, side, dims, m_ref, z_ref, mask_ref, resm_ref, rb_ref, rw_ref, ro_ref, cq_ref, ckv_ref, cg_ref, co_ref, op_ref, ow_ref,
                 sb_ref, sq_ref, so_ref, eb_ref, eq_ref, eo_ref, m_out, z_out,
                 smask, q_buf, k_buf, v_buf, g_buf, att_buf, raw_buf, w_buf, den_buf, rbias, pick, rbox, rflat, wt_row, wt_col,
                 part, cut, got1, mine, back, small, logit_buf, val_buf, a_f32, a_send, c_send, zblk, opm_f32, opmw_buf, count_buf, pairs_buf,
                 a_buf, c_buf, acc, got, terms, zsend, zrows, z_f, bias, msg, inbox, flat,
                 sa, ra, sb, rb, sc1, rc1, sc2, rc2, sd1, rd1, sd2, rd2,
                 s1, r1, s2, r2, s3, r3, s4, r4, s5, r5, s6, r6, s7, r7, s8, r8):
    mh, md, heads = dims
    me = lax.axis_index('dap')
    y, x, c = position(me, side)
    half = side // 2
    seq, ch, res = m_ref.shape
    r, _, w, pc = z_ref.shape
    blk = a_buf.shape[2]
    width = mh * md
    e = op_ref.shape[0] // 2

    def dev(yy, xx, cc):
        return (yy * side + xx) * 2 + cc

    def exchange_all(box, src_of, send_sem, recv_sem):
        copies = []
        for k in range(1, n):
            dst = lax.rem(me + k, n)
            cp = remote(src_of(dst), box.at[me], send_sem.at[k], recv_sem.at[k], dst)
            cp.start()
            copies.append(cp)
        box[me] = src_of(me)[...]
        return copies

    barrier = pltpu.get_barrier_semaphore()
    for k in range(1, n):
        pl.semaphore_signal(barrier, inc=1, device_id={'dap': lax.rem(me + k, n)}, device_id_type=MESH)

    for i in range(r):
        for t in range(side):
            z_f[i, t * w:(t + 1) * w, :] = z_ref[i, t].astype(F32)
    rmsg = rbox.at[n]
    rmsg[...] = bias_rows(z_f, rb_ref, mh)
    pl.semaphore_wait(barrier, n - 1)
    gathers = exchange_all(rbox, lambda p: rmsg, sa, ra)
    rows_to_block(me, side, z_ref, zblk, sb, rb)

    smask[...] = mask_ref[pl.ds(pl.multiple_of(me * seq, seq), seq), :].astype(F32)
    wt_row[...] = ro_ref[...].astype(F32).T.astype(BF16)
    wt_col[...] = co_ref[...].astype(F32).T.astype(BF16)
    row_id = lax.broadcasted_iota(jnp.int32, (width, 2 * res), 0) // md
    lane_id = lax.broadcasted_iota(jnp.int32, (width, 2 * res), 1) // res
    for p in range(mh // 2):
        pick[p] = jnp.where(row_id == 2 * p + lane_id, 1.0, 0.0).astype(BF16)
    row_project(mh, md, m_ref, smask, rw_ref, q_buf, k_buf, v_buf, g_buf)

    for cp in gathers:
        cp.wait()
    rflat[...] = rbox[:n].astype(F32).reshape(n * r * mh, res)
    for h in range(mh):
        rbias[h // 2, :, (h % 2) * res:(h % 2 + 1) * res] = rflat[pl.ds(h, res, stride=mh), :].T * LOG2E
    row_attend(mh, md, rbias, pick, q_buf, k_buf, v_buf, att_buf, raw_buf, w_buf, den_buf)
    new_buf, ln_buf = q_buf, v_buf
    part[0] = row_finish(m_ref, smask, wt_row, g_buf, att_buf, new_buf, ln_buf)

    def all_reduce(terms_n, combine, send1, recv1, send2, recv2):
        own = res // n
        for t in range(terms_n):
            turned = part[t].T
            for p in range(n):
                cut[p, t] = turned[p * own:(p + 1) * own]
        copies = []
        for k in range(1, n):
            dst = lax.rem(me + k, n)
            cp = remote(cut.at[dst, :terms_n], got1.at[me, :terms_n], send1.at[k], recv1.at[k], dst)
            cp.start()
            copies.append(cp)
        got1[me, :terms_n] = cut[me, :terms_n]
        for cp in copies:
            cp.wait()
        total = combine(got1[...])
        slot_id = 0 if terms_n == 1 else 1
        mine[slot_id] = total
        back[slot_id, me] = total
        copies = []
        for k in range(1, n):
            cp = remote(mine.at[slot_id], back.at[slot_id, me], send2.at[k], recv2.at[k], lax.rem(me + k, n))
            cp.start()
            copies.append(cp)
        for cp in copies:
            cp.wait()
        return jnp.concatenate([back[slot_id, p] for p in range(n)], axis=0).T

    count = jnp.sum(mask_ref[...].astype(F32), axis=0, keepdims=True) + 1e-10
    qsum = all_reduce(1, combine_sum, sc1, rc1, sc2, rc2)
    small[...] = dot(cq_ref[...], (qsum / count).astype(BF16)).astype(BF16).astype(F32)
    query = [small[pl.ds(d, mh, stride=md), :] for d in range(md)]
    sums, top, den = col_sums(query, ln_buf, smask, ckv_ref, logit_buf, val_buf)
    for d in range(md):
        part[0, pl.ds(d, mh, stride=md), :] = sums[d]
        part[1, pl.ds(d, mh, stride=md), :] = top
        part[2, pl.ds(d, mh, stride=md), :] = den
    attended = all_reduce(3, combine_softmax, sd1, rd1, sd2, rd2)
    proj = att_buf
    col_finish(attended, new_buf, ln_buf, smask, cg_ref, wt_col, op_ref, m_out, proj)

    planes = proj.reshape(seq * 2 * e, res)

    def turn(t, _):
        a_f32[pl.ds(t, res, stride=e), :] = planes[pl.ds(t, seq, stride=2 * e), :].T
        other = planes[pl.ds(e + t, seq, stride=2 * e), :].T.astype(BF16)
        for b in range(side):
            c_send[b, pl.ds(pl.multiple_of(t * w, w), w), :] = other[b * w:(b + 1) * w]
        return 0
    lax.fori_loop(0, e, turn, 0)
    for b in range(side):
        a_send[b] = a_f32[b * blk:(b + 1) * blk].astype(BF16)
    rows_to_block_wait(me, side, z_ref, zblk, sb, rb)

    def count_pairs():
        step = seq

        def add(t, _):
            rows = mask_ref[pl.ds(pl.multiple_of(t * step, step), step), :].astype(F32)
            pairs_buf[...] += dot(rows.T.astype(BF16), rows.astype(BF16))
            return 0
        pairs_buf[...] = jnp.zeros_like(pairs_buf)
        lax.fori_loop(0, mask_ref.shape[0] // step, add, 0)
        size = (w // 2 * w, res)
        row = lax.broadcasted_iota(jnp.int32, size, 0)
        lane = lax.broadcasted_iota(jnp.int32, size, 1)
        pick_i = jnp.where(lane == y * w + c * (w // 2) + row // w, 1.0, 0.0).astype(BF16)
        whole = pairs_buf[...]
        high = jnp.floor(whole * (1.0 / 128.0))
        both = dot(pick_i, high.astype(BF16)) * 128.0 + dot(pick_i, (whole - high * 128.0).astype(BF16))
        one = jnp.sum(jnp.where(lane == x * w + row % w, both, 0.0), axis=1, keepdims=True)
        count_buf[...] = jnp.broadcast_to(1e-3 + one, size)
        opm_f32[...] = ow_ref[...].astype(F32)
        for f in range(e):
            rows_f = opm_f32[pl.ds(f, e, stride=e), :].astype(BF16)
            for i in range(128 // e):
                opmw_buf[(f * (128 // e) + i) * e:(f * (128 // e) + i + 1) * e, :] = rows_f

    def gather_bias(turned):
        for h in range(heads):
            plane = flat[pl.ds(h, res, stride=heads), :]
            bias[h] = plane.T if turned else plane

    def slot(buf, yy, xx, rows=None):
        rows = pl.ds(0, blk) if rows is None else rows
        return buf.at[yy, xx // 2, rows, pl.ds(pl.multiple_of((xx % 2) * seq, seq), seq)]

    order = [0, 1, side - 1] + list(range(2, side - 1))
    first = {}
    for k in [1, side - 1] + list(range(2, side - 1)):
        ty, tx = lax.rem(y + k, side), lax.rem(x + k, side)
        cp = remote(a_send.at[ty], slot(a_buf, y, x), s1.at[0, k], r1.at[0, k], dev(ty, x, c))
        cq = remote(c_send.at[tx], slot(c_buf, y, x), s1.at[1, k], r1.at[1, k], dev(y, tx, c))
        cp.start()
        cq.start()
        first[k] = (cp, cq)
    started = []
    hop = {}
    halves = [pl.ds(0, blk // 2), pl.ds(blk // 2, blk // 2)]
    xn, yn = [lax.rem(x + 1, side), lax.rem(x + side - 1, side)], [lax.rem(y + 1, side), lax.rem(y + side - 1, side)]

    def spread(k):
        sy, sx = lax.rem(y - k + side, side), lax.rem(x - k + side, side)
        for d in range(2):
            src = a_send.at[y] if k == 0 else slot(a_buf, sy, x)
            cp = remote(src, slot(a_buf, sy, x), s2.at[0, k, d], r2.at[0, k, d], dev(y, xn[d], c))
            src = c_send.at[x] if k == 0 else slot(c_buf, y, sx)
            cq = remote(src, slot(c_buf, y, sx), s2.at[1, k, d], r2.at[1, k, d], dev(yn[d], x, c))
            cp.start()
            cq.start()
            hop[k, d] = (cp, cq)

    def relay(k):
        sy, sx = lax.rem(y - k + side, side), lax.rem(x - k + side, side)
        for d in range(2):
            hop[k, d][0].wait_recv()
            fx = xn[1 - d]
            f = remote(slot(a_buf, sy, fx, halves[d]), slot(a_buf, sy, fx, halves[d]), s3.at[0, k, d], r3.at[0, k, d], dev(y, xn[d], c))
            f.start()
            hop[k, d][1].wait_recv()
            fy = yn[1 - d]
            g = remote(slot(c_buf, fy, sx, halves[d]), slot(c_buf, fy, sx, halves[d]), s3.at[1, k, d], r3.at[1, k, d], dev(yn[d], x, c))
            g.start()
            started.extend([f, g])

    lanes = pl.ds(pl.multiple_of((x % 2) * seq, seq), seq)
    for pos, k in enumerate(order):
        if k:
            first[k][0].wait_recv()
            first[k][1].wait_recv()
        spread(k)
        if pos == 0:
            a_buf[y, x // 2, :, lanes] = a_send[y]
            c_buf[y, x // 2, :, lanes] = c_send[x]
        else:
            relay(order[pos - 1])
    relay(order[-1])
    count_pairs()
    for k in order[1:]:
        first[k][0].wait_send()
        first[k][1].wait_send()
    for pair in hop.values():
        pair[0].wait_send()
        pair[1].wait_send()
    for f in started:
        f.wait()

    cols = blk // 2

    def product(base, dst):
        def chunk(t, _):
            yy, xx = t // half, t % half
            part = lax.dot_general(c_buf[yy, xx], a_buf[yy, xx, pl.ds(pl.multiple_of(base, cols), cols), :], NT, preferred_element_type=F32)

            @pl.when(t == 0)
            def _():
                dst[...] = part

            @pl.when(t > 0)
            def _():
                dst[...] += part
            return 0
        lax.fori_loop(0, side * half, chunk, 0)

    product((1 - c) * cols, acc.at[0])
    swap = remote(acc.at[0], got, s4, r4, dev(y, x, 1 - c))
    swap.start()
    product(c * cols, acc.at[1])
    swap.wait()

    per = 128 // e
    lane_i = lax.broadcasted_iota(jnp.int32, (w, 128), 1) // e
    keep = [(lane_i == i).astype(F32) for i in range(per)]

    def place(f, _):
        for g in range(cols // 128):
            rows = pl.ds(pl.multiple_of(f * w, w), w)
            both = acc[1, rows, g * 128:(g + 1) * 128] + got[rows, g * 128:(g + 1) * 128]
            for i in range(per):
                r0 = (g * per + i) * w
                terms[r0:r0 + w, pl.ds(pl.multiple_of(f * 128, 128), 128)] = (both * keep[i]).astype(BF16)
        return 0
    lax.fori_loop(0, blk // w, place, 0)
    update = dot(terms[...], opmw_buf[...]) / count_buf[...]
    fresh = (zblk[...].reshape(side * r * w, pc).astype(F32) + update).astype(BF16)
    zsend[...] = fresh.reshape(side, r, w, pc)

    my_core = x // half
    for t in range(side):
        dst = y * 2 * side + (c * half + t // 2) * 2 + t % 2

        @pl.when(dst != me)
        def _():
            remote(zsend.at[t], zrows.at[x], s5.at[t], r5.at[x], dst).start()

        @pl.when(dst == me)
        def _():
            zrows[x] = zsend[t]
    for t in range(side):
        dst = y * 2 * side + (c * half + t // 2) * 2 + t % 2
        src = y * 2 * side + t * 2 + my_core

        @pl.when(dst != me)
        def _():
            remote(zsend.at[t], zrows.at[x], s5.at[t], r5.at[x], dst).wait_send()

        @pl.when(src != me)
        def _():
            remote(zsend.at[t], zrows.at[t], s5.at[t], r5.at[t], dst).wait_recv()
    for t in range(side):
        z_f[:, t * w:(t + 1) * w, :] = zrows[t].astype(F32)

    nh = r * heads
    msg[0, 0, :nh] = bias_rows(z_f, sb_ref, heads)
    for cp in exchange_all(inbox.at[0, :, :nh], lambda p: msg.at[0, 0, :nh], s6, r6):
        cp.wait()
    flat[...] = inbox[0, :, :nh].astype(F32).reshape(n * nh, res)
    gather_bias(False)
    maskb = (resm_ref[...].astype(F32) - 1.0) * 1e4
    triangle(z_f, bias, maskb, sq_ref, so_ref, heads)

    rr = r * r

    def pack(slot_id):
        for p in range(n):
            msg[slot_id, p, :rr] = jnp.concatenate([z_f[i, p * r:(p + 1) * r, :] for i in range(r)], axis=0).astype(BF16)

    def unpack(slot_id):
        flat[...] = inbox[slot_id, :, :rr].astype(F32).reshape(n * rr, pc)
        for i in range(r):
            z_f[i] = flat[pl.ds(i, res, stride=r), :]

    pack(1)
    rows_b = bias_rows(z_f, eb_ref, heads)
    for p in range(n):
        msg[1, p, rr:] = rows_b
    for cp in exchange_all(inbox.at[1], lambda p: msg.at[1, p], s7, r7):
        cp.wait()
    flat[...] = inbox[1, :, rr:].astype(F32).reshape(n * nh, res)
    gather_bias(True)
    unpack(1)
    triangle(z_f, bias, maskb, eq_ref, eo_ref, heads)
    pack(2)
    for cp in exchange_all(inbox.at[2, :, :rr], lambda p: msg.at[2, p, :rr], s8, r8):
        cp.wait()
    unpack(2)
    z_out[...] = z_f[...].astype(BF16)


def block_call(n, side, dims, ops):
    m, z = ops[0], ops[1]
    seq, ch, res = m.shape
    r, _, w, pc = z.shape
    mh, md, heads = dims
    width, e = mh * md, ops[11].shape[0] // 2
    blk = w * e
    vm, dma = pltpu.VMEM, pltpu.SemaphoreType.DMA
    assert r == heads and res == 128 and seq == 128 and pc == 128
    own = res // n
    buf = vm((side, half_of(side), blk, 2 * seq), BF16)
    tall = vm((seq, width, res), BF16)
    box = vm((3, n, 2 * r * r, pc), BF16)
    scratch = [vm((seq, res), F32), tall, vm((seq, res, width + 16), BF16), tall, tall, vm((seq, width, res), F32),
               vm((2, mh // 2, res, 2 * res), F32), vm((2, mh // 2, res, 2 * res), BF16), vm((2, mh // 2, 8, 2 * res), F32),
               vm((mh // 2, res, 2 * res), F32), vm((mh // 2, width, 2 * res), BF16), vm((n + 1, r * mh, res), BF16), vm((n * r * mh, res), F32),
               vm((ch, width), BF16), vm((ch, width), BF16),
               vm((3, width, res), F32), vm((n, 3, own, width), F32), vm((n, 3, own, width), F32), vm((2, own, width), F32), vm((2, n, own, width), F32),
               vm((width, res), F32), vm((seq, mh, res), F32), vm((seq, md, res), F32), vm((res * e, seq), F32),
               vm((side, blk, seq), BF16), vm((side, blk, seq), BF16), vm((side, r, w, pc), BF16), vm((e * e, pc), F32), vm((e * 128, pc), BF16),
               vm((w // 2 * w, pc), F32), vm((res, res), F32),
               buf, buf, vm((2, blk, blk // 2), F32), vm((blk, blk // 2), F32), vm((w // 2 * w, e * 128), BF16),
               vm((side, r, w, pc), BF16), vm((side, r, w, pc), BF16), vm((r, res, pc), F32),
               vm((heads, res, res), F32), box, box, vm((n * r * r, pc), F32),
               dma((n,)), dma((n,)), dma((side,)), dma((side,))] + [dma((n,))] * 8 + [
               dma((2, side)), dma((2, side)), dma((2, side, 2)), dma((2, side, 2)), dma((2, side, 2)), dma((2, side, 2)),
               dma, dma, dma((side,)), dma((side,))] + [dma((n,))] * 6
    return pl.pallas_call(
        functools.partial(block_kernel, n, side, dims),
        out_shape=[jax.ShapeDtypeStruct((seq, ch, res), BF16), jax.ShapeDtypeStruct((r, res, pc), BF16)],
        in_specs=[vmem()] * len(ops), out_specs=[vmem()] * 2, scratch_shapes=scratch,
        compiler_params=pltpu.CompilerParams(collective_id=0, has_side_effects=True, vmem_limit_bytes=63 * 1024 * 1024),
        name='evoformer_block')(*ops)


def half_of(side):
    return side // 2


def solution(mesh):
    n = mesh.shape['dap']
    side = math.isqrt(n // 2)
    assert 2 * side * side == n

    def block(msa, pair, mask_full, res_mask, row_bias_w, row_qkvg_w, row_out_w, col_query_w, col_kv_w, col_gate_w, col_out_w, opm_proj_w, opm_out_w, start_bias_w, start_qkvg_w, start_out_w, end_bias_w, end_qkvg_w, end_out_w):
        r, res, pc = pair.shape
        ch = msa.shape[-1]
        last = lambda weight: jnp.moveaxis(weight, 0, -1).reshape(-1, weight.shape[0])
        first = lambda weight: weight.reshape(-1, weight.shape[-1])
        ops = [msa.transpose(0, 2, 1), pair.reshape(r, side, res // side, pc), mask_full, res_mask[None],
               row_bias_w.T, last(row_qkvg_w), first(row_out_w), last(col_query_w), last(col_kv_w), last(col_gate_w), first(col_out_w),
               last(opm_proj_w), first(opm_out_w), start_bias_w.T, last(start_qkvg_w), first(start_out_w), end_bias_w.T, last(end_qkvg_w), first(end_out_w)]
        msa_out, pair_out = block_call(n, side, col_gate_w.shape[1:] + (start_bias_w.shape[-1],), ops)
        return msa_out.transpose(0, 2, 1), pair_out

    row_spec = P(('data', 'dap'), None, None)
    in_specs = (row_spec, row_spec, P('data', None), P('data')) + (P(),) * 15
    return jax.shard_map(block, mesh=mesh, in_specs=in_specs, out_specs=(row_spec, row_spec), check_vma=False)
```

```python
import functools
import math

import jax
import jax.numpy as jnp
from jax import lax
from jax.experimental import pallas as pl
from jax.experimental.pallas import tpu as pltpu
from jax.sharding import PartitionSpec as P

MESH = pl.DeviceIdType.MESH
F32 = jnp.float32
BF16 = jnp.bfloat16
NT = (((1,), (1,)), ((), ()))


def dot(a, b):
    return jnp.dot(a, b, preferred_element_type=F32)


def dot_nt(a, b):
    return lax.dot_general(a, b, NT, preferred_element_type=F32)


LOG2E = 1.4426950408889634
BLOCK = 16


def norm_cols(x):
    mean = jnp.mean(x, axis=0, keepdims=True)
    cen = x - mean
    var = jnp.mean(cen * cen, axis=0, keepdims=True)
    return (cen * lax.rsqrt(var + 1e-5)).astype(BF16)


def wide(ref, g):
    return jnp.concatenate([ref[g * BLOCK + u] for u in range(BLOCK)], axis=1)


def put(ref, g, value):
    res = ref.shape[-1]
    for u in range(BLOCK):
        ref[g * BLOCK + u] = value[:, u * res:(u + 1) * res]


def split_mask(hd):
    whole = jnp.float32(-1e4 * hd ** 0.5)
    high = whole.astype(BF16).astype(F32)
    mid = (whole - high).astype(BF16).astype(F32)
    return high, mid, whole - high - mid


def row_project(heads, hd, m_ref, mask_ref, wt_ref, q_buf, k_buf, v_buf, g_buf):
    seq, ch, res = m_ref.shape
    width = heads * hd
    terms = split_mask(hd)

    def step(g, _):
        proj = jnp.dot(wt_ref[...], norm_cols(wide(m_ref, g).astype(F32)), preferred_element_type=F32)
        put(q_buf, g, proj[:width].astype(BF16))
        put(v_buf, g, proj[2 * width:3 * width].astype(BF16))
        put(g_buf, g, proj[3 * width:].astype(BF16))
        for u in range(BLOCK):
            s = g * BLOCK + u
            off = 1.0 - mask_ref[pl.ds(s, 1), :]
            row = lax.broadcasted_iota(jnp.int32, (16, res), 0)
            extra = jnp.where(row == 0, terms[0], jnp.where(row == 1, terms[1], jnp.where(row == 2, terms[2], 0.0))) * off
            k_buf[s] = jnp.concatenate([proj[width:2 * width, u * res:(u + 1) * res], extra], axis=0).T.astype(BF16)
        return 0
    lax.fori_loop(0, seq // BLOCK, step, 0)


def row_attend(heads, hd, bias_ref, pick_ref, q_buf, k_buf, v_buf, att_buf, raw_buf, w_buf, den_buf):
    seq, width, res = q_buf.shape
    pairs = heads // 2
    scale = LOG2E * hd ** -0.5
    row = lax.broadcasted_iota(jnp.int32, (16, 2 * res), 0)
    ones = jnp.where(row < 3, 1.0, 0.0).astype(BF16)

    def logits(s, b):
        qt = q_buf[s]
        q2 = jnp.concatenate([qt, qt], axis=1)
        keys = k_buf[s]
        for p in range(pairs):
            raw_buf[b, p] = jnp.dot(keys, jnp.concatenate([q2 * pick_ref[p], ones], axis=0), preferred_element_type=F32)

    def weigh(b):
        for p in range(pairs):
            t = raw_buf[b, p] * scale + bias_ref[p]
            w = jnp.exp2(t - jnp.max(t, axis=0, keepdims=True))
            w_buf[b, p] = w.astype(BF16)
            den_buf[b, p] = jnp.broadcast_to(1.0 / jnp.sum(w, axis=0, keepdims=True), (8, 2 * res))

    def values(s, b):
        for p in range(pairs):
            lo = 2 * p * hd
            o = jnp.dot(v_buf[s, lo:lo + 2 * hd], w_buf[b, p], preferred_element_type=F32) * den_buf[b, p, 0:1]
            att_buf[s, lo:lo + hd] = o[:hd, :res]
            att_buf[s, lo + hd:lo + 2 * hd] = o[hd:, res:]

    logits(0, 0)
    logits(1, 1)
    weigh(0)

    def step(t, _):
        s = 2 * t
        logits(jnp.minimum(s + 2, seq - 1), 0)
        weigh(1)
        values(s, 0)
        logits(jnp.minimum(s + 3, seq - 1), 1)
        weigh(0)
        values(s + 1, 1)
        return 0
    lax.fori_loop(0, seq // 2, step, 0)


def row_finish(m_ref, mask_ref, wo_ref, g_buf, att_buf, new_ref, ln_ref):
    seq, ch, res = m_ref.shape

    def step(g, total):
        y = (jax.nn.sigmoid(wide(g_buf, g).astype(F32)) * wide(att_buf, g)).astype(BF16)
        new = (wide(m_ref, g).astype(F32) + jnp.dot(wo_ref[...], y, preferred_element_type=F32)).astype(BF16)
        put(new_ref, g, new)
        ln = norm_cols(new.astype(F32))
        put(ln_ref, g, ln)
        for u in range(BLOCK):
            total += ln[:, u * res:(u + 1) * res].astype(F32) * mask_ref[pl.ds(g * BLOCK + u, 1), :]
        return total
    return lax.fori_loop(0, seq // BLOCK, step, jnp.zeros((ch, res), F32))


def col_sums(query, ln_ref, mask_ref, wkv_ref, logit_buf, val_buf):
    seq, ch, res = ln_ref.shape
    hd, heads = len(query), query[0].shape[0]
    scale = hd ** -0.5

    def first(g, top):
        kv = jnp.dot(wkv_ref[...], wide(ln_ref, g), preferred_element_type=F32).astype(BF16).astype(F32)
        for u in range(BLOCK):
            s = g * BLOCK + u
            k = kv[:hd, u * res:(u + 1) * res]
            logit = query[0] * k[0:1]
            for d in range(1, hd):
                logit += query[d] * k[d:d + 1]
            logit = logit * scale + (mask_ref[pl.ds(s, 1), :] - 1.0) * 1e4
            logit_buf[s] = logit
            val_buf[s] = kv[hd:, u * res:(u + 1) * res]
            top = jnp.maximum(top, logit)
        return top
    top = lax.fori_loop(0, seq // BLOCK, first, jnp.full((heads, res), -jnp.inf, F32))

    def second(g, carry):
        den, acc = carry
        acc = list(acc)
        for u in range(BLOCK):
            s = g * BLOCK + u
            w = jnp.exp(logit_buf[s] - top)
            den = den + w
            wb = w.astype(BF16).astype(F32)
            val = val_buf[s]
            for d in range(hd):
                acc[d] = acc[d] + wb * val[d:d + 1]
        return den, tuple(acc)
    zero = jnp.zeros((heads, res), F32)
    den, acc = lax.fori_loop(0, seq // BLOCK, second, (zero, (zero,) * hd))
    return acc, top, den


def col_finish(att, m_ref, ln_ref, mask_ref, wg_ref, wo_ref, wp_ref, out_ref, proj_ref):
    seq, ch, res = m_ref.shape

    def step(g, _):
        tiled = jnp.concatenate([att] * BLOCK, axis=1)
        gate = jnp.dot(wg_ref[...], wide(ln_ref, g), preferred_element_type=F32).astype(BF16).astype(F32)
        y = (jax.nn.sigmoid(gate) * tiled).astype(BF16)
        new = (wide(m_ref, g).astype(F32) + jnp.dot(wo_ref[...], y, preferred_element_type=F32)).astype(BF16)
        put(out_ref, g, new)
        proj = jnp.dot(wp_ref[...], norm_cols(new.astype(F32)), preferred_element_type=F32).astype(BF16)
        for u in range(BLOCK):
            s = g * BLOCK + u
            proj_ref[s] = (proj[:, u * res:(u + 1) * res].astype(F32) * mask_ref[pl.ds(s, 1), :]).astype(proj_ref.dtype)
        return 0
    lax.fori_loop(0, seq // BLOCK, step, 0)


def remote(src, dst, send_sem, recv_sem, dev):
    return pltpu.make_async_remote_copy(src_ref=src, dst_ref=dst, send_sem=send_sem, recv_sem=recv_sem,
                                        device_id={'dap': dev}, device_id_type=MESH)


def vmem():
    return pl.BlockSpec(memory_space=pltpu.VMEM)


def position(me, side):
    return me // (2 * side), (me // 2) % side, me % 2


def rows_to_block(me, side, rows_ref, block_ref, send_sem, recv_sem):
    y, x, c = position(me, side)
    half = side // 2
    slot = (x % half) * 2 + c
    core = x // half
    for t in range(side):
        dst = y * 2 * side + t * 2 + core

        @pl.when(dst != me)
        def _():
            remote(rows_ref.at[:, t], block_ref.at[slot], send_sem.at[t], recv_sem.at[slot], dst).start()

        @pl.when(dst == me)
        def _():
            block_ref[slot] = rows_ref[:, t]


def rows_to_block_wait(me, side, rows_ref, block_ref, send_sem, recv_sem):
    y, x, c = position(me, side)
    half = side // 2
    core = x // half
    for t in range(side):
        dst = y * 2 * side + t * 2 + core
        src = y * 2 * side + (c * half + t // 2) * 2 + t % 2

        @pl.when(dst != me)
        def _():
            remote(rows_ref.at[:, t], block_ref.at[t], send_sem.at[t], recv_sem.at[t], dst).wait_send()

        @pl.when(src != me)
        def _():
            remote(rows_ref.at[:, 0], block_ref.at[t], send_sem.at[t], recv_sem.at[t], dst).wait_recv()


def norm_rows(x):
    mean = jnp.mean(x, axis=-1, keepdims=True)
    cen = x - mean
    var = jnp.mean(cen * cen, axis=-1, keepdims=True)
    return (cen * lax.rsqrt(var + 1e-5)).astype(BF16)


def triangle(z_ref, bias_ref, maskb, qkvg_ref, out_w_ref, heads):
    rows, res, ch = z_ref.shape
    width = qkvg_ref.shape[0] // 4
    hd = width // heads
    lane_head = lax.broadcasted_iota(jnp.int32, (res, width), 1) // hd
    picks = [(lane_head == h).astype(F32) for h in range(heads)]
    pick_bf = jnp.concatenate(picks, axis=0).astype(BF16)
    bias = bias_ref[...].reshape(heads * res, res) + maskb
    projs = [dot_nt(norm_rows(z_ref[i]), qkvg_ref[...]) for i in range(rows)]
    raws = []
    for i in range(rows):
        q = projs[i][:, :width].astype(BF16)
        k = projs[i][:, width:2 * width].astype(BF16)
        raws.append(lax.dot_general(jnp.concatenate([q] * heads, axis=0) * pick_bf, k, (((1,), (1,)), ((), ())), preferred_element_type=F32))
    outs = []
    for i in range(rows):
        t = raws[i] * hd ** -0.5 + bias
        w = jnp.exp(t - jnp.max(t, axis=-1, keepdims=True))
        den = 1.0 / jnp.sum(w, axis=-1, keepdims=True)
        v = projs[i][:, 2 * width:3 * width].astype(BF16)
        outs.append(jnp.dot(w.astype(BF16), v, preferred_element_type=F32) * den)
    for i in range(rows):
        att = outs[i][:res] * picks[0]
        for h in range(1, heads):
            att += outs[i][h * res:(h + 1) * res] * picks[h]
        gate = projs[i][:, 3 * width:].astype(BF16).astype(F32)
        y = (jax.nn.sigmoid(gate) * att).astype(BF16)
        z_ref[i] = (z_ref[i] + jnp.dot(y, out_w_ref[...], preferred_element_type=F32)).astype(BF16).astype(F32)


def bias_rows(z_f, wb_ref, heads):
    parts = [dot_nt(wb_ref[...], norm_rows(z_f[i]))[:heads] for i in range(z_f.shape[0])]
    return jnp.concatenate(parts, axis=0).astype(BF16)


def combine_sum(got):
    return jnp.sum(got[:, 0], axis=0)


def combine_softmax(got):
    acc, top, den = got[:, 0], got[:, 1], got[:, 2]
    scale = jnp.exp(top - jnp.max(top, axis=0, keepdims=True))
    return jnp.sum(acc * scale, axis=0) / jnp.sum(den * scale, axis=0)


def block_kernel(n, side, dims, m_hbm, z_ref, mask_hbm, resm_ref, rb_ref, rw_ref, ro_ref, cq_ref, ckv_ref, cg_ref, co_ref, op_ref, ow_hbm,
                 sb_ref, sq_hbm, so_ref, eb_ref, eq_hbm, eo_ref, m_out, z_out,
                 m_ref, mask_ref, ow_ref, sq_ref, eq_ref, load_sem,
                 smask, q_buf, k_buf, v_buf, g_buf, att_buf, raw_buf, w_buf, den_buf, rbias, pick, rbox, rflat, wt_row, wt_col,
                 part, cut, got1, mine, back, small, logit_buf, val_buf, a_f32, a_send, c_send, zblk, opm_f32, opmw_buf, count_buf, pairs_buf,
                 a_buf, c_buf, acc, got, terms, zsend, zrows, z_f, bias, msg, inbox, flat,
                 sa, ra, sb, rb, sc1, rc1, sc2, rc2, sd1, rd1, sd2, rd2,
                 s1, r1, s2, r2, s3, r3, s4, r4, s5, r5, s6, r6, s7, r7, s8, r8):
    mh, md, heads = dims
    me = lax.axis_index('dap')
    y, x, c = position(me, side)
    half = side // 2
    seq, ch, res = m_ref.shape
    r, _, w, pc = z_ref.shape
    blk = a_buf.shape[2]
    width = mh * md
    e = op_ref.shape[0] // 2

    def dev(yy, xx, cc):
        return (yy * side + xx) * 2 + cc

    def exchange_all(box, src_of, send_sem, recv_sem):
        copies = []
        for k in range(1, n):
            dst = lax.rem(me + k, n)
            cp = remote(src_of(dst), box.at[me], send_sem.at[k], recv_sem.at[k], dst)
            cp.start()
            copies.append(cp)
        box[me] = src_of(me)[...]
        return copies

    barrier = pltpu.get_barrier_semaphore()
    for k in range(1, n):
        pl.semaphore_signal(barrier, inc=1, device_id={'dap': lax.rem(me + k, n)}, device_id_type=MESH)
    loads = [pltpu.make_async_copy(src, dst, load_sem.at[i]) for i, (src, dst) in enumerate(
        [(m_hbm, m_ref), (mask_hbm, mask_ref), (ow_hbm, ow_ref), (sq_hbm, sq_ref), (eq_hbm, eq_ref)])]
    for load in loads:
        load.start()

    for i in range(r):
        for t in range(side):
            z_f[i, t * w:(t + 1) * w, :] = z_ref[i, t].astype(F32)
    rmsg = rbox.at[n]
    rmsg[...] = bias_rows(z_f, rb_ref, mh)
    pl.semaphore_wait(barrier, n - 1)
    gathers = exchange_all(rbox, lambda p: rmsg, sa, ra)
    rows_to_block(me, side, z_ref, zblk, sb, rb)

    loads[0].wait()
    loads[1].wait()
    smask[...] = mask_ref[pl.ds(pl.multiple_of(me * seq, seq), seq), :].astype(F32)
    wt_row[...] = ro_ref[...].astype(F32).T.astype(BF16)
    wt_col[...] = co_ref[...].astype(F32).T.astype(BF16)
    row_id = lax.broadcasted_iota(jnp.int32, (width, 2 * res), 0) // md
    lane_id = lax.broadcasted_iota(jnp.int32, (width, 2 * res), 1) // res
    for p in range(mh // 2):
        pick[p] = jnp.where(row_id == 2 * p + lane_id, 1.0, 0.0).astype(BF16)
    row_project(mh, md, m_ref, smask, rw_ref, q_buf, k_buf, v_buf, g_buf)

    for cp in gathers:
        cp.wait()
    rflat[...] = rbox[:n].astype(F32).reshape(n * r * mh, res)
    for h in range(mh):
        rbias[h // 2, :, (h % 2) * res:(h % 2 + 1) * res] = rflat[pl.ds(h, res, stride=mh), :].T * LOG2E
    row_attend(mh, md, rbias, pick, q_buf, k_buf, v_buf, att_buf, raw_buf, w_buf, den_buf)
    new_buf, ln_buf, last_buf = q_buf, v_buf, g_buf
    part[0] = row_finish(m_ref, smask, wt_row, g_buf, att_buf, new_buf, ln_buf)

    def all_reduce(terms_n, combine, send1, recv1, send2, recv2):
        own = res // n
        for t in range(terms_n):
            turned = part[t].T
            for p in range(n):
                cut[p, t] = turned[p * own:(p + 1) * own]
        copies = []
        for k in range(1, n):
            dst = lax.rem(me + k, n)
            cp = remote(cut.at[dst, :terms_n], got1.at[me, :terms_n], send1.at[k], recv1.at[k], dst)
            cp.start()
            copies.append(cp)
        got1[me, :terms_n] = cut[me, :terms_n]
        for cp in copies:
            cp.wait()
        total = combine(got1[...])
        slot_id = 0 if terms_n == 1 else 1
        mine[slot_id] = total
        back[slot_id, me] = total
        copies = []
        for k in range(1, n):
            cp = remote(mine.at[slot_id], back.at[slot_id, me], send2.at[k], recv2.at[k], lax.rem(me + k, n))
            cp.start()
            copies.append(cp)
        for cp in copies:
            cp.wait()
        return jnp.concatenate([back[slot_id, p] for p in range(n)], axis=0).T

    count = jnp.sum(mask_ref[...].astype(F32), axis=0, keepdims=True) + 1e-10
    qsum = all_reduce(1, combine_sum, sc1, rc1, sc2, rc2)
    small[...] = dot(cq_ref[...], (qsum / count).astype(BF16)).astype(BF16).astype(F32)
    query = [small[pl.ds(d, mh, stride=md), :] for d in range(md)]
    sums, top, den = col_sums(query, ln_buf, smask, ckv_ref, logit_buf, val_buf)
    for d in range(md):
        part[0, pl.ds(d, mh, stride=md), :] = sums[d]
        part[1, pl.ds(d, mh, stride=md), :] = top
        part[2, pl.ds(d, mh, stride=md), :] = den
    attended = all_reduce(3, combine_softmax, sd1, rd1, sd2, rd2)
    proj = att_buf
    col_finish(attended, new_buf, ln_buf, smask, cg_ref, wt_col, op_ref, last_buf, proj)
    store = pltpu.make_async_copy(last_buf, m_out, load_sem.at[len(loads)])
    store.start()
    for load in loads[2:]:
        load.wait()

    planes = proj.reshape(seq * 2 * e, res)

    eye = jnp.where(lax.broadcasted_iota(jnp.int32, (res, res), 0) == lax.broadcasted_iota(jnp.int32, (res, res), 1), 1.0, 0.0).astype(BF16)

    def turned(t):
        return dot_nt(eye, planes[pl.ds(t, seq, stride=2 * e), :].astype(BF16))

    def turn_a(t, _):
        for u in range(4):
            a_f32[pl.ds(4 * t + u, res, stride=e), :] = turned(4 * t + u)
        return 0

    def turn_c(t, _):
        for u in range(4):
            f = 4 * t + u
            other = turned(e + f).astype(BF16)
            for b in range(side):
                c_send[b, pl.ds(pl.multiple_of(f * w, w), w), :] = other[b * w:(b + 1) * w]
        return 0
    def count_pairs():
        step = seq

        def add(t, _):
            rows = mask_ref[pl.ds(pl.multiple_of(t * step, step), step), :].astype(F32)
            pairs_buf[...] += dot(rows.T.astype(BF16), rows.astype(BF16))
            return 0
        pairs_buf[...] = jnp.zeros_like(pairs_buf)
        lax.fori_loop(0, mask_ref.shape[0] // step, add, 0)
        size = (w // 2 * w, res)
        row = lax.broadcasted_iota(jnp.int32, size, 0)
        lane = lax.broadcasted_iota(jnp.int32, size, 1)
        pick_i = jnp.where(lane == y * w + c * (w // 2) + row // w, 1.0, 0.0).astype(BF16)
        whole = pairs_buf[...]
        high = jnp.floor(whole * (1.0 / 128.0))
        both = dot(pick_i, high.astype(BF16)) * 128.0 + dot(pick_i, (whole - high * 128.0).astype(BF16))
        one = jnp.sum(jnp.where(lane == x * w + row % w, both, 0.0), axis=1, keepdims=True)
        count_buf[...] = jnp.broadcast_to(1e-3 + one, size)
        opm_f32[...] = ow_ref[...].astype(F32)
        for f in range(e):
            rows_f = opm_f32[pl.ds(f, e, stride=e), :].astype(BF16)
            for i in range(128 // e):
                opmw_buf[(f * (128 // e) + i) * e:(f * (128 // e) + i + 1) * e, :] = rows_f

    def gather_bias(turned):
        for h in range(heads):
            plane = flat[pl.ds(h, res, stride=heads), :]
            bias[h] = plane.T if turned else plane

    places = {0: (0, 0), 1: (0, 1), side - 1: (1, 0), 2: (1, 1)}

    def slot(buf, k, l, rows=None):
        pair_id, part_id = places[l]
        return buf.at[k, pair_id, pl.ds(0, blk) if rows is None else rows, pl.ds(part_id * seq, seq)]

    order = [0, 1, side - 1, 2]
    assert side == len(order)
    xn, yn = [lax.rem(x + 1, side), lax.rem(x + side - 1, side)], [lax.rem(y + 1, side), lax.rem(y + side - 1, side)]
    back_by = [1, side - 1]
    halves = [pl.ds(0, blk // 2), pl.ds(blk // 2, blk // 2)]
    first, hop, passed = [{}, {}], {}, {}

    def send_first(which):
        for k in order[1:]:
            ty, tx = lax.rem(y + k, side), lax.rem(x + k, side)
            if which == 0:
                cp = remote(a_send.at[ty], slot(a_buf, k, 0), s1.at[0, k], r1.at[0, k], dev(ty, x, c))
            else:
                cp = remote(c_send.at[tx], slot(c_buf, 0, k), s1.at[1, k], r1.at[1, k], dev(y, tx, c))
            cp.start()
            first[which][k] = cp

    def spread(which, k):
        for d in range(2):
            if which == 0:
                cp = remote(a_send.at[y] if k == 0 else slot(a_buf, k, 0), slot(a_buf, k, back_by[d]), s2.at[0, k, d], r2.at[0, k, d], dev(y, xn[d], c))
            else:
                cp = remote(c_send.at[x] if k == 0 else slot(c_buf, 0, k), slot(c_buf, back_by[d], k), s2.at[1, k, d], r2.at[1, k, d], dev(yn[d], x, c))
            cp.start()
            hop[which, k, d] = cp

    def relay(k):
        for d in range(2):
            hop[0, k, d].wait_recv()
            f = remote(slot(a_buf, k, back_by[d], halves[d]), slot(a_buf, k, 2, halves[d]), s3.at[0, k, d], r3.at[0, k, d], dev(y, xn[d], c))
            f.start()
            hop[1, k, d].wait_recv()
            g = remote(slot(c_buf, back_by[d], k, halves[d]), slot(c_buf, 2, k, halves[d]), s3.at[1, k, d], r3.at[1, k, d], dev(yn[d], x, c))
            g.start()
            passed[k, d] = (f, g)

    def wait_passed(k):
        for d in range(2):
            for f in passed[k, d]:
                f.wait_recv()

    cols = blk // 2

    def product(chunk, dst_id, fresh=False):
        k, p = chunk
        base = jnp.where(dst_id == 0, 1 - c, c) * cols
        part_sum = dot_nt(c_buf[k, p], a_buf[k, p, pl.ds(pl.multiple_of(base, cols), cols), :])
        if fresh:
            acc[dst_id] = part_sum
        else:
            acc[dst_id] += part_sum

    def products(chunk, fresh=False):
        product(chunk, 0, fresh)
        product(chunk, 1, fresh)

    lax.fori_loop(0, e // 4, turn_a, 0)
    for b in range(side):
        a_send[b] = a_f32[b * blk:(b + 1) * blk].astype(BF16)
    send_first(0)
    spread(0, 0)
    lax.fori_loop(0, e // 4, turn_c, 0)
    send_first(1)
    spread(1, 0)
    a_buf[0, 0, :, :seq] = a_send[y]
    c_buf[0, 0, :, :seq] = c_send[x]
    rows_to_block_wait(me, side, z_ref, zblk, sb, rb)
    count_pairs()
    one, three, two = order[1:]
    first[0][one].wait_recv()
    first[1][one].wait_recv()
    spread(0, one)
    spread(1, one)
    relay(0)
    first[0][three].wait_recv()
    first[1][three].wait_recv()
    spread(0, three)
    spread(1, three)
    relay(one)
    products((0, 0), True)
    first[0][two].wait_recv()
    first[1][two].wait_recv()
    spread(0, two)
    spread(1, two)
    products((one, 0))
    relay(three)
    products((three, 0))
    wait_passed(0)
    products((0, 1))
    relay(two)
    wait_passed(one)
    products((two, 0))
    rest = [(one, 1), (three, 1), (two, 1)]
    wait_passed(three)
    wait_passed(two)
    for chunk in rest:
        product(chunk, 0)
    swap = remote(acc.at[0], got, s4, r4, dev(y, x, 1 - c))
    swap.start()
    for chunk in rest:
        product(chunk, 1)
    for k in order[1:]:
        first[0][k].wait_send()
        first[1][k].wait_send()
    for cp in hop.values():
        cp.wait_send()
    for pair in passed.values():
        for f in pair:
            f.wait_send()
    swap.wait()

    per = 128 // e
    lane_i = lax.broadcasted_iota(jnp.int32, (w, 128), 1) // e
    keep = [(lane_i == i).astype(F32) for i in range(per)]

    def place(f, _):
        for g in range(cols // 128):
            rows = pl.ds(pl.multiple_of(f * w, w), w)
            both = acc[1, rows, g * 128:(g + 1) * 128] + got[rows, g * 128:(g + 1) * 128]
            for i in range(per):
                r0 = (g * per + i) * w
                terms[r0:r0 + w, pl.ds(pl.multiple_of(f * 128, 128), 128)] = (both * keep[i]).astype(BF16)
        return 0
    lax.fori_loop(0, blk // w, place, 0)
    update = dot(terms[...], opmw_buf[...]) / count_buf[...]
    fresh = (zblk[...].reshape(side * r * w, pc).astype(F32) + update).astype(BF16)
    zsend[...] = fresh.reshape(side, r, w, pc)

    my_core = x // half
    for t in range(side):
        dst = y * 2 * side + (c * half + t // 2) * 2 + t % 2

        @pl.when(dst != me)
        def _():
            remote(zsend.at[t], zrows.at[x], s5.at[t], r5.at[x], dst).start()

        @pl.when(dst == me)
        def _():
            zrows[x] = zsend[t]
    for t in range(side):
        dst = y * 2 * side + (c * half + t // 2) * 2 + t % 2
        src = y * 2 * side + t * 2 + my_core

        @pl.when(dst != me)
        def _():
            remote(zsend.at[t], zrows.at[x], s5.at[t], r5.at[x], dst).wait_send()

        @pl.when(src != me)
        def _():
            remote(zsend.at[t], zrows.at[t], s5.at[t], r5.at[t], dst).wait_recv()
    for t in range(side):
        z_f[:, t * w:(t + 1) * w, :] = zrows[t].astype(F32)

    nh = r * heads
    msg[0, 0, :nh] = bias_rows(z_f, sb_ref, heads)
    for cp in exchange_all(inbox.at[0, :, :nh], lambda p: msg.at[0, 0, :nh], s6, r6):
        cp.wait()
    flat[...] = inbox[0, :, :nh].astype(F32).reshape(n * nh, res)
    gather_bias(False)
    maskb = (resm_ref[...].astype(F32) - 1.0) * 1e4
    triangle(z_f, bias, maskb, sq_ref, so_ref, heads)

    rr = r * r

    def pack(slot_id):
        for p in range(n):
            msg[slot_id, p, :rr] = jnp.concatenate([z_f[i, p * r:(p + 1) * r, :] for i in range(r)], axis=0).astype(BF16)

    def unpack(slot_id):
        flat[...] = inbox[slot_id, :, :rr].astype(F32).reshape(n * rr, pc)
        for i in range(r):
            z_f[i] = flat[pl.ds(i, res, stride=r), :]

    pack(1)
    rows_b = bias_rows(z_f, eb_ref, heads)
    for p in range(n):
        msg[1, p, rr:] = rows_b
    for cp in exchange_all(inbox.at[1], lambda p: msg.at[1, p], s7, r7):
        cp.wait()
    flat[...] = inbox[1, :, rr:].astype(F32).reshape(n * nh, res)
    gather_bias(True)
    unpack(1)
    triangle(z_f, bias, maskb, eq_ref, eo_ref, heads)
    pack(2)
    for cp in exchange_all(inbox.at[2, :, :rr], lambda p: msg.at[2, p, :rr], s8, r8):
        cp.wait()
    unpack(2)
    z_out[...] = z_f[...].astype(BF16)
    store.wait()


def block_call(n, side, dims, ops):
    m, z = ops[0], ops[1]
    seq, ch, res = m.shape
    r, _, w, pc = z.shape
    mh, md, heads = dims
    width, e = mh * md, ops[11].shape[0] // 2
    blk = w * e
    vm, dma = pltpu.VMEM, pltpu.SemaphoreType.DMA
    assert r == heads and res == 128 and seq == 128 and pc == 128
    own = res // n
    buf = vm((side, half_of(side), blk, 2 * seq), BF16)
    tall = vm((seq, width, res), BF16)
    box = vm((3, n, 2 * r * r, pc), BF16)
    large = [0, 2, 12, 14, 17]
    scratch = [vm(ops[i].shape, ops[i].dtype) for i in large] + [dma((len(large) + 1,))]
    scratch += [vm((seq, res), F32), tall, vm((seq, res, width + 16), BF16), tall, tall, vm((seq, width, res), F32),
               vm((2, mh // 2, res, 2 * res), F32), vm((2, mh // 2, res, 2 * res), BF16), vm((2, mh // 2, 8, 2 * res), F32),
               vm((mh // 2, res, 2 * res), F32), vm((mh // 2, width, 2 * res), BF16), vm((n + 1, r * mh, res), BF16), vm((n * r * mh, res), F32),
               vm((ch, width), BF16), vm((ch, width), BF16),
               vm((3, width, res), F32), vm((n, 3, own, width), F32), vm((n, 3, own, width), F32), vm((2, own, width), F32), vm((2, n, own, width), F32),
               vm((width, res), F32), vm((seq, mh, res), F32), vm((seq, md, res), F32), vm((res * e, seq), F32),
               vm((side, blk, seq), BF16), vm((side, blk, seq), BF16), vm((side, r, w, pc), BF16), vm((e * e, pc), F32), vm((e * 128, pc), BF16),
               vm((w // 2 * w, pc), F32), vm((res, res), F32),
               buf, buf, vm((2, blk, blk // 2), F32), vm((blk, blk // 2), F32), vm((w // 2 * w, e * 128), BF16),
               vm((side, r, w, pc), BF16), vm((side, r, w, pc), BF16), vm((r, res, pc), F32),
               vm((heads, res, res), F32), box, box, vm((n * r * r, pc), F32),
               dma((n,)), dma((n,)), dma((side,)), dma((side,))] + [dma((n,))] * 8 + [
               dma((2, side)), dma((2, side)), dma((2, side, 2)), dma((2, side, 2)), dma((2, side, 2)), dma((2, side, 2)),
               dma, dma, dma((side,)), dma((side,))] + [dma((n,))] * 6
    return pl.pallas_call(
        functools.partial(block_kernel, n, side, dims),
        out_shape=[jax.ShapeDtypeStruct((seq, ch, res), BF16), jax.ShapeDtypeStruct((r, res, pc), BF16)],
        in_specs=[pl.BlockSpec(memory_space=pl.ANY) if i in large else vmem() for i in range(len(ops))],
        out_specs=[pl.BlockSpec(memory_space=pl.ANY), vmem()], scratch_shapes=scratch,
        compiler_params=pltpu.CompilerParams(collective_id=0, has_side_effects=True, vmem_limit_bytes=63 * 1024 * 1024),
        name='evoformer_block')(*ops)


def half_of(side):
    return side // 2


def solution(mesh):
    n = mesh.shape['dap']
    side = math.isqrt(n // 2)
    assert 2 * side * side == n

    def block(msa, pair, mask_full, res_mask, row_bias_w, row_qkvg_w, row_out_w, col_query_w, col_kv_w, col_gate_w, col_out_w, opm_proj_w, opm_out_w, start_bias_w, start_qkvg_w, start_out_w, end_bias_w, end_qkvg_w, end_out_w):
        r, res, pc = pair.shape
        ch = msa.shape[-1]
        last = lambda weight: jnp.moveaxis(weight, 0, -1).reshape(-1, weight.shape[0])
        first = lambda weight: weight.reshape(-1, weight.shape[-1])
        ops = [msa.transpose(0, 2, 1), pair.reshape(r, side, res // side, pc), mask_full, res_mask[None],
               row_bias_w.T, last(row_qkvg_w), first(row_out_w), last(col_query_w), last(col_kv_w), last(col_gate_w), first(col_out_w),
               last(opm_proj_w), first(opm_out_w), start_bias_w.T, last(start_qkvg_w), first(start_out_w), end_bias_w.T, last(end_qkvg_w), first(end_out_w)]
        msa_out, pair_out = block_call(n, side, col_gate_w.shape[1:] + (start_bias_w.shape[-1],), ops)
        return msa_out.transpose(0, 2, 1), pair_out

    row_spec = P(('data', 'dap'), None, None)
    in_specs = (row_spec, row_spec, P('data', None), P('data')) + (P(),) * 15
    return jax.shard_map(block, mesh=mesh, in_specs=in_specs, out_specs=(row_spec, row_spec), check_vma=False)
```

```python
import functools
import math

import jax
import jax.numpy as jnp
from jax import lax
from jax.experimental import pallas as pl
from jax.experimental.pallas import tpu as pltpu
from jax.sharding import PartitionSpec as P

MESH = pl.DeviceIdType.MESH
F32 = jnp.float32
BF16 = jnp.bfloat16
NT = (((1,), (1,)), ((), ()))


def dot(a, b):
    return jnp.dot(a, b, preferred_element_type=F32)


def dot_nt(a, b):
    return lax.dot_general(a, b, NT, preferred_element_type=F32)


LOG2E = 1.4426950408889634
BLOCK = 16


def norm_cols(x):
    mean = jnp.mean(x, axis=0, keepdims=True)
    cen = x - mean
    var = jnp.mean(cen * cen, axis=0, keepdims=True)
    return (cen * lax.rsqrt(var + 1e-5)).astype(BF16)


def wide(ref, g):
    return jnp.concatenate([ref[g * BLOCK + u] for u in range(BLOCK)], axis=1)


def put(ref, g, value):
    res = ref.shape[-1]
    for u in range(BLOCK):
        ref[g * BLOCK + u] = value[:, u * res:(u + 1) * res]


def split_mask(hd):
    whole = jnp.float32(-1e4 * hd ** 0.5)
    high = whole.astype(BF16).astype(F32)
    mid = (whole - high).astype(BF16).astype(F32)
    return high, mid, whole - high - mid


def row_project(heads, hd, m_ref, mask_ref, wt_ref, q_buf, k_buf, v_buf, g_buf):
    seq, ch, res = m_ref.shape
    width = heads * hd
    terms = split_mask(hd)

    def step(g, _):
        proj = jnp.dot(wt_ref[...], norm_cols(wide(m_ref, g).astype(F32)), preferred_element_type=F32)
        put(q_buf, g, proj[:width].astype(BF16))
        put(v_buf, g, proj[2 * width:3 * width].astype(BF16))
        put(g_buf, g, proj[3 * width:].astype(BF16))
        for u in range(BLOCK):
            s = g * BLOCK + u
            off = 1.0 - mask_ref[pl.ds(s, 1), :]
            row = lax.broadcasted_iota(jnp.int32, (16, res), 0)
            extra = jnp.where(row == 0, terms[0], jnp.where(row == 1, terms[1], jnp.where(row == 2, terms[2], 0.0))) * off
            k_buf[s] = jnp.concatenate([proj[width:2 * width, u * res:(u + 1) * res], extra], axis=0).T.astype(BF16)
        return 0
    lax.fori_loop(0, seq // BLOCK, step, 0)


def row_attend(heads, hd, bias_ref, pick_ref, q_buf, k_buf, v_buf, att_buf, raw_buf, w_buf, den_buf):
    seq, width, res = q_buf.shape
    pairs = heads // 2
    scale = LOG2E * hd ** -0.5
    row = lax.broadcasted_iota(jnp.int32, (16, 2 * res), 0)
    ones = jnp.where(row < 3, 1.0, 0.0).astype(BF16)

    def logits(s, b, p):
        qt = q_buf[s]
        q2 = jnp.concatenate([qt, qt], axis=1)
        raw_buf[b, p] = jnp.dot(k_buf[s], jnp.concatenate([q2 * pick_ref[p], ones], axis=0), preferred_element_type=F32)

    def weigh(b, p):
        t = raw_buf[b, p] * scale + bias_ref[p]
        w = jnp.exp2(t - jnp.max(t, axis=0, keepdims=True))
        w_buf[b, p] = w.astype(BF16)
        den_buf[b, p] = jnp.broadcast_to(1.0 / jnp.sum(w, axis=0, keepdims=True), (8, 2 * res))

    def values(s, b, p):
        lo = 2 * p * hd
        o = jnp.dot(v_buf[s, lo:lo + 2 * hd], w_buf[b, p], preferred_element_type=F32) * den_buf[b, p, 0:1]
        att_buf[s, lo:lo + hd] = o[:hd, :res]
        att_buf[s, lo + hd:lo + 2 * hd] = o[hd:, res:]

    for p in range(pairs):
        logits(0, 0, p)
    for p in range(pairs):
        logits(1, 1, p)
        weigh(0, p)

    def step(t, _):
        for u in range(4):
            s = 4 * t + u
            for p in range(pairs):
                logits(jnp.minimum(s + 2, seq - 1), u % 2, p)
                weigh((u + 1) % 2, p)
                values(s, u % 2, p)
        return 0
    lax.fori_loop(0, seq // 4, step, 0)


def row_finish(m_ref, mask_ref, wo_ref, g_buf, att_buf, new_ref, ln_ref):
    seq, ch, res = m_ref.shape

    def step(g, total):
        y = (jax.nn.sigmoid(wide(g_buf, g).astype(F32)) * wide(att_buf, g)).astype(BF16)
        new = (wide(m_ref, g).astype(F32) + jnp.dot(wo_ref[...], y, preferred_element_type=F32)).astype(BF16)
        put(new_ref, g, new)
        ln = norm_cols(new.astype(F32))
        put(ln_ref, g, ln)
        for u in range(BLOCK):
            total += ln[:, u * res:(u + 1) * res].astype(F32) * mask_ref[pl.ds(g * BLOCK + u, 1), :]
        return total
    return lax.fori_loop(0, seq // BLOCK, step, jnp.zeros((ch, res), F32))


def col_project(ln_ref, wkv_ref, key_buf, val_buf):
    seq, ch, res = ln_ref.shape
    hd = key_buf.shape[1]

    def step(g, _):
        kv = jnp.dot(wkv_ref[...], wide(ln_ref, g), preferred_element_type=F32).astype(BF16).astype(F32)
        put(key_buf, g, kv[:hd])
        put(val_buf, g, kv[hd:])
        return 0
    lax.fori_loop(0, seq // BLOCK, step, 0)


def col_gates(ln_ref, wg_ref, gate_buf):
    seq, ch, res = ln_ref.shape

    def step(g, _):
        gate = jnp.dot(wg_ref[...], wide(ln_ref, g), preferred_element_type=F32).astype(BF16).astype(F32)
        put(gate_buf, g, jax.nn.sigmoid(gate))
        return 0
    lax.fori_loop(0, seq // BLOCK, step, 0)


def col_sums(query, mask_ref, key_buf, val_buf):
    seq, hd, res = val_buf.shape
    heads = query[0].shape[0]
    scale = hd ** -0.5

    def first(g, top):
        for u in range(BLOCK):
            s = g * BLOCK + u
            k = key_buf[s]
            logit = query[0] * k[0:1]
            for d in range(1, hd):
                logit += query[d] * k[d:d + 1]
            logit = logit * scale + (mask_ref[pl.ds(s, 1), :] - 1.0) * 1e4
            key_buf[s] = logit
            top = jnp.maximum(top, logit)
        return top
    top = lax.fori_loop(0, seq // BLOCK, first, jnp.full((heads, res), -jnp.inf, F32))

    def second(g, carry):
        den, acc = carry
        acc = list(acc)
        for u in range(BLOCK):
            s = g * BLOCK + u
            w = jnp.exp(key_buf[s] - top)
            den = den + w
            wb = w.astype(BF16).astype(F32)
            val = val_buf[s]
            for d in range(hd):
                acc[d] = acc[d] + wb * val[d:d + 1]
        return den, tuple(acc)
    zero = jnp.zeros((heads, res), F32)
    den, acc = lax.fori_loop(0, seq // BLOCK, second, (zero, (zero,) * hd))
    return acc, top, den


def col_finish(att, m_ref, mask_ref, wo_ref, wp_ref, out_ref, proj_ref):
    seq, ch, res = m_ref.shape

    def step(g, _):
        tiled = jnp.concatenate([att] * BLOCK, axis=1)
        y = (wide(proj_ref, g) * tiled).astype(BF16)
        new = (wide(m_ref, g).astype(F32) + jnp.dot(wo_ref[...], y, preferred_element_type=F32)).astype(BF16)
        put(out_ref, g, new)
        proj = jnp.dot(wp_ref[...], norm_cols(new.astype(F32)), preferred_element_type=F32).astype(BF16)
        for u in range(BLOCK):
            s = g * BLOCK + u
            proj_ref[s] = (proj[:, u * res:(u + 1) * res].astype(F32) * mask_ref[pl.ds(s, 1), :]).astype(proj_ref.dtype)
        return 0
    lax.fori_loop(0, seq // BLOCK, step, 0)


def remote(src, dst, send_sem, recv_sem, dev):
    return pltpu.make_async_remote_copy(src_ref=src, dst_ref=dst, send_sem=send_sem, recv_sem=recv_sem,
                                        device_id={'dap': dev}, device_id_type=MESH)


def vmem():
    return pl.BlockSpec(memory_space=pltpu.VMEM)


def position(me, side):
    return me // (2 * side), (me // 2) % side, me % 2


def rows_to_block(me, side, rows_ref, block_ref, send_sem, recv_sem):
    y, x, c = position(me, side)
    half = side // 2
    slot = (x % half) * 2 + c
    core = x // half
    for t in range(side):
        dst = y * 2 * side + t * 2 + core

        @pl.when(dst != me)
        def _():
            remote(rows_ref.at[:, t], block_ref.at[slot], send_sem.at[t], recv_sem.at[slot], dst).start()

        @pl.when(dst == me)
        def _():
            block_ref[slot] = rows_ref[:, t]


def rows_to_block_wait(me, side, rows_ref, block_ref, send_sem, recv_sem):
    y, x, c = position(me, side)
    half = side // 2
    core = x // half
    for t in range(side):
        dst = y * 2 * side + t * 2 + core
        src = y * 2 * side + (c * half + t // 2) * 2 + t % 2

        @pl.when(dst != me)
        def _():
            remote(rows_ref.at[:, t], block_ref.at[t], send_sem.at[t], recv_sem.at[t], dst).wait_send()

        @pl.when(src != me)
        def _():
            remote(rows_ref.at[:, 0], block_ref.at[t], send_sem.at[t], recv_sem.at[t], dst).wait_recv()


def norm_rows(x):
    mean = jnp.mean(x, axis=-1, keepdims=True)
    cen = x - mean
    var = jnp.mean(cen * cen, axis=-1, keepdims=True)
    return (cen * lax.rsqrt(var + 1e-5)).astype(BF16)


def triangle(z_ref, bias_ref, maskb, qkvg_ref, out_w_ref, heads):
    rows, res, ch = z_ref.shape
    width = qkvg_ref.shape[0] // 4
    hd = width // heads
    lane_head = lax.broadcasted_iota(jnp.int32, (res, width), 1) // hd
    picks = [(lane_head == h).astype(F32) for h in range(heads)]
    pick_bf = jnp.concatenate(picks, axis=0).astype(BF16)
    bias = bias_ref[...].reshape(heads * res, res) + maskb
    projs = [dot_nt(norm_rows(z_ref[i]), qkvg_ref[...]) for i in range(rows)]
    raws = []
    for i in range(rows):
        q = projs[i][:, :width].astype(BF16)
        k = projs[i][:, width:2 * width].astype(BF16)
        raws.append(lax.dot_general(jnp.concatenate([q] * heads, axis=0) * pick_bf, k, (((1,), (1,)), ((), ())), preferred_element_type=F32))
    outs = []
    for i in range(rows):
        t = raws[i] * hd ** -0.5 + bias
        w = jnp.exp(t - jnp.max(t, axis=-1, keepdims=True))
        den = 1.0 / jnp.sum(w, axis=-1, keepdims=True)
        v = projs[i][:, 2 * width:3 * width].astype(BF16)
        outs.append(jnp.dot(w.astype(BF16), v, preferred_element_type=F32) * den)
    for i in range(rows):
        att = outs[i][:res] * picks[0]
        for h in range(1, heads):
            att += outs[i][h * res:(h + 1) * res] * picks[h]
        gate = projs[i][:, 3 * width:].astype(BF16).astype(F32)
        y = (jax.nn.sigmoid(gate) * att).astype(BF16)
        z_ref[i] = (z_ref[i] + jnp.dot(y, out_w_ref[...], preferred_element_type=F32)).astype(BF16).astype(F32)


def bias_rows(z_f, wb_ref, heads):
    parts = [dot_nt(wb_ref[...], norm_rows(z_f[i]))[:heads] for i in range(z_f.shape[0])]
    return jnp.concatenate(parts, axis=0).astype(BF16)


def combine_sum(got):
    return jnp.sum(got[:, 0], axis=0)


def combine_softmax(got):
    acc, top, den = got[:, 0], got[:, 1], got[:, 2]
    scale = jnp.exp(top - jnp.max(top, axis=0, keepdims=True))
    return jnp.sum(acc * scale, axis=0) / jnp.sum(den * scale, axis=0)


def block_kernel(n, side, dims, m_hbm, z_ref, mask_hbm, resm_ref, rb_ref, rw_ref, ro_ref, cq_ref, ckv_ref, cg_ref, co_ref, op_ref, ow_hbm,
                 sb_ref, sq_hbm, so_ref, eb_ref, eq_hbm, eo_ref, m_out, z_out,
                 m_ref, mask_ref, ow_ref, sq_ref, eq_ref, load_sem,
                 smask, q_buf, k_buf, v_buf, g_buf, att_buf, raw_buf, w_buf, den_buf, rbias, pick, rbox, rflat, wt_row, wt_col,
                 part, cut, got1, mine, back, small, logit_buf, val_buf, a_f32, a_send, c_send, zblk, opm_f32, opmw_buf, count_buf, pairs_buf,
                 a_buf, c_buf, acc, got, terms, zsend, zrows, z_f, bias, msg, inbox, flat,
                 sa, ra, sb, rb, sc1, rc1, sc2, rc2, sd1, rd1, sd2, rd2,
                 s1, r1, s2, r2, s3, r3, s4, r4, s5, r5, s6, r6, s7, r7, s8, r8):
    mh, md, heads = dims
    me = lax.axis_index('dap')
    y, x, c = position(me, side)
    half = side // 2
    seq, ch, res = m_ref.shape
    r, _, w, pc = z_ref.shape
    blk = a_buf.shape[2]
    width = mh * md
    e = op_ref.shape[0] // 2

    def dev(yy, xx, cc):
        return (yy * side + xx) * 2 + cc

    def exchange_all(box, src_of, send_sem, recv_sem):
        copies = []
        for k in range(1, n):
            dst = lax.rem(me + k, n)
            cp = remote(src_of(dst), box.at[me], send_sem.at[k], recv_sem.at[k], dst)
            cp.start()
            copies.append(cp)
        box[me] = src_of(me)[...]
        return copies

    barrier = pltpu.get_barrier_semaphore()
    for k in range(1, n):
        pl.semaphore_signal(barrier, inc=1, device_id={'dap': lax.rem(me + k, n)}, device_id_type=MESH)
    loads = [pltpu.make_async_copy(src, dst, load_sem.at[i]) for i, (src, dst) in enumerate(
        [(m_hbm, m_ref), (mask_hbm, mask_ref), (ow_hbm, ow_ref), (sq_hbm, sq_ref), (eq_hbm, eq_ref)])]
    for load in loads:
        load.start()

    for i in range(r):
        for t in range(side):
            z_f[i, t * w:(t + 1) * w, :] = z_ref[i, t].astype(F32)
    rmsg = rbox.at[n]
    rmsg[...] = bias_rows(z_f, rb_ref, mh)
    pl.semaphore_wait(barrier, n - 1)
    gathers = exchange_all(rbox, lambda p: rmsg, sa, ra)
    rows_to_block(me, side, z_ref, zblk, sb, rb)

    loads[0].wait()
    loads[1].wait()
    smask[...] = mask_ref[pl.ds(pl.multiple_of(me * seq, seq), seq), :].astype(F32)
    wt_row[...] = ro_ref[...].astype(F32).T.astype(BF16)
    wt_col[...] = co_ref[...].astype(F32).T.astype(BF16)
    row_id = lax.broadcasted_iota(jnp.int32, (width, 2 * res), 0) // md
    lane_id = lax.broadcasted_iota(jnp.int32, (width, 2 * res), 1) // res
    for p in range(mh // 2):
        pick[p] = jnp.where(row_id == 2 * p + lane_id, 1.0, 0.0).astype(BF16)
    row_project(mh, md, m_ref, smask, rw_ref, q_buf, k_buf, v_buf, g_buf)

    for cp in gathers:
        cp.wait()
    rflat[...] = rbox[:n].astype(F32).reshape(n * r * mh, res)
    for h in range(mh):
        rbias[h // 2, :, (h % 2) * res:(h % 2 + 1) * res] = rflat[pl.ds(h, res, stride=mh), :].T * LOG2E
    row_attend(mh, md, rbias, pick, q_buf, k_buf, v_buf, att_buf, raw_buf, w_buf, den_buf)
    new_buf, ln_buf, last_buf = q_buf, v_buf, g_buf
    part[0] = row_finish(m_ref, smask, wt_row, g_buf, att_buf, new_buf, ln_buf)

    def all_reduce(terms_n, combine, send1, recv1, send2, recv2, beside1, beside2):
        own = res // n
        for t in range(terms_n):
            turned = part[t].T
            for p in range(n):
                cut[p, t] = turned[p * own:(p + 1) * own]
        copies = []
        for k in range(1, n):
            dst = lax.rem(me + k, n)
            cp = remote(cut.at[dst, :terms_n], got1.at[me, :terms_n], send1.at[k], recv1.at[k], dst)
            cp.start()
            copies.append(cp)
        got1[me, :terms_n] = cut[me, :terms_n]
        beside1()
        for cp in copies:
            cp.wait()
        total = combine(got1[...])
        slot_id = 0 if terms_n == 1 else 1
        mine[slot_id] = total
        back[slot_id, me] = total
        copies = []
        for k in range(1, n):
            cp = remote(mine.at[slot_id], back.at[slot_id, me], send2.at[k], recv2.at[k], lax.rem(me + k, n))
            cp.start()
            copies.append(cp)
        beside2()
        for cp in copies:
            cp.wait()
        return jnp.concatenate([back[slot_id, p] for p in range(n)], axis=0).T

    def count_pairs():
        step = seq

        def add(t, _):
            rows = mask_ref[pl.ds(pl.multiple_of(t * step, step), step), :].astype(F32)
            pairs_buf[...] += dot(rows.T.astype(BF16), rows.astype(BF16))
            return 0
        pairs_buf[...] = jnp.zeros_like(pairs_buf)
        lax.fori_loop(0, mask_ref.shape[0] // step, add, 0)
        size = (w // 2 * w, res)
        row = lax.broadcasted_iota(jnp.int32, size, 0)
        lane = lax.broadcasted_iota(jnp.int32, size, 1)
        pick_i = jnp.where(lane == y * w + c * (w // 2) + row // w, 1.0, 0.0).astype(BF16)
        whole = pairs_buf[...]
        high = jnp.floor(whole * (1.0 / 128.0))
        both = dot(pick_i, high.astype(BF16)) * 128.0 + dot(pick_i, (whole - high * 128.0).astype(BF16))
        one = jnp.sum(jnp.where(lane == x * w + row % w, both, 0.0), axis=1, keepdims=True)
        count_buf[...] = jnp.broadcast_to(1e-3 + one, size)
        opm_f32[...] = ow_ref[...].astype(F32)
        for f in range(e):
            rows_f = opm_f32[pl.ds(f, e, stride=e), :].astype(BF16)
            for i in range(128 // e):
                opmw_buf[(f * (128 // e) + i) * e:(f * (128 // e) + i + 1) * e, :] = rows_f

    for load in loads[2:]:
        load.wait()
    proj = att_buf
    count = []

    def project():
        count.append(jnp.sum(mask_ref[...].astype(F32), axis=0, keepdims=True) + 1e-10)
        col_project(ln_buf, ckv_ref, logit_buf, val_buf)

    qsum = all_reduce(1, combine_sum, sc1, rc1, sc2, rc2, project, lambda: col_gates(ln_buf, cg_ref, proj))
    small[...] = dot(cq_ref[...], (qsum / count[0]).astype(BF16)).astype(BF16).astype(F32)
    query = [small[pl.ds(d, mh, stride=md), :] for d in range(md)]
    sums, top, den = col_sums(query, smask, logit_buf, val_buf)
    for d in range(md):
        part[0, pl.ds(d, mh, stride=md), :] = sums[d]
        part[1, pl.ds(d, mh, stride=md), :] = top
        part[2, pl.ds(d, mh, stride=md), :] = den
    attended = all_reduce(3, combine_softmax, sd1, rd1, sd2, rd2, count_pairs, lambda: None)
    col_finish(attended, new_buf, smask, wt_col, op_ref, last_buf, proj)
    store = pltpu.make_async_copy(last_buf, m_out, load_sem.at[len(loads)])
    store.start()

    planes = proj.reshape(seq * 2 * e, res)

    eye = jnp.where(lax.broadcasted_iota(jnp.int32, (res, res), 0) == lax.broadcasted_iota(jnp.int32, (res, res), 1), 1.0, 0.0).astype(BF16)

    def turned(t):
        return dot_nt(eye, planes[pl.ds(t, seq, stride=2 * e), :].astype(BF16))

    def turn_a(t, _):
        for u in range(4):
            a_f32[pl.ds(4 * t + u, res, stride=e), :] = turned(4 * t + u)
        return 0

    def turn_c(t, _):
        for u in range(4):
            f = 4 * t + u
            other = turned(e + f).astype(BF16)
            for b in range(side):
                c_send[b, pl.ds(pl.multiple_of(f * w, w), w), :] = other[b * w:(b + 1) * w]
        return 0
    def gather_bias(turned):
        for h in range(heads):
            plane = flat[pl.ds(h, res, stride=heads), :]
            bias[h] = plane.T if turned else plane

    places = {0: (0, 0), 1: (0, 1), side - 1: (1, 0), 2: (1, 1)}

    def slot(buf, k, l, rows=None):
        pair_id, part_id = places[l]
        return buf.at[k, pair_id, pl.ds(0, blk) if rows is None else rows, pl.ds(part_id * seq, seq)]

    order = [0, 1, side - 1, 2]
    assert side == len(order)
    xn, yn = [lax.rem(x + 1, side), lax.rem(x + side - 1, side)], [lax.rem(y + 1, side), lax.rem(y + side - 1, side)]
    back_by = [1, side - 1]
    halves = [pl.ds(0, blk // 2), pl.ds(blk // 2, blk // 2)]
    first, hop, passed = [{}, {}], {}, {}

    def send_first(which):
        for k in order[1:]:
            ty, tx = lax.rem(y + k, side), lax.rem(x + k, side)
            if which == 0:
                cp = remote(a_send.at[ty], slot(a_buf, k, 0), s1.at[0, k], r1.at[0, k], dev(ty, x, c))
            else:
                cp = remote(c_send.at[tx], slot(c_buf, 0, k), s1.at[1, k], r1.at[1, k], dev(y, tx, c))
            cp.start()
            first[which][k] = cp

    def spread(which, k):
        for d in range(2):
            if which == 0:
                cp = remote(a_send.at[y] if k == 0 else slot(a_buf, k, 0), slot(a_buf, k, back_by[d]), s2.at[0, k, d], r2.at[0, k, d], dev(y, xn[d], c))
            else:
                cp = remote(c_send.at[x] if k == 0 else slot(c_buf, 0, k), slot(c_buf, back_by[d], k), s2.at[1, k, d], r2.at[1, k, d], dev(yn[d], x, c))
            cp.start()
            hop[which, k, d] = cp

    def relay(k):
        for d in range(2):
            hop[0, k, d].wait_recv()
            f = remote(slot(a_buf, k, back_by[d], halves[d]), slot(a_buf, k, 2, halves[d]), s3.at[0, k, d], r3.at[0, k, d], dev(y, xn[d], c))
            f.start()
            hop[1, k, d].wait_recv()
            g = remote(slot(c_buf, back_by[d], k, halves[d]), slot(c_buf, 2, k, halves[d]), s3.at[1, k, d], r3.at[1, k, d], dev(yn[d], x, c))
            g.start()
            passed[k, d] = (f, g)

    def wait_passed(k):
        for d in range(2):
            for f in passed[k, d]:
                f.wait_recv()

    cols = blk // 2

    def product(chunk, dst_id, fresh=False):
        k, p = chunk
        base = jnp.where(dst_id == 0, 1 - c, c) * cols
        part_sum = dot_nt(c_buf[k, p], a_buf[k, p, pl.ds(pl.multiple_of(base, cols), cols), :])
        if fresh:
            acc[dst_id] = part_sum
        else:
            acc[dst_id] += part_sum

    def products(chunk, fresh=False):
        product(chunk, 0, fresh)
        product(chunk, 1, fresh)

    lax.fori_loop(0, e // 4, turn_a, 0)
    for b in range(side):
        a_send[b] = a_f32[b * blk:(b + 1) * blk].astype(BF16)
    send_first(0)
    spread(0, 0)
    lax.fori_loop(0, e // 4, turn_c, 0)
    send_first(1)
    spread(1, 0)
    a_buf[0, 0, :, :seq] = a_send[y]
    c_buf[0, 0, :, :seq] = c_send[x]
    rows_to_block_wait(me, side, z_ref, zblk, sb, rb)
    one, three, two = order[1:]
    first[0][one].wait_recv()
    first[1][one].wait_recv()
    spread(0, one)
    spread(1, one)
    relay(0)
    first[0][three].wait_recv()
    first[1][three].wait_recv()
    spread(0, three)
    spread(1, three)
    relay(one)
    products((0, 0), True)
    first[0][two].wait_recv()
    first[1][two].wait_recv()
    spread(0, two)
    spread(1, two)
    products((one, 0))
    relay(three)
    products((three, 0))
    wait_passed(0)
    products((0, 1))
    relay(two)
    wait_passed(one)
    products((two, 0))
    rest = [(one, 1), (three, 1), (two, 1)]
    wait_passed(three)
    wait_passed(two)
    for chunk in rest:
        product(chunk, 0)
    swap = remote(acc.at[0], got, s4, r4, dev(y, x, 1 - c))
    swap.start()
    for chunk in rest:
        product(chunk, 1)
    for k in order[1:]:
        first[0][k].wait_send()
        first[1][k].wait_send()
    for cp in hop.values():
        cp.wait_send()
    for pair in passed.values():
        for f in pair:
            f.wait_send()
    swap.wait()

    per = 128 // e
    lane_i = lax.broadcasted_iota(jnp.int32, (w, 128), 1) // e
    keep = [(lane_i == i).astype(F32) for i in range(per)]

    def place(f, _):
        for g in range(cols // 128):
            rows = pl.ds(pl.multiple_of(f * w, w), w)
            both = acc[1, rows, g * 128:(g + 1) * 128] + got[rows, g * 128:(g + 1) * 128]
            for i in range(per):
                r0 = (g * per + i) * w
                terms[r0:r0 + w, pl.ds(pl.multiple_of(f * 128, 128), 128)] = (both * keep[i]).astype(BF16)
        return 0
    lax.fori_loop(0, blk // w, place, 0)
    update = dot(terms[...], opmw_buf[...]) / count_buf[...]
    fresh = (zblk[...].reshape(side * r * w, pc).astype(F32) + update).astype(BF16)
    zsend[...] = fresh.reshape(side, r, w, pc)

    nh = r * heads
    groups = (w // 2) * w // 128
    part_bias = dot_nt(sb_ref[...], norm_rows(fresh.astype(F32)))[:heads]
    msg[0, 0, :nh] = jnp.concatenate([part_bias[:, g * 128:(g + 1) * 128] for g in range(groups)], axis=0).astype(BF16)
    gathers = exchange_all(inbox.at[0, :, :nh], lambda p: msg.at[0, 0, :nh], s6, r6)
    my_core = x // half
    for t in range(side):
        dst = y * 2 * side + (c * half + t // 2) * 2 + t % 2

        @pl.when(dst != me)
        def _():
            remote(zsend.at[t], zrows.at[x], s5.at[t], r5.at[x], dst).start()

        @pl.when(dst == me)
        def _():
            zrows[x] = zsend[t]
    for t in range(side):
        dst = y * 2 * side + (c * half + t // 2) * 2 + t % 2
        src = y * 2 * side + t * 2 + my_core

        @pl.when(dst != me)
        def _():
            remote(zsend.at[t], zrows.at[x], s5.at[t], r5.at[x], dst).wait_send()

        @pl.when(src != me)
        def _():
            remote(zsend.at[t], zrows.at[t], s5.at[t], r5.at[t], dst).wait_recv()
    for t in range(side):
        z_f[:, t * w:(t + 1) * w, :] = zrows[t].astype(F32)

    for cp in gathers:
        cp.wait()
    flat[...] = inbox[0, :, :nh].astype(F32).reshape(n * nh, res)
    per_y = 2 * groups
    for yy in range(side):
        for h in range(heads):
            pieces = [flat[pl.ds((yy * side + xx) * per_y * heads + h, per_y, stride=heads), :] for xx in range(side)]
            for i in range(128 // w):
                bias[h, pl.ds(yy * w + i, per_y, stride=128 // w), :] = jnp.concatenate([piece[:, i * w:(i + 1) * w] for piece in pieces], axis=1)
    maskb = (resm_ref[...].astype(F32) - 1.0) * 1e4
    triangle(z_f, bias, maskb, sq_ref, so_ref, heads)

    rr = r * r

    def pack(slot_id):
        for p in range(n):
            msg[slot_id, p, :rr] = jnp.concatenate([z_f[i, p * r:(p + 1) * r, :] for i in range(r)], axis=0).astype(BF16)

    def unpack(slot_id):
        flat[...] = inbox[slot_id, :, :rr].astype(F32).reshape(n * rr, pc)
        for i in range(r):
            z_f[i] = flat[pl.ds(i, res, stride=r), :]

    pack(1)
    rows_b = bias_rows(z_f, eb_ref, heads)
    for p in range(n):
        msg[1, p, rr:] = rows_b
    for cp in exchange_all(inbox.at[1], lambda p: msg.at[1, p], s7, r7):
        cp.wait()
    flat[...] = inbox[1, :, rr:].astype(F32).reshape(n * nh, res)
    gather_bias(True)
    unpack(1)
    triangle(z_f, bias, maskb, eq_ref, eo_ref, heads)
    pack(2)
    for cp in exchange_all(inbox.at[2, :, :rr], lambda p: msg.at[2, p, :rr], s8, r8):
        cp.wait()
    unpack(2)
    z_out[...] = z_f[...].astype(BF16)
    store.wait()


def block_call(n, side, dims, ops):
    m, z = ops[0], ops[1]
    seq, ch, res = m.shape
    r, _, w, pc = z.shape
    mh, md, heads = dims
    width, e = mh * md, ops[11].shape[0] // 2
    blk = w * e
    vm, dma = pltpu.VMEM, pltpu.SemaphoreType.DMA
    assert r == heads and mh == md and res == 128 and seq == 128 and pc == 128
    own = res // n
    buf = vm((side, half_of(side), blk, 2 * seq), BF16)
    tall = vm((seq, width, res), BF16)
    box = vm((3, n, 2 * r * r, pc), BF16)
    large = [0, 2, 12, 14, 17]
    scratch = [vm(ops[i].shape, ops[i].dtype) for i in large] + [dma((len(large) + 1,))]
    scratch += [vm((seq, res), F32), tall, vm((seq, res, width + 16), BF16), tall, tall, vm((seq, width, res), F32),
               vm((2, mh // 2, res, 2 * res), F32), vm((2, mh // 2, res, 2 * res), BF16), vm((2, mh // 2, 8, 2 * res), F32),
               vm((mh // 2, res, 2 * res), F32), vm((mh // 2, width, 2 * res), BF16), vm((n + 1, r * mh, res), BF16), vm((n * r * mh, res), F32),
               vm((ch, width), BF16), vm((ch, width), BF16),
               vm((3, width, res), F32), vm((n, 3, own, width), F32), vm((n, 3, own, width), F32), vm((2, own, width), F32), vm((2, n, own, width), F32),
               vm((width, res), F32), vm((seq, mh, res), F32), vm((seq, md, res), F32), vm((res * e, seq), F32),
               vm((side, blk, seq), BF16), vm((side, blk, seq), BF16), vm((side, r, w, pc), BF16), vm((e * e, pc), F32), vm((e * 128, pc), BF16),
               vm((w // 2 * w, pc), F32), vm((res, res), F32),
               buf, buf, vm((2, blk, blk // 2), F32), vm((blk, blk // 2), F32), vm((w // 2 * w, e * 128), BF16),
               vm((side, r, w, pc), BF16), vm((side, r, w, pc), BF16), vm((r, res, pc), F32),
               vm((heads, res, res), F32), box, box, vm((n * r * r, pc), F32),
               dma((n,)), dma((n,)), dma((side,)), dma((side,))] + [dma((n,))] * 8 + [
               dma((2, side)), dma((2, side)), dma((2, side, 2)), dma((2, side, 2)), dma((2, side, 2)), dma((2, side, 2)),
               dma, dma, dma((side,)), dma((side,))] + [dma((n,))] * 6
    return pl.pallas_call(
        functools.partial(block_kernel, n, side, dims),
        out_shape=[jax.ShapeDtypeStruct((seq, ch, res), BF16), jax.ShapeDtypeStruct((r, res, pc), BF16)],
        in_specs=[pl.BlockSpec(memory_space=pl.ANY) if i in large else vmem() for i in range(len(ops))],
        out_specs=[pl.BlockSpec(memory_space=pl.ANY), vmem()], scratch_shapes=scratch,
        compiler_params=pltpu.CompilerParams(collective_id=0, has_side_effects=True, vmem_limit_bytes=63 * 1024 * 1024),
        name='evoformer_block')(*ops)


def half_of(side):
    return side // 2


def solution(mesh):
    n = mesh.shape['dap']
    side = math.isqrt(n // 2)
    assert 2 * side * side == n

    def block(msa, pair, mask_full, res_mask, row_bias_w, row_qkvg_w, row_out_w, col_query_w, col_kv_w, col_gate_w, col_out_w, opm_proj_w, opm_out_w, start_bias_w, start_qkvg_w, start_out_w, end_bias_w, end_qkvg_w, end_out_w):
        r, res, pc = pair.shape
        ch = msa.shape[-1]
        last = lambda weight: jnp.moveaxis(weight, 0, -1).reshape(-1, weight.shape[0])
        first = lambda weight: weight.reshape(-1, weight.shape[-1])
        ops = [msa.transpose(0, 2, 1), pair.reshape(r, side, res // side, pc), mask_full, res_mask[None],
               row_bias_w.T, last(row_qkvg_w), first(row_out_w), last(col_query_w), last(col_kv_w), last(col_gate_w), first(col_out_w),
               last(opm_proj_w), first(opm_out_w), start_bias_w.T, last(start_qkvg_w), first(start_out_w), end_bias_w.T, last(end_qkvg_w), first(end_out_w)]
        msa_out, pair_out = block_call(n, side, col_gate_w.shape[1:] + (start_bias_w.shape[-1],), ops)
        return msa_out.transpose(0, 2, 1), pair_out

    row_spec = P(('data', 'dap'), None, None)
    in_specs = (row_spec, row_spec, P('data', None), P('data')) + (P(),) * 15
    return jax.shard_map(block, mesh=mesh, in_specs=in_specs, out_specs=(row_spec, row_spec), check_vma=False)
```

```python
import functools
import math

import jax
import jax.numpy as jnp
from jax import lax
from jax.experimental import pallas as pl
from jax.experimental.pallas import tpu as pltpu
from jax.sharding import PartitionSpec as P

MESH = pl.DeviceIdType.MESH
F32 = jnp.float32
BF16 = jnp.bfloat16
NT = (((1,), (1,)), ((), ()))


def dot(a, b):
    return jnp.dot(a, b, preferred_element_type=F32)


def dot_nt(a, b):
    return lax.dot_general(a, b, NT, preferred_element_type=F32)


LOG2E = 1.4426950408889634
BLOCK = 16


def norm_cols(x):
    mean = jnp.mean(x, axis=0, keepdims=True)
    cen = x - mean
    var = jnp.mean(cen * cen, axis=0, keepdims=True)
    return (cen * lax.rsqrt(var + 1e-5)).astype(BF16)


def wide(ref, g):
    return jnp.concatenate([ref[g * BLOCK + u] for u in range(BLOCK)], axis=1)


def put(ref, g, value):
    res = ref.shape[-1]
    for u in range(BLOCK):
        ref[g * BLOCK + u] = value[:, u * res:(u + 1) * res]


def split_mask(hd):
    whole = jnp.float32(-1e4 * hd ** 0.5)
    high = whole.astype(BF16).astype(F32)
    mid = (whole - high).astype(BF16).astype(F32)
    return high, mid, whole - high - mid


def row_project(heads, hd, m_ref, mask_ref, wt_ref, q_buf, k_buf, v_buf, g_buf):
    seq, ch, res = m_ref.shape
    width = heads * hd
    terms = split_mask(hd)

    def step(g, _):
        proj = jnp.dot(wt_ref[...], norm_cols(wide(m_ref, g).astype(F32)), preferred_element_type=F32)
        put(q_buf, g, proj[:width].astype(BF16))
        put(v_buf, g, proj[2 * width:3 * width].astype(BF16))
        put(g_buf, g, proj[3 * width:].astype(BF16))
        for u in range(BLOCK):
            s = g * BLOCK + u
            off = 1.0 - mask_ref[pl.ds(s, 1), :]
            row = lax.broadcasted_iota(jnp.int32, (16, res), 0)
            extra = jnp.where(row == 0, terms[0], jnp.where(row == 1, terms[1], jnp.where(row == 2, terms[2], 0.0))) * off
            k_buf[s] = jnp.concatenate([proj[width:2 * width, u * res:(u + 1) * res], extra], axis=0).T.astype(BF16)
        return 0
    lax.fori_loop(0, seq // BLOCK, step, 0, unroll=2)


def row_attend(heads, hd, bias_ref, pick_ref, q_buf, k_buf, v_buf, att_buf, raw_buf, w_buf, den_buf):
    seq, width, res = q_buf.shape
    pairs = heads // 2
    scale = LOG2E * hd ** -0.5
    row = lax.broadcasted_iota(jnp.int32, (16, 2 * res), 0)
    ones = jnp.where(row < 3, 1.0, 0.0).astype(BF16)

    def logits(s, b, p):
        qt = q_buf[s]
        q2 = jnp.concatenate([qt, qt], axis=1)
        raw_buf[b, p] = jnp.dot(k_buf[s], jnp.concatenate([q2 * pick_ref[p], ones], axis=0), preferred_element_type=F32)

    def weigh(b, p):
        t = raw_buf[b, p] * scale + bias_ref[p]
        w = jnp.exp2(t - jnp.max(t, axis=0, keepdims=True))
        w_buf[b, p] = w.astype(BF16)
        den_buf[b, p] = jnp.broadcast_to(1.0 / jnp.sum(w, axis=0, keepdims=True), (8, 2 * res))

    def values(s, b, p):
        lo = 2 * p * hd
        o = jnp.dot(v_buf[s, lo:lo + 2 * hd], w_buf[b, p], preferred_element_type=F32) * den_buf[b, p, 0:1]
        att_buf[s, lo:lo + hd] = o[:hd, :res]
        att_buf[s, lo + hd:lo + 2 * hd] = o[hd:, res:]

    for p in range(pairs):
        logits(0, 0, p)
    for p in range(pairs):
        logits(1, 1, p)
        weigh(0, p)

    def step(t, _):
        for u in range(4):
            s = 4 * t + u
            for p in range(pairs):
                logits(jnp.minimum(s + 2, seq - 1), u % 2, p)
                weigh((u + 1) % 2, p)
                values(s, u % 2, p)
        return 0
    lax.fori_loop(0, seq // 4, step, 0)


def row_finish(m_ref, mask_ref, wo_ref, g_buf, att_buf, new_ref, ln_ref):
    seq, ch, res = m_ref.shape

    def step(g, total):
        y = (jax.nn.sigmoid(wide(g_buf, g).astype(F32)) * wide(att_buf, g)).astype(BF16)
        new = (wide(m_ref, g).astype(F32) + jnp.dot(wo_ref[...], y, preferred_element_type=F32)).astype(BF16)
        put(new_ref, g, new)
        ln = norm_cols(new.astype(F32))
        put(ln_ref, g, ln)
        for u in range(BLOCK):
            total += ln[:, u * res:(u + 1) * res].astype(F32) * mask_ref[pl.ds(g * BLOCK + u, 1), :]
        return total
    return lax.fori_loop(0, seq // BLOCK, step, jnp.zeros((ch, res), F32), unroll=2)


def col_project(ln_ref, wkv_ref, key_buf, val_buf):
    seq, ch, res = ln_ref.shape
    hd = key_buf.shape[1]

    def step(g, _):
        kv = jnp.dot(wkv_ref[...], wide(ln_ref, g), preferred_element_type=F32).astype(BF16).astype(F32)
        put(key_buf, g, kv[:hd])
        put(val_buf, g, kv[hd:])
        return 0
    lax.fori_loop(0, seq // BLOCK, step, 0, unroll=2)


def col_gates(ln_ref, wg_ref, gate_buf):
    seq, ch, res = ln_ref.shape

    def step(g, _):
        gate = jnp.dot(wg_ref[...], wide(ln_ref, g), preferred_element_type=F32).astype(BF16).astype(F32)
        put(gate_buf, g, jax.nn.sigmoid(gate))
        return 0
    lax.fori_loop(0, seq // BLOCK, step, 0, unroll=2)


def col_sums(query, mask_ref, key_buf, val_buf):
    seq, hd, res = val_buf.shape
    heads = query[0].shape[0]
    scale = hd ** -0.5

    def first(g, top):
        for u in range(BLOCK):
            s = g * BLOCK + u
            k = key_buf[s]
            logit = query[0] * k[0:1]
            for d in range(1, hd):
                logit += query[d] * k[d:d + 1]
            logit = logit * scale + (mask_ref[pl.ds(s, 1), :] - 1.0) * 1e4
            key_buf[s] = logit
            top = jnp.maximum(top, logit)
        return top
    top = lax.fori_loop(0, seq // BLOCK, first, jnp.full((heads, res), -jnp.inf, F32))

    def second(g, carry):
        den, acc = carry
        acc = list(acc)
        for u in range(BLOCK):
            s = g * BLOCK + u
            w = jnp.exp(key_buf[s] - top)
            den = den + w
            wb = w.astype(BF16).astype(F32)
            val = val_buf[s]
            for d in range(hd):
                acc[d] = acc[d] + wb * val[d:d + 1]
        return den, tuple(acc)
    zero = jnp.zeros((heads, res), F32)
    den, acc = lax.fori_loop(0, seq // BLOCK, second, (zero, (zero,) * hd))
    return acc, top, den


def col_finish(att, m_ref, mask_ref, wo_ref, wp_ref, out_ref, proj_ref):
    seq, ch, res = m_ref.shape

    def step(g, _):
        tiled = jnp.concatenate([att] * BLOCK, axis=1)
        y = (wide(proj_ref, g) * tiled).astype(BF16)
        new = (wide(m_ref, g).astype(F32) + jnp.dot(wo_ref[...], y, preferred_element_type=F32)).astype(BF16)
        put(out_ref, g, new)
        proj = jnp.dot(wp_ref[...], norm_cols(new.astype(F32)), preferred_element_type=F32).astype(BF16)
        for u in range(BLOCK):
            s = g * BLOCK + u
            proj_ref[s] = (proj[:, u * res:(u + 1) * res].astype(F32) * mask_ref[pl.ds(s, 1), :]).astype(proj_ref.dtype)
        return 0
    lax.fori_loop(0, seq // BLOCK, step, 0, unroll=2)


def remote(src, dst, send_sem, recv_sem, dev):
    return pltpu.make_async_remote_copy(src_ref=src, dst_ref=dst, send_sem=send_sem, recv_sem=recv_sem,
                                        device_id={'dap': dev}, device_id_type=MESH)


def vmem():
    return pl.BlockSpec(memory_space=pltpu.VMEM)


def position(me, side):
    return me // (2 * side), (me // 2) % side, me % 2


def rows_to_block(me, side, rows_ref, block_ref, send_sem, recv_sem):
    y, x, c = position(me, side)
    half = side // 2
    slot = (x % half) * 2 + c
    core = x // half
    for t in range(side):
        dst = y * 2 * side + t * 2 + core

        @pl.when(dst != me)
        def _():
            remote(rows_ref.at[:, t], block_ref.at[slot], send_sem.at[t], recv_sem.at[slot], dst).start()

        @pl.when(dst == me)
        def _():
            block_ref[slot] = rows_ref[:, t]


def rows_to_block_wait(me, side, rows_ref, block_ref, send_sem, recv_sem):
    y, x, c = position(me, side)
    half = side // 2
    core = x // half
    for t in range(side):
        dst = y * 2 * side + t * 2 + core
        src = y * 2 * side + (c * half + t // 2) * 2 + t % 2

        @pl.when(dst != me)
        def _():
            remote(rows_ref.at[:, t], block_ref.at[t], send_sem.at[t], recv_sem.at[t], dst).wait_send()

        @pl.when(src != me)
        def _():
            remote(rows_ref.at[:, 0], block_ref.at[t], send_sem.at[t], recv_sem.at[t], dst).wait_recv()


def norm_rows(x):
    mean = jnp.mean(x, axis=-1, keepdims=True)
    cen = x - mean
    var = jnp.mean(cen * cen, axis=-1, keepdims=True)
    return (cen * lax.rsqrt(var + 1e-5)).astype(BF16)


def triangle(z_ref, bias_ref, maskb, qkvg_ref, out_w_ref, heads):
    rows, res, ch = z_ref.shape
    width = qkvg_ref.shape[0] // 4
    hd = width // heads
    lane_head = lax.broadcasted_iota(jnp.int32, (res, width), 1) // hd
    picks = [(lane_head == h).astype(F32) for h in range(heads)]
    pick_bf = jnp.concatenate(picks, axis=0).astype(BF16)
    bias = bias_ref[...].reshape(heads * res, res) + maskb
    projs = [dot_nt(norm_rows(z_ref[i]), qkvg_ref[...]) for i in range(rows)]
    raws = []
    for i in range(rows):
        q = projs[i][:, :width].astype(BF16)
        k = projs[i][:, width:2 * width].astype(BF16)
        raws.append(lax.dot_general(jnp.concatenate([q] * heads, axis=0) * pick_bf, k, (((1,), (1,)), ((), ())), preferred_element_type=F32))
    outs = []
    for i in range(rows):
        t = raws[i] * hd ** -0.5 + bias
        w = jnp.exp(t - jnp.max(t, axis=-1, keepdims=True))
        den = 1.0 / jnp.sum(w, axis=-1, keepdims=True)
        v = projs[i][:, 2 * width:3 * width].astype(BF16)
        outs.append(jnp.dot(w.astype(BF16), v, preferred_element_type=F32) * den)
    for i in range(rows):
        att = outs[i][:res] * picks[0]
        for h in range(1, heads):
            att += outs[i][h * res:(h + 1) * res] * picks[h]
        gate = projs[i][:, 3 * width:].astype(BF16).astype(F32)
        y = (jax.nn.sigmoid(gate) * att).astype(BF16)
        z_ref[i] = (z_ref[i] + jnp.dot(y, out_w_ref[...], preferred_element_type=F32)).astype(BF16).astype(F32)


def bias_rows(z_f, wb_ref, heads):
    parts = [dot_nt(wb_ref[...], norm_rows(z_f[i]))[:heads] for i in range(z_f.shape[0])]
    return jnp.concatenate(parts, axis=0).astype(BF16)


def combine_sum(got):
    return jnp.sum(got[:, 0], axis=0)


def combine_softmax(got):
    acc, top, den = got[:, 0], got[:, 1], got[:, 2]
    scale = jnp.exp(top - jnp.max(top, axis=0, keepdims=True))
    return jnp.sum(acc * scale, axis=0) / jnp.sum(den * scale, axis=0)


def block_kernel(n, side, dims, n_ops, *refs):
    operands, (m_out, z_out), loaded, load_sem, rest = refs[:n_ops], refs[n_ops:n_ops + 2], refs[n_ops + 2:2 * n_ops + 2], refs[2 * n_ops + 2], refs[2 * n_ops + 3:]
    m_ref, z_ref, mask_ref, resm_ref, rb_ref, rw_ref, ro_ref, cq_ref, ckv_ref, cg_ref, co_ref, op_ref, ow_ref, sb_ref, sq_ref, so_ref, eb_ref, eq_ref, eo_ref = loaded
    (
                 smask, q_buf, k_buf, v_buf, g_buf, att_buf, raw_buf, w_buf, den_buf, rbias, pick, rbox, rflat, wt_row, wt_col,
                 part, cut, got1, mine, back, small, logit_buf, val_buf, a_f32, a_send, c_send, zblk, opm_f32, opmw_buf, count_buf, pairs_buf,
                 a_buf, c_buf, acc, got, terms, zsend, zrows, z_f, bias, msg, inbox, flat,
                 sa, ra, sb, rb, sc1, rc1, sc2, rc2, sd1, rd1, sd2, rd2,
                 s1, r1, s2, r2, s3, r3, s4, r4, s5, r5, s6, r6, s7, r7, s8, r8) = rest
    mh, md, heads = dims
    me = lax.axis_index('dap')
    y, x, c = position(me, side)
    half = side // 2
    seq, ch, res = m_ref.shape
    r, _, w, pc = z_ref.shape
    blk = a_buf.shape[2]
    width = mh * md
    e = op_ref.shape[0] // 2

    def dev(yy, xx, cc):
        return (yy * side + xx) * 2 + cc

    def exchange_all(box, src_of, send_sem, recv_sem):
        copies = []
        for k in range(1, n):
            dst = lax.rem(me + k, n)
            cp = remote(src_of(dst), box.at[me], send_sem.at[k], recv_sem.at[k], dst)
            cp.start()
            copies.append(cp)
        box[me] = src_of(me)[...]
        return copies

    barrier = pltpu.get_barrier_semaphore()
    for k in range(1, n):
        pl.semaphore_signal(barrier, inc=1, device_id={'dap': lax.rem(me + k, n)}, device_id_type=MESH)
    loads = [pltpu.make_async_copy(src, dst, load_sem.at[i]) for i, (src, dst) in enumerate(zip(operands, loaded))]
    urgent = [1, 4]
    for i in urgent:
        loads[i].start()
    for i in range(n_ops):
        if i not in urgent:
            loads[i].start()
    for i in urgent:
        loads[i].wait()

    for i in range(r):
        for t in range(side):
            z_f[i, t * w:(t + 1) * w, :] = z_ref[i, t].astype(F32)
    rmsg = rbox.at[n]
    rmsg[...] = bias_rows(z_f, rb_ref, mh)
    pl.semaphore_wait(barrier, n - 1)
    gathers = exchange_all(rbox, lambda p: rmsg, sa, ra)
    rows_to_block(me, side, z_ref, zblk, sb, rb)

    for i in range(n_ops):
        if i not in urgent:
            loads[i].wait()
    smask[...] = mask_ref[pl.ds(pl.multiple_of(me * seq, seq), seq), :].astype(F32)
    wt_row[...] = ro_ref[...].astype(F32).T.astype(BF16)
    wt_col[...] = co_ref[...].astype(F32).T.astype(BF16)
    row_id = lax.broadcasted_iota(jnp.int32, (width, 2 * res), 0) // md
    lane_id = lax.broadcasted_iota(jnp.int32, (width, 2 * res), 1) // res
    for p in range(mh // 2):
        pick[p] = jnp.where(row_id == 2 * p + lane_id, 1.0, 0.0).astype(BF16)
    row_project(mh, md, m_ref, smask, rw_ref, q_buf, k_buf, v_buf, g_buf)

    for cp in gathers:
        cp.wait()
    rflat[...] = rbox[:n].astype(F32).reshape(n * r * mh, res)
    for h in range(mh):
        rbias[h // 2, :, (h % 2) * res:(h % 2 + 1) * res] = rflat[pl.ds(h, res, stride=mh), :].T * LOG2E
    row_attend(mh, md, rbias, pick, q_buf, k_buf, v_buf, att_buf, raw_buf, w_buf, den_buf)
    new_buf, ln_buf, last_buf = q_buf, v_buf, g_buf
    part[0] = row_finish(m_ref, smask, wt_row, g_buf, att_buf, new_buf, ln_buf)

    def all_reduce(terms_n, combine, send1, recv1, send2, recv2, beside1, beside2):
        own = res // n
        for t in range(terms_n):
            turned = part[t].T
            for p in range(n):
                cut[p, t] = turned[p * own:(p + 1) * own]
        copies = []
        for k in range(1, n):
            dst = lax.rem(me + k, n)
            cp = remote(cut.at[dst, :terms_n], got1.at[me, :terms_n], send1.at[k], recv1.at[k], dst)
            cp.start()
            copies.append(cp)
        got1[me, :terms_n] = cut[me, :terms_n]
        beside1()
        for cp in copies:
            cp.wait()
        total = combine(got1[...])
        slot_id = 0 if terms_n == 1 else 1
        mine[slot_id] = total
        back[slot_id, me] = total
        copies = []
        for k in range(1, n):
            cp = remote(mine.at[slot_id], back.at[slot_id, me], send2.at[k], recv2.at[k], lax.rem(me + k, n))
            cp.start()
            copies.append(cp)
        beside2()
        for cp in copies:
            cp.wait()
        return jnp.concatenate([back[slot_id, p] for p in range(n)], axis=0).T

    def count_pairs():
        step = seq

        def add(t, total):
            rows = mask_ref[pl.ds(pl.multiple_of(t * step, step), step), :].astype(F32)
            return total + dot(rows.T.astype(BF16), rows.astype(BF16))
        pairs_buf[...] = lax.fori_loop(0, mask_ref.shape[0] // step, add, jnp.zeros((res, res), F32), unroll=8)
        size = (w // 2 * w, res)
        row = lax.broadcasted_iota(jnp.int32, size, 0)
        lane = lax.broadcasted_iota(jnp.int32, size, 1)
        pick_i = jnp.where(lane == y * w + c * (w // 2) + row // w, 1.0, 0.0).astype(BF16)
        whole = pairs_buf[...]
        high = jnp.floor(whole * (1.0 / 128.0))
        both = dot(pick_i, high.astype(BF16)) * 128.0 + dot(pick_i, (whole - high * 128.0).astype(BF16))
        one = jnp.sum(jnp.where(lane == x * w + row % w, both, 0.0), axis=1, keepdims=True)
        count_buf[...] = jnp.broadcast_to(1e-3 + one, size)
        opm_f32[...] = ow_ref[...].astype(F32)
        for f in range(e):
            rows_f = opm_f32[pl.ds(f, e, stride=e), :].astype(BF16)
            for i in range(128 // e):
                opmw_buf[(f * (128 // e) + i) * e:(f * (128 // e) + i + 1) * e, :] = rows_f

    proj = att_buf
    count = []

    def project():
        count.append(jnp.sum(mask_ref[...].astype(F32), axis=0, keepdims=True) + 1e-10)
        col_project(ln_buf, ckv_ref, logit_buf, val_buf)

    qsum = all_reduce(1, combine_sum, sc1, rc1, sc2, rc2, project, lambda: col_gates(ln_buf, cg_ref, proj))
    small[...] = dot(cq_ref[...], (qsum / count[0]).astype(BF16)).astype(BF16).astype(F32)
    query = [small[pl.ds(d, mh, stride=md), :] for d in range(md)]
    sums, top, den = col_sums(query, smask, logit_buf, val_buf)
    for d in range(md):
        part[0, pl.ds(d, mh, stride=md), :] = sums[d]
        part[1, pl.ds(d, mh, stride=md), :] = top
        part[2, pl.ds(d, mh, stride=md), :] = den
    attended = all_reduce(3, combine_softmax, sd1, rd1, sd2, rd2, count_pairs, lambda: None)
    col_finish(attended, new_buf, smask, wt_col, op_ref, last_buf, proj)
    store = pltpu.make_async_copy(last_buf, m_out, load_sem.at[len(loads)])
    store.start()

    planes = proj.reshape(seq * 2 * e, res)

    eye = jnp.where(lax.broadcasted_iota(jnp.int32, (res, res), 0) == lax.broadcasted_iota(jnp.int32, (res, res), 1), 1.0, 0.0).astype(BF16)

    def turned(t):
        return dot_nt(eye, planes[pl.ds(t, seq, stride=2 * e), :].astype(BF16))

    def turn_a(t, _):
        for u in range(4):
            a_f32[pl.ds(4 * t + u, res, stride=e), :] = turned(4 * t + u)
        return 0

    def turn_c(t, _):
        for u in range(4):
            f = 4 * t + u
            other = turned(e + f).astype(BF16)
            for b in range(side):
                c_send[b, pl.ds(pl.multiple_of(f * w, w), w), :] = other[b * w:(b + 1) * w]
        return 0
    def gather_bias(turned):
        for h in range(heads):
            plane = flat[pl.ds(h, res, stride=heads), :]
            bias[h] = plane.T if turned else plane

    places = {0: (0, 0), 1: (0, 1), side - 1: (1, 0), 2: (1, 1)}

    def slot(buf, k, l, rows=None):
        pair_id, part_id = places[l]
        return buf.at[k, pair_id, pl.ds(0, blk) if rows is None else rows, pl.ds(part_id * seq, seq)]

    order = [0, 1, side - 1, 2]
    assert side == len(order)
    xn, yn = [lax.rem(x + 1, side), lax.rem(x + side - 1, side)], [lax.rem(y + 1, side), lax.rem(y + side - 1, side)]
    back_by = [1, side - 1]
    halves = [pl.ds(0, blk // 2), pl.ds(blk // 2, blk // 2)]
    first, hop, passed = [{}, {}], {}, {}

    def send_first(which):
        for k in order[1:]:
            ty, tx = lax.rem(y + k, side), lax.rem(x + k, side)
            if which == 0:
                cp = remote(a_send.at[ty], slot(a_buf, k, 0), s1.at[0, k], r1.at[0, k], dev(ty, x, c))
            else:
                cp = remote(c_send.at[tx], slot(c_buf, 0, k), s1.at[1, k], r1.at[1, k], dev(y, tx, c))
            cp.start()
            first[which][k] = cp

    def spread(which, k):
        for d in range(2):
            if which == 0:
                cp = remote(a_send.at[y] if k == 0 else slot(a_buf, k, 0), slot(a_buf, k, back_by[d]), s2.at[0, k, d], r2.at[0, k, d], dev(y, xn[d], c))
            else:
                cp = remote(c_send.at[x] if k == 0 else slot(c_buf, 0, k), slot(c_buf, back_by[d], k), s2.at[1, k, d], r2.at[1, k, d], dev(yn[d], x, c))
            cp.start()
            hop[which, k, d] = cp

    def relay(k):
        for d in range(2):
            hop[0, k, d].wait_recv()
            f = remote(slot(a_buf, k, back_by[d], halves[d]), slot(a_buf, k, 2, halves[d]), s3.at[0, k, d], r3.at[0, k, d], dev(y, xn[d], c))
            f.start()
            hop[1, k, d].wait_recv()
            g = remote(slot(c_buf, back_by[d], k, halves[d]), slot(c_buf, 2, k, halves[d]), s3.at[1, k, d], r3.at[1, k, d], dev(yn[d], x, c))
            g.start()
            passed[k, d] = (f, g)

    def wait_passed(k):
        for d in range(2):
            for f in passed[k, d]:
                f.wait_recv()

    cols = blk // 2

    def product(chunk, dst_id, fresh=False):
        k, p = chunk
        base = jnp.where(dst_id == 0, 1 - c, c) * cols
        part_sum = dot_nt(c_buf[k, p], a_buf[k, p, pl.ds(pl.multiple_of(base, cols), cols), :])
        if fresh:
            acc[dst_id] = part_sum
        else:
            acc[dst_id] += part_sum

    def products(chunk, fresh=False):
        product(chunk, 0, fresh)
        product(chunk, 1, fresh)

    lax.fori_loop(0, e // 4, turn_a, 0, unroll=2)
    for b in range(side):
        a_send[b] = a_f32[b * blk:(b + 1) * blk].astype(BF16)
    send_first(0)
    spread(0, 0)
    lax.fori_loop(0, e // 4, turn_c, 0, unroll=2)
    send_first(1)
    spread(1, 0)
    a_buf[0, 0, :, :seq] = a_send[y]
    c_buf[0, 0, :, :seq] = c_send[x]
    rows_to_block_wait(me, side, z_ref, zblk, sb, rb)
    one, three, two = order[1:]
    first[0][one].wait_recv()
    first[1][one].wait_recv()
    spread(0, one)
    spread(1, one)
    relay(0)
    first[0][three].wait_recv()
    first[1][three].wait_recv()
    spread(0, three)
    spread(1, three)
    relay(one)
    products((0, 0), True)
    first[0][two].wait_recv()
    first[1][two].wait_recv()
    spread(0, two)
    spread(1, two)
    products((one, 0))
    relay(three)
    products((three, 0))
    wait_passed(0)
    products((0, 1))
    relay(two)
    wait_passed(one)
    products((two, 0))
    products((one, 1))
    wait_passed(three)
    products((three, 1))
    wait_passed(two)
    product((two, 1), 0)
    swap = remote(acc.at[0], got, s4, r4, dev(y, x, 1 - c))
    swap.start()
    product((two, 1), 1)
    for k in order[1:]:
        first[0][k].wait_send()
        first[1][k].wait_send()
    for cp in hop.values():
        cp.wait_send()
    for pair in passed.values():
        for f in pair:
            f.wait_send()
    swap.wait()

    per = 128 // e
    lane_i = lax.broadcasted_iota(jnp.int32, (w, 128), 1) // e
    keep = [(lane_i == i).astype(F32) for i in range(per)]

    def place(f, _):
        for g in range(cols // 128):
            rows = pl.ds(pl.multiple_of(f * w, w), w)
            both = acc[1, rows, g * 128:(g + 1) * 128] + got[rows, g * 128:(g + 1) * 128]
            for i in range(per):
                r0 = (g * per + i) * w
                terms[r0:r0 + w, pl.ds(pl.multiple_of(f * 128, 128), 128)] = (both * keep[i]).astype(BF16)
        return 0
    lax.fori_loop(0, blk // w, place, 0)
    update = dot(terms[...], opmw_buf[...]) / count_buf[...]
    fresh = (zblk[...].reshape(side * r * w, pc).astype(F32) + update).astype(BF16)
    zsend[...] = fresh.reshape(side, r, w, pc)

    nh = r * heads
    groups = (w // 2) * w // 128
    part_bias = dot_nt(sb_ref[...], norm_rows(fresh.astype(F32)))[:heads]
    msg[0, 0, :nh] = jnp.concatenate([part_bias[:, g * 128:(g + 1) * 128] for g in range(groups)], axis=0).astype(BF16)
    gathers = exchange_all(inbox.at[0, :, :nh], lambda p: msg.at[0, 0, :nh], s6, r6)
    my_core = x // half
    for t in range(side):
        dst = y * 2 * side + (c * half + t // 2) * 2 + t % 2

        @pl.when(dst != me)
        def _():
            remote(zsend.at[t], zrows.at[x], s5.at[t], r5.at[x], dst).start()

        @pl.when(dst == me)
        def _():
            zrows[x] = zsend[t]
    for t in range(side):
        dst = y * 2 * side + (c * half + t // 2) * 2 + t % 2
        src = y * 2 * side + t * 2 + my_core

        @pl.when(dst != me)
        def _():
            remote(zsend.at[t], zrows.at[x], s5.at[t], r5.at[x], dst).wait_send()

        @pl.when(src != me)
        def _():
            remote(zsend.at[t], zrows.at[t], s5.at[t], r5.at[t], dst).wait_recv()
    for t in range(side):
        z_f[:, t * w:(t + 1) * w, :] = zrows[t].astype(F32)

    for cp in gathers:
        cp.wait()
    flat[...] = inbox[0, :, :nh].astype(F32).reshape(n * nh, res)
    per_y = 2 * groups
    for yy in range(side):
        for h in range(heads):
            pieces = [flat[pl.ds((yy * side + xx) * per_y * heads + h, per_y, stride=heads), :] for xx in range(side)]
            for i in range(128 // w):
                bias[h, pl.ds(yy * w + i, per_y, stride=128 // w), :] = jnp.concatenate([piece[:, i * w:(i + 1) * w] for piece in pieces], axis=1)
    maskb = (resm_ref[...].astype(F32) - 1.0) * 1e4
    triangle(z_f, bias, maskb, sq_ref, so_ref, heads)

    rr = r * r

    def pack(slot_id):
        for p in range(n):
            msg[slot_id, p, :rr] = jnp.concatenate([z_f[i, p * r:(p + 1) * r, :] for i in range(r)], axis=0).astype(BF16)

    def unpack(slot_id):
        flat[...] = inbox[slot_id, :, :rr].astype(F32).reshape(n * rr, pc)
        for i in range(r):
            z_f[i] = flat[pl.ds(i, res, stride=r), :]

    pack(1)
    rows_b = bias_rows(z_f, eb_ref, heads)
    for p in range(n):
        msg[1, p, rr:] = rows_b
    for cp in exchange_all(inbox.at[1], lambda p: msg.at[1, p], s7, r7):
        cp.wait()
    flat[...] = inbox[1, :, rr:].astype(F32).reshape(n * nh, res)
    gather_bias(True)
    unpack(1)
    triangle(z_f, bias, maskb, eq_ref, eo_ref, heads)
    pack(2)
    for cp in exchange_all(inbox.at[2, :, :rr], lambda p: msg.at[2, p, :rr], s8, r8):
        cp.wait()
    unpack(2)
    z_out[...] = z_f[...].astype(BF16)
    store.wait()


def block_call(n, side, dims, ops):
    m, z = ops[0], ops[1]
    seq, ch, res = m.shape
    r, _, w, pc = z.shape
    mh, md, heads = dims
    width, e = mh * md, ops[11].shape[0] // 2
    blk = w * e
    vm, dma = pltpu.VMEM, pltpu.SemaphoreType.DMA
    assert r == heads and mh == md and res == 128 and seq == 128 and pc == 128
    own = res // n
    buf = vm((side, half_of(side), blk, 2 * seq), BF16)
    tall = vm((seq, width, res), BF16)
    box = vm((3, n, 2 * r * r, pc), BF16)
    scratch = [vm(op.shape, op.dtype) for op in ops] + [dma((len(ops) + 1,))]
    scratch += [vm((seq, res), F32), tall, vm((seq, res, width + 16), BF16), tall, tall, vm((seq, width, res), F32),
               vm((2, mh // 2, res, 2 * res), F32), vm((2, mh // 2, res, 2 * res), BF16), vm((2, mh // 2, 8, 2 * res), F32),
               vm((mh // 2, res, 2 * res), F32), vm((mh // 2, width, 2 * res), BF16), vm((n + 1, r * mh, res), BF16), vm((n * r * mh, res), F32),
               vm((ch, width), BF16), vm((ch, width), BF16),
               vm((3, width, res), F32), vm((n, 3, own, width), F32), vm((n, 3, own, width), F32), vm((2, own, width), F32), vm((2, n, own, width), F32),
               vm((width, res), F32), vm((seq, mh, res), F32), vm((seq, md, res), F32), vm((res * e, seq), F32),
               vm((side, blk, seq), BF16), vm((side, blk, seq), BF16), vm((side, r, w, pc), BF16), vm((e * e, pc), F32), vm((e * 128, pc), BF16),
               vm((w // 2 * w, pc), F32), vm((res, res), F32),
               buf, buf, vm((2, blk, blk // 2), F32), vm((blk, blk // 2), F32), vm((w // 2 * w, e * 128), BF16),
               vm((side, r, w, pc), BF16), vm((side, r, w, pc), BF16), vm((r, res, pc), F32),
               vm((heads, res, res), F32), box, box, vm((n * r * r, pc), F32),
               dma((n,)), dma((n,)), dma((side,)), dma((side,))] + [dma((n,))] * 8 + [
               dma((2, side)), dma((2, side)), dma((2, side, 2)), dma((2, side, 2)), dma((2, side, 2)), dma((2, side, 2)),
               dma, dma, dma((side,)), dma((side,))] + [dma((n,))] * 6
    return pl.pallas_call(
        functools.partial(block_kernel, n, side, dims, len(ops)),
        out_shape=[jax.ShapeDtypeStruct((seq, ch, res), BF16), jax.ShapeDtypeStruct((r, res, pc), BF16)],
        in_specs=[pl.BlockSpec(memory_space=pl.ANY)] * len(ops),
        out_specs=[pl.BlockSpec(memory_space=pl.ANY), vmem()], scratch_shapes=scratch,
        compiler_params=pltpu.CompilerParams(collective_id=0, has_side_effects=True, vmem_limit_bytes=63 * 1024 * 1024),
        name='evoformer_block')(*ops)


def half_of(side):
    return side // 2


def solution(mesh):
    n = mesh.shape['dap']
    side = math.isqrt(n // 2)
    assert 2 * side * side == n

    def block(msa, pair, mask_full, res_mask, row_bias_w, row_qkvg_w, row_out_w, col_query_w, col_kv_w, col_gate_w, col_out_w, opm_proj_w, opm_out_w, start_bias_w, start_qkvg_w, start_out_w, end_bias_w, end_qkvg_w, end_out_w):
        r, res, pc = pair.shape
        ch = msa.shape[-1]
        last = lambda weight: jnp.moveaxis(weight, 0, -1).reshape(-1, weight.shape[0])
        first = lambda weight: weight.reshape(-1, weight.shape[-1])
        ops = [msa.transpose(0, 2, 1), pair.reshape(r, side, res // side, pc), mask_full, res_mask[None],
               row_bias_w.T, last(row_qkvg_w), first(row_out_w), last(col_query_w), last(col_kv_w), last(col_gate_w), first(col_out_w),
               last(opm_proj_w), first(opm_out_w), start_bias_w.T, last(start_qkvg_w), first(start_out_w), end_bias_w.T, last(end_qkvg_w), first(end_out_w)]
        msa_out, pair_out = block_call(n, side, col_gate_w.shape[1:] + (start_bias_w.shape[-1],), ops)
        return msa_out.transpose(0, 2, 1), pair_out

    row_spec = P(('data', 'dap'), None, None)
    in_specs = (row_spec, row_spec, P('data', None), P('data')) + (P(),) * 15
    return jax.shard_map(block, mesh=mesh, in_specs=in_specs, out_specs=(row_spec, row_spec), check_vma=False)
```

```python
import functools
import math

import jax
import jax.numpy as jnp
from jax import lax
from jax.experimental import pallas as pl
from jax.experimental.pallas import tpu as pltpu
from jax.sharding import PartitionSpec as P

MESH = pl.DeviceIdType.MESH
F32 = jnp.float32
BF16 = jnp.bfloat16
NT = (((1,), (1,)), ((), ()))


def dot(a, b):
    return jnp.dot(a, b, preferred_element_type=F32)


def dot_nt(a, b):
    return lax.dot_general(a, b, NT, preferred_element_type=F32)


LOG2E = 1.4426950408889634
BLOCK = 16


def norm_cols(x):
    mean = jnp.mean(x, axis=0, keepdims=True)
    cen = x - mean
    var = jnp.mean(cen * cen, axis=0, keepdims=True)
    return (cen * lax.rsqrt(var + 1e-5)).astype(BF16)


def wide(ref, g):
    return jnp.concatenate([ref[g * BLOCK + u] for u in range(BLOCK)], axis=1)


def put(ref, g, value):
    res = ref.shape[-1]
    for u in range(BLOCK):
        ref[g * BLOCK + u] = value[:, u * res:(u + 1) * res]


def split_mask(hd):
    whole = jnp.float32(-1e4 * hd ** 0.5)
    high = whole.astype(BF16).astype(F32)
    mid = (whole - high).astype(BF16).astype(F32)
    return high, mid, whole - high - mid


def row_project(heads, hd, m_ref, mask_ref, wt_ref, q_buf, k_buf, v_buf, g_buf):
    seq, ch, res = m_ref.shape
    width = heads * hd
    terms = split_mask(hd)

    def step(g, _):
        proj = jnp.dot(wt_ref[...], norm_cols(wide(m_ref, g).astype(F32)), preferred_element_type=F32)
        put(q_buf, g, proj[:width].astype(BF16))
        put(v_buf, g, proj[2 * width:3 * width].astype(BF16))
        put(g_buf, g, proj[3 * width:].astype(BF16))
        for u in range(BLOCK):
            s = g * BLOCK + u
            off = 1.0 - mask_ref[pl.ds(s, 1), :]
            row = lax.broadcasted_iota(jnp.int32, (16, res), 0)
            extra = jnp.where(row == 0, terms[0], jnp.where(row == 1, terms[1], jnp.where(row == 2, terms[2], 0.0))) * off
            k_buf[s] = jnp.concatenate([proj[width:2 * width, u * res:(u + 1) * res], extra], axis=0).T.astype(BF16)
        return 0
    lax.fori_loop(0, seq // BLOCK, step, 0, unroll=4)


def row_attend(heads, hd, bias_ref, pick_ref, q_buf, k_buf, v_buf, att_buf, raw_buf, w_buf, den_buf):
    seq, width, res = q_buf.shape
    pairs = heads // 2
    scale = LOG2E * hd ** -0.5
    row = lax.broadcasted_iota(jnp.int32, (16, 2 * res), 0)
    ones = jnp.where(row < 3, 1.0, 0.0).astype(BF16)

    def logits(s, b, p):
        qt = q_buf[s]
        q2 = jnp.concatenate([qt, qt], axis=1)
        raw_buf[b, p] = jnp.dot(k_buf[s], jnp.concatenate([q2 * pick_ref[p], ones], axis=0), preferred_element_type=F32)

    def weigh(b, p):
        t = raw_buf[b, p] * scale + bias_ref[p]
        w = jnp.exp2(t - jnp.max(t, axis=0, keepdims=True))
        w_buf[b, p] = w.astype(BF16)
        den_buf[b, p] = jnp.broadcast_to(1.0 / jnp.sum(w, axis=0, keepdims=True), (8, 2 * res))

    def values(s, b, p):
        lo = 2 * p * hd
        o = jnp.dot(v_buf[s, lo:lo + 2 * hd], w_buf[b, p], preferred_element_type=F32) * den_buf[b, p, 0:1]
        att_buf[s, lo:lo + hd] = o[:hd, :res]
        att_buf[s, lo + hd:lo + 2 * hd] = o[hd:, res:]

    for p in range(pairs):
        logits(0, 0, p)
    for p in range(pairs):
        logits(1, 1, p)
        weigh(0, p)

    def step(t, _):
        for u in range(8):
            s = 8 * t + u
            for p in range(pairs):
                logits(jnp.minimum(s + 2, seq - 1), u % 2, p)
                weigh((u + 1) % 2, p)
                values(s, u % 2, p)
        return 0
    lax.fori_loop(0, seq // 8, step, 0)


def row_finish(m_ref, mask_ref, wo_ref, g_buf, att_buf, new_ref, ln_ref):
    seq, ch, res = m_ref.shape

    def step(g, total):
        y = (jax.nn.sigmoid(wide(g_buf, g).astype(F32)) * wide(att_buf, g)).astype(BF16)
        new = (wide(m_ref, g).astype(F32) + jnp.dot(wo_ref[...], y, preferred_element_type=F32)).astype(BF16)
        put(new_ref, g, new)
        ln = norm_cols(new.astype(F32))
        put(ln_ref, g, ln)
        for u in range(BLOCK):
            total += ln[:, u * res:(u + 1) * res].astype(F32) * mask_ref[pl.ds(g * BLOCK + u, 1), :]
        return total
    return lax.fori_loop(0, seq // BLOCK, step, jnp.zeros((ch, res), F32), unroll=2)


def col_project(ln_ref, wkv_ref, key_buf, val_buf):
    seq, ch, res = ln_ref.shape
    hd = key_buf.shape[1]

    def step(g, _):
        kv = jnp.dot(wkv_ref[...], wide(ln_ref, g), preferred_element_type=F32).astype(BF16).astype(F32)
        put(key_buf, g, kv[:hd])
        put(val_buf, g, kv[hd:])
        return 0
    lax.fori_loop(0, seq // BLOCK, step, 0, unroll=4)


def col_gates(ln_ref, wg_ref, gate_buf):
    seq, ch, res = ln_ref.shape

    def step(g, _):
        gate = jnp.dot(wg_ref[...], wide(ln_ref, g), preferred_element_type=F32).astype(BF16).astype(F32)
        put(gate_buf, g, jax.nn.sigmoid(gate))
        return 0
    lax.fori_loop(0, seq // BLOCK, step, 0, unroll=4)


def col_sums(query, mask_ref, key_buf, val_buf):
    seq, hd, res = val_buf.shape
    heads = query[0].shape[0]
    scale = hd ** -0.5

    def first(g, top):
        for u in range(BLOCK):
            s = g * BLOCK + u
            k = key_buf[s]
            logit = query[0] * k[0:1]
            for d in range(1, hd):
                logit += query[d] * k[d:d + 1]
            logit = logit * scale + (mask_ref[pl.ds(s, 1), :] - 1.0) * 1e4
            key_buf[s] = logit
            top = jnp.maximum(top, logit)
        return top
    top = lax.fori_loop(0, seq // BLOCK, first, jnp.full((heads, res), -jnp.inf, F32))

    def second(g, carry):
        den, acc = carry
        acc = list(acc)
        for u in range(BLOCK):
            s = g * BLOCK + u
            w = jnp.exp(key_buf[s] - top)
            den = den + w
            wb = w.astype(BF16).astype(F32)
            val = val_buf[s]
            for d in range(hd):
                acc[d] = acc[d] + wb * val[d:d + 1]
        return den, tuple(acc)
    zero = jnp.zeros((heads, res), F32)
    den, acc = lax.fori_loop(0, seq // BLOCK, second, (zero, (zero,) * hd))
    return acc, top, den


def col_finish(att, m_ref, mask_ref, wo_ref, wp_ref, out_ref, proj_ref):
    seq, ch, res = m_ref.shape

    def step(g, _):
        tiled = jnp.concatenate([att] * BLOCK, axis=1)
        y = (wide(proj_ref, g) * tiled).astype(BF16)
        new = (wide(m_ref, g).astype(F32) + jnp.dot(wo_ref[...], y, preferred_element_type=F32)).astype(BF16)
        put(out_ref, g, new)
        proj = jnp.dot(wp_ref[...], norm_cols(new.astype(F32)), preferred_element_type=F32).astype(BF16)
        for u in range(BLOCK):
            s = g * BLOCK + u
            proj_ref[s] = (proj[:, u * res:(u + 1) * res].astype(F32) * mask_ref[pl.ds(s, 1), :]).astype(proj_ref.dtype)
        return 0
    lax.fori_loop(0, seq // BLOCK, step, 0, unroll=4)


def remote(src, dst, send_sem, recv_sem, dev):
    return pltpu.make_async_remote_copy(src_ref=src, dst_ref=dst, send_sem=send_sem, recv_sem=recv_sem,
                                        device_id={'dap': dev}, device_id_type=MESH)


def vmem():
    return pl.BlockSpec(memory_space=pltpu.VMEM)


def position(me, side):
    return me // (2 * side), (me // 2) % side, me % 2


def rows_to_block(me, side, rows_ref, block_ref, send_sem, recv_sem):
    y, x, c = position(me, side)
    half = side // 2
    slot = (x % half) * 2 + c
    core = x // half
    for t in range(side):
        dst = y * 2 * side + t * 2 + core

        @pl.when(dst != me)
        def _():
            remote(rows_ref.at[:, t], block_ref.at[slot], send_sem.at[t], recv_sem.at[slot], dst).start()

        @pl.when(dst == me)
        def _():
            block_ref[slot] = rows_ref[:, t]


def rows_to_block_wait(me, side, rows_ref, block_ref, send_sem, recv_sem):
    y, x, c = position(me, side)
    half = side // 2
    core = x // half
    for t in range(side):
        dst = y * 2 * side + t * 2 + core
        src = y * 2 * side + (c * half + t // 2) * 2 + t % 2

        @pl.when(dst != me)
        def _():
            remote(rows_ref.at[:, t], block_ref.at[t], send_sem.at[t], recv_sem.at[t], dst).wait_send()

        @pl.when(src != me)
        def _():
            remote(rows_ref.at[:, 0], block_ref.at[t], send_sem.at[t], recv_sem.at[t], dst).wait_recv()


def norm_rows(x):
    mean = jnp.mean(x, axis=-1, keepdims=True)
    cen = x - mean
    var = jnp.mean(cen * cen, axis=-1, keepdims=True)
    return (cen * lax.rsqrt(var + 1e-5)).astype(BF16)


def triangle(z_ref, bias_ref, maskb, qkvg_ref, out_w_ref, heads):
    rows, res, ch = z_ref.shape
    width = qkvg_ref.shape[0] // 4
    hd = width // heads
    lane_head = lax.broadcasted_iota(jnp.int32, (res, width), 1) // hd
    picks = [(lane_head == h).astype(F32) for h in range(heads)]
    pick_bf = jnp.concatenate(picks, axis=0).astype(BF16)
    bias = bias_ref[...].reshape(heads * res, res) + maskb
    projs = [dot_nt(norm_rows(z_ref[i]), qkvg_ref[...]) for i in range(rows)]
    raws = []
    for i in range(rows):
        q = projs[i][:, :width].astype(BF16)
        k = projs[i][:, width:2 * width].astype(BF16)
        raws.append(lax.dot_general(jnp.concatenate([q] * heads, axis=0) * pick_bf, k, (((1,), (1,)), ((), ())), preferred_element_type=F32))
    outs = []
    for i in range(rows):
        t = raws[i] * hd ** -0.5 + bias
        w = jnp.exp(t - jnp.max(t, axis=-1, keepdims=True))
        den = 1.0 / jnp.sum(w, axis=-1, keepdims=True)
        v = projs[i][:, 2 * width:3 * width].astype(BF16)
        outs.append(jnp.dot(w.astype(BF16), v, preferred_element_type=F32) * den)
    for i in range(rows):
        att = outs[i][:res] * picks[0]
        for h in range(1, heads):
            att += outs[i][h * res:(h + 1) * res] * picks[h]
        gate = projs[i][:, 3 * width:].astype(BF16).astype(F32)
        y = (jax.nn.sigmoid(gate) * att).astype(BF16)
        z_ref[i] = (z_ref[i] + jnp.dot(y, out_w_ref[...], preferred_element_type=F32)).astype(BF16).astype(F32)


def bias_rows(z_f, wb_ref, heads):
    parts = [dot_nt(wb_ref[...], norm_rows(z_f[i]))[:heads] for i in range(z_f.shape[0])]
    return jnp.concatenate(parts, axis=0).astype(BF16)


def combine_sum(got):
    return jnp.sum(got[:, 0], axis=0)


def combine_softmax(got):
    acc, top, den = got[:, 0], got[:, 1], got[:, 2]
    scale = jnp.exp(top - jnp.max(top, axis=0, keepdims=True))
    return jnp.sum(acc * scale, axis=0) / jnp.sum(den * scale, axis=0)


def block_kernel(n, side, dims, n_ops, *refs):
    operands, (m_out, z_out), loaded, load_sem, rest = refs[:n_ops], refs[n_ops:n_ops + 2], refs[n_ops + 2:2 * n_ops + 2], refs[2 * n_ops + 2], refs[2 * n_ops + 3:]
    m_ref, z_ref, mask_ref, resm_ref, rb_ref, rw_ref, ro_ref, cq_ref, ckv_ref, cg_ref, co_ref, op_ref, ow_ref, sb_ref, sq_ref, so_ref, eb_ref, eq_ref, eo_ref = loaded
    (
                 smask, q_buf, k_buf, v_buf, g_buf, att_buf, raw_buf, w_buf, den_buf, rbias, pick, rbox, rflat, wt_row, wt_col,
                 part, cut, got1, mine, back, small, logit_buf, val_buf, a_f32, a_send, c_send, zblk, opm_f32, opmw_buf, count_buf, pairs_buf,
                 a_buf, c_buf, acc, got, terms, zsend, zrows, z_f, bias, msg, inbox, flat,
                 sa, ra, sb, rb, sc1, rc1, sc2, rc2, sd1, rd1, sd2, rd2,
                 s1, r1, s2, r2, s3, r3, s4, r4, s5, r5, s6, r6, s7, r7, s8, r8) = rest
    mh, md, heads = dims
    me = lax.axis_index('dap')
    y, x, c = position(me, side)
    half = side // 2
    seq, ch, res = m_ref.shape
    r, _, w, pc = z_ref.shape
    blk = a_buf.shape[2]
    width = mh * md
    e = op_ref.shape[0] // 2

    def dev(yy, xx, cc):
        return (yy * side + xx) * 2 + cc

    def ring(d):
        return min(d, side - d)

    steps = [(dy, dx, dc) for dy in range(side) for dx in range(side) for dc in range(2) if dy + dx + dc]
    steps.sort(key=lambda t: -(ring(t[0]) + ring(t[1])))
    peers = [((dy * side + dx) * 2 + dc, dev(lax.rem(y + dy, side), lax.rem(x + dx, side), lax.rem(c + dc, 2))) for dy, dx, dc in steps]

    def exchange_all(box, src_of, send_sem, recv_sem):
        copies = []
        for k, dst in peers:
            cp = remote(src_of(dst), box.at[me], send_sem.at[k], recv_sem.at[k], dst)
            cp.start()
            copies.append(cp)
        box[me] = src_of(me)[...]
        return copies

    barrier = pltpu.get_barrier_semaphore()
    for _, dst in peers:
        pl.semaphore_signal(barrier, inc=1, device_id={'dap': dst}, device_id_type=MESH)
    loads = [pltpu.make_async_copy(src, dst, load_sem.at[i]) for i, (src, dst) in enumerate(zip(operands, loaded))]
    urgent = [1, 4]
    for i in urgent:
        loads[i].start()
    for i in range(n_ops):
        if i not in urgent:
            loads[i].start()
    for i in urgent:
        loads[i].wait()

    for i in range(r):
        for t in range(side):
            z_f[i, t * w:(t + 1) * w, :] = z_ref[i, t].astype(F32)
    rmsg = rbox.at[n]
    rmsg[...] = bias_rows(z_f, rb_ref, mh)
    pl.semaphore_wait(barrier, n - 1)
    gathers = exchange_all(rbox, lambda p: rmsg, sa, ra)
    rows_to_block(me, side, z_ref, zblk, sb, rb)

    for i in range(n_ops):
        if i not in urgent:
            loads[i].wait()
    smask[...] = mask_ref[pl.ds(pl.multiple_of(me * seq, seq), seq), :].astype(F32)
    wt_row[...] = ro_ref[...].astype(F32).T.astype(BF16)
    wt_col[...] = co_ref[...].astype(F32).T.astype(BF16)
    row_id = lax.broadcasted_iota(jnp.int32, (width, 2 * res), 0) // md
    lane_id = lax.broadcasted_iota(jnp.int32, (width, 2 * res), 1) // res
    for p in range(mh // 2):
        pick[p] = jnp.where(row_id == 2 * p + lane_id, 1.0, 0.0).astype(BF16)
    row_project(mh, md, m_ref, smask, rw_ref, q_buf, k_buf, v_buf, g_buf)

    for cp in gathers:
        cp.wait()
    rflat[...] = rbox[:n].astype(F32).reshape(n * r * mh, res)
    for h in range(mh):
        rbias[h // 2, :, (h % 2) * res:(h % 2 + 1) * res] = rflat[pl.ds(h, res, stride=mh), :].T * LOG2E
    row_attend(mh, md, rbias, pick, q_buf, k_buf, v_buf, att_buf, raw_buf, w_buf, den_buf)
    new_buf, ln_buf, last_buf = q_buf, v_buf, g_buf
    part[0] = row_finish(m_ref, smask, wt_row, g_buf, att_buf, new_buf, ln_buf)

    def all_reduce(terms_n, combine, send1, recv1, send2, recv2, beside1, beside2):
        own = res // n
        for t in range(terms_n):
            turned = part[t].T
            for p in range(n):
                cut[p, t] = turned[p * own:(p + 1) * own]
        copies = []
        for k, dst in peers:
            cp = remote(cut.at[dst, :terms_n], got1.at[me, :terms_n], send1.at[k], recv1.at[k], dst)
            cp.start()
            copies.append(cp)
        got1[me, :terms_n] = cut[me, :terms_n]
        beside1()
        for cp in copies:
            cp.wait()
        total = combine(got1[...])
        slot_id = 0 if terms_n == 1 else 1
        mine[slot_id] = total
        back[slot_id, me] = total
        copies = []
        for k, dst in peers:
            cp = remote(mine.at[slot_id], back.at[slot_id, me], send2.at[k], recv2.at[k], dst)
            cp.start()
            copies.append(cp)
        beside2()
        for cp in copies:
            cp.wait()
        return jnp.concatenate([back[slot_id, p] for p in range(n)], axis=0).T

    def count_pairs():
        step = seq

        def add(t, total):
            rows = mask_ref[pl.ds(pl.multiple_of(t * step, step), step), :].astype(F32)
            return total + dot(rows.T.astype(BF16), rows.astype(BF16))
        pairs_buf[...] = lax.fori_loop(0, mask_ref.shape[0] // step, add, jnp.zeros((res, res), F32), unroll=8)
        size = (w // 2 * w, res)
        row = lax.broadcasted_iota(jnp.int32, size, 0)
        lane = lax.broadcasted_iota(jnp.int32, size, 1)
        pick_i = jnp.where(lane == y * w + c * (w // 2) + row // w, 1.0, 0.0).astype(BF16)
        whole = pairs_buf[...]
        high = jnp.floor(whole * (1.0 / 128.0))
        both = dot(pick_i, high.astype(BF16)) * 128.0 + dot(pick_i, (whole - high * 128.0).astype(BF16))
        one = jnp.sum(jnp.where(lane == x * w + row % w, both, 0.0), axis=1, keepdims=True)
        count_buf[...] = jnp.broadcast_to(1e-3 + one, size)
        opm_f32[...] = ow_ref[...].astype(F32)
        for f in range(e):
            rows_f = opm_f32[pl.ds(f, e, stride=e), :].astype(BF16)
            for i in range(128 // e):
                opmw_buf[(f * (128 // e) + i) * e:(f * (128 // e) + i + 1) * e, :] = rows_f

    proj = att_buf
    count = []

    def project():
        count.append(jnp.sum(mask_ref[...].astype(F32), axis=0, keepdims=True) + 1e-10)
        col_project(ln_buf, ckv_ref, logit_buf, val_buf)

    qsum = all_reduce(1, combine_sum, sc1, rc1, sc2, rc2, project, lambda: col_gates(ln_buf, cg_ref, proj))
    small[...] = dot(cq_ref[...], (qsum / count[0]).astype(BF16)).astype(BF16).astype(F32)
    query = [small[pl.ds(d, mh, stride=md), :] for d in range(md)]
    sums, top, den = col_sums(query, smask, logit_buf, val_buf)
    for d in range(md):
        part[0, pl.ds(d, mh, stride=md), :] = sums[d]
        part[1, pl.ds(d, mh, stride=md), :] = top
        part[2, pl.ds(d, mh, stride=md), :] = den
    attended = all_reduce(3, combine_softmax, sd1, rd1, sd2, rd2, count_pairs, lambda: None)
    col_finish(attended, new_buf, smask, wt_col, op_ref, last_buf, proj)
    store = pltpu.make_async_copy(last_buf, m_out, load_sem.at[len(loads)])
    store.start()

    planes = proj.reshape(seq * 2 * e, res)

    eye = jnp.where(lax.broadcasted_iota(jnp.int32, (res, res), 0) == lax.broadcasted_iota(jnp.int32, (res, res), 1), 1.0, 0.0).astype(BF16)

    def turned(t):
        return dot_nt(eye, planes[pl.ds(t, seq, stride=2 * e), :].astype(BF16))

    def turn_a(t, _):
        for u in range(4):
            a_f32[pl.ds(4 * t + u, res, stride=e), :] = turned(4 * t + u)
        return 0

    def turn_c(t, _):
        for u in range(4):
            f = 4 * t + u
            other = turned(e + f).astype(BF16)
            for b in range(side):
                c_send[b, pl.ds(pl.multiple_of(f * w, w), w), :] = other[b * w:(b + 1) * w]
        return 0
    def gather_bias(turned):
        for h in range(heads):
            plane = flat[pl.ds(h, res, stride=heads), :]
            bias[h] = plane.T if turned else plane

    places = {0: (0, 0), 1: (0, 1), side - 1: (1, 0), 2: (1, 1)}

    def slot(buf, k, l, rows=None):
        pair_id, part_id = places[l]
        return buf.at[k, pair_id, pl.ds(0, blk) if rows is None else rows, pl.ds(part_id * seq, seq)]

    order = [0, 1, side - 1, 2]
    assert side == len(order)
    xn, yn = [lax.rem(x + 1, side), lax.rem(x + side - 1, side)], [lax.rem(y + 1, side), lax.rem(y + side - 1, side)]
    back_by = [1, side - 1]
    halves = [pl.ds(0, blk // 2), pl.ds(blk // 2, blk // 2)]
    first, hop, passed = [{}, {}], {}, {}

    def send_first(which):
        for k in order[1:]:
            ty, tx = lax.rem(y + k, side), lax.rem(x + k, side)
            if which == 0:
                cp = remote(a_send.at[ty], slot(a_buf, k, 0), s1.at[0, k], r1.at[0, k], dev(ty, x, c))
            else:
                cp = remote(c_send.at[tx], slot(c_buf, 0, k), s1.at[1, k], r1.at[1, k], dev(y, tx, c))
            cp.start()
            first[which][k] = cp

    def spread(which, k):
        for d in range(2):
            if which == 0:
                cp = remote(a_send.at[y] if k == 0 else slot(a_buf, k, 0), slot(a_buf, k, back_by[d]), s2.at[0, k, d], r2.at[0, k, d], dev(y, xn[d], c))
            else:
                cp = remote(c_send.at[x] if k == 0 else slot(c_buf, 0, k), slot(c_buf, back_by[d], k), s2.at[1, k, d], r2.at[1, k, d], dev(yn[d], x, c))
            cp.start()
            hop[which, k, d] = cp

    def relay(k):
        for d in range(2):
            hop[0, k, d].wait_recv()
            f = remote(slot(a_buf, k, back_by[d], halves[d]), slot(a_buf, k, 2, halves[d]), s3.at[0, k, d], r3.at[0, k, d], dev(y, xn[d], c))
            f.start()
            hop[1, k, d].wait_recv()
            g = remote(slot(c_buf, back_by[d], k, halves[d]), slot(c_buf, 2, k, halves[d]), s3.at[1, k, d], r3.at[1, k, d], dev(yn[d], x, c))
            g.start()
            passed[k, d] = (f, g)

    def wait_passed(k):
        for d in range(2):
            for f in passed[k, d]:
                f.wait_recv()

    cols = blk // 2

    def product(chunk, dst_id, fresh=False):
        k, p = chunk
        base = jnp.where(dst_id == 0, 1 - c, c) * cols
        part_sum = dot_nt(c_buf[k, p], a_buf[k, p, pl.ds(pl.multiple_of(base, cols), cols), :])
        if fresh:
            acc[dst_id] = part_sum
        else:
            acc[dst_id] += part_sum

    def products(chunk, fresh=False):
        product(chunk, 0, fresh)
        product(chunk, 1, fresh)

    lax.fori_loop(0, e // 4, turn_a, 0, unroll=2)
    for b in range(side):
        a_send[b] = a_f32[b * blk:(b + 1) * blk].astype(BF16)
    send_first(0)
    spread(0, 0)
    lax.fori_loop(0, e // 4, turn_c, 0, unroll=2)
    send_first(1)
    spread(1, 0)
    a_buf[0, 0, :, :seq] = a_send[y]
    c_buf[0, 0, :, :seq] = c_send[x]
    rows_to_block_wait(me, side, z_ref, zblk, sb, rb)
    one, three, two = order[1:]
    first[0][one].wait_recv()
    first[1][one].wait_recv()
    spread(0, one)
    spread(1, one)
    relay(0)
    first[0][three].wait_recv()
    first[1][three].wait_recv()
    spread(0, three)
    spread(1, three)
    relay(one)
    products((0, 0), True)
    first[0][two].wait_recv()
    first[1][two].wait_recv()
    spread(0, two)
    spread(1, two)
    products((one, 0))
    relay(three)
    products((three, 0))
    wait_passed(0)
    products((0, 1))
    relay(two)
    wait_passed(one)
    products((two, 0))
    products((one, 1))
    wait_passed(three)
    products((three, 1))
    wait_passed(two)
    product((two, 1), 0)
    swap = remote(acc.at[0], got, s4, r4, dev(y, x, 1 - c))
    swap.start()
    product((two, 1), 1)
    for k in order[1:]:
        first[0][k].wait_send()
        first[1][k].wait_send()
    for cp in hop.values():
        cp.wait_send()
    for pair in passed.values():
        for f in pair:
            f.wait_send()
    swap.wait()

    per = 128 // e
    lane_i = lax.broadcasted_iota(jnp.int32, (w, 128), 1) // e
    keep = [(lane_i == i).astype(F32) for i in range(per)]

    def place(f, _):
        for g in range(cols // 128):
            rows = pl.ds(pl.multiple_of(f * w, w), w)
            both = acc[1, rows, g * 128:(g + 1) * 128] + got[rows, g * 128:(g + 1) * 128]
            for i in range(per):
                r0 = (g * per + i) * w
                terms[r0:r0 + w, pl.ds(pl.multiple_of(f * 128, 128), 128)] = (both * keep[i]).astype(BF16)
        return 0
    lax.fori_loop(0, blk // w, place, 0)
    update = dot(terms[...], opmw_buf[...]) / count_buf[...]
    fresh = (zblk[...].reshape(side * r * w, pc).astype(F32) + update).astype(BF16)
    zsend[...] = fresh.reshape(side, r, w, pc)

    nh = r * heads
    groups = (w // 2) * w // 128
    part_bias = dot_nt(sb_ref[...], norm_rows(fresh.astype(F32)))[:heads]
    msg[0, 0, :nh] = jnp.concatenate([part_bias[:, g * 128:(g + 1) * 128] for g in range(groups)], axis=0).astype(BF16)
    gathers = exchange_all(inbox.at[0, :, :nh], lambda p: msg.at[0, 0, :nh], s6, r6)
    my_core = x // half
    for t in range(side):
        dst = y * 2 * side + (c * half + t // 2) * 2 + t % 2

        @pl.when(dst != me)
        def _():
            remote(zsend.at[t], zrows.at[x], s5.at[t], r5.at[x], dst).start()

        @pl.when(dst == me)
        def _():
            zrows[x] = zsend[t]
    for t in range(side):
        dst = y * 2 * side + (c * half + t // 2) * 2 + t % 2
        src = y * 2 * side + t * 2 + my_core

        @pl.when(dst != me)
        def _():
            remote(zsend.at[t], zrows.at[x], s5.at[t], r5.at[x], dst).wait_send()

        @pl.when(src != me)
        def _():
            remote(zsend.at[t], zrows.at[t], s5.at[t], r5.at[t], dst).wait_recv()
    for t in range(side):
        z_f[:, t * w:(t + 1) * w, :] = zrows[t].astype(F32)

    for cp in gathers:
        cp.wait()
    flat[...] = inbox[0, :, :nh].astype(F32).reshape(n * nh, res)
    per_y = 2 * groups
    for yy in range(side):
        for h in range(heads):
            pieces = [flat[pl.ds((yy * side + xx) * per_y * heads + h, per_y, stride=heads), :] for xx in range(side)]
            for i in range(128 // w):
                bias[h, pl.ds(yy * w + i, per_y, stride=128 // w), :] = jnp.concatenate([piece[:, i * w:(i + 1) * w] for piece in pieces], axis=1)
    maskb = (resm_ref[...].astype(F32) - 1.0) * 1e4
    triangle(z_f, bias, maskb, sq_ref, so_ref, heads)

    rr = r * r

    def pack(slot_id):
        for p in range(n):
            msg[slot_id, p, :rr] = jnp.concatenate([z_f[i, p * r:(p + 1) * r, :] for i in range(r)], axis=0).astype(BF16)

    def unpack(slot_id):
        flat[...] = inbox[slot_id, :, :rr].astype(F32).reshape(n * rr, pc)
        for i in range(r):
            z_f[i] = flat[pl.ds(i, res, stride=r), :]

    pack(1)
    rows_b = bias_rows(z_f, eb_ref, heads)
    for p in range(n):
        msg[1, p, rr:] = rows_b
    for cp in exchange_all(inbox.at[1], lambda p: msg.at[1, p], s7, r7):
        cp.wait()
    flat[...] = inbox[1, :, rr:].astype(F32).reshape(n * nh, res)
    gather_bias(True)
    unpack(1)
    triangle(z_f, bias, maskb, eq_ref, eo_ref, heads)
    pack(2)
    for cp in exchange_all(inbox.at[2, :, :rr], lambda p: msg.at[2, p, :rr], s8, r8):
        cp.wait()
    unpack(2)
    z_out[...] = z_f[...].astype(BF16)
    store.wait()


def block_call(n, side, dims, ops):
    m, z = ops[0], ops[1]
    seq, ch, res = m.shape
    r, _, w, pc = z.shape
    mh, md, heads = dims
    width, e = mh * md, ops[11].shape[0] // 2
    blk = w * e
    vm, dma = pltpu.VMEM, pltpu.SemaphoreType.DMA
    assert r == heads and mh == md and res == 128 and seq == 128 and pc == 128
    own = res // n
    buf = vm((side, half_of(side), blk, 2 * seq), BF16)
    tall = vm((seq, width, res), BF16)
    box = vm((3, n, 2 * r * r, pc), BF16)
    scratch = [vm(op.shape, op.dtype) for op in ops] + [dma((len(ops) + 1,))]
    scratch += [vm((seq, res), F32), tall, vm((seq, res, width + 16), BF16), tall, tall, vm((seq, width, res), F32),
               vm((2, mh // 2, res, 2 * res), F32), vm((2, mh // 2, res, 2 * res), BF16), vm((2, mh // 2, 8, 2 * res), F32),
               vm((mh // 2, res, 2 * res), F32), vm((mh // 2, width, 2 * res), BF16), vm((n + 1, r * mh, res), BF16), vm((n * r * mh, res), F32),
               vm((ch, width), BF16), vm((ch, width), BF16),
               vm((3, width, res), F32), vm((n, 3, own, width), F32), vm((n, 3, own, width), F32), vm((2, own, width), F32), vm((2, n, own, width), F32),
               vm((width, res), F32), vm((seq, mh, res), F32), vm((seq, md, res), F32), vm((res * e, seq), F32),
               vm((side, blk, seq), BF16), vm((side, blk, seq), BF16), vm((side, r, w, pc), BF16), vm((e * e, pc), F32), vm((e * 128, pc), BF16),
               vm((w // 2 * w, pc), F32), vm((res, res), F32),
               buf, buf, vm((2, blk, blk // 2), F32), vm((blk, blk // 2), F32), vm((w // 2 * w, e * 128), BF16),
               vm((side, r, w, pc), BF16), vm((side, r, w, pc), BF16), vm((r, res, pc), F32),
               vm((heads, res, res), F32), box, box, vm((n * r * r, pc), F32),
               dma((n,)), dma((n,)), dma((side,)), dma((side,))] + [dma((n,))] * 8 + [
               dma((2, side)), dma((2, side)), dma((2, side, 2)), dma((2, side, 2)), dma((2, side, 2)), dma((2, side, 2)),
               dma, dma, dma((side,)), dma((side,))] + [dma((n,))] * 6
    return pl.pallas_call(
        functools.partial(block_kernel, n, side, dims, len(ops)),
        out_shape=[jax.ShapeDtypeStruct((seq, ch, res), BF16), jax.ShapeDtypeStruct((r, res, pc), BF16)],
        in_specs=[pl.BlockSpec(memory_space=pl.ANY)] * len(ops),
        out_specs=[pl.BlockSpec(memory_space=pl.ANY), vmem()], scratch_shapes=scratch,
        compiler_params=pltpu.CompilerParams(collective_id=0, has_side_effects=True, vmem_limit_bytes=63 * 1024 * 1024),
        name='evoformer_block')(*ops)


def half_of(side):
    return side // 2


def solution(mesh):
    n = mesh.shape['dap']
    side = math.isqrt(n // 2)
    assert 2 * side * side == n

    def block(msa, pair, mask_full, res_mask, row_bias_w, row_qkvg_w, row_out_w, col_query_w, col_kv_w, col_gate_w, col_out_w, opm_proj_w, opm_out_w, start_bias_w, start_qkvg_w, start_out_w, end_bias_w, end_qkvg_w, end_out_w):
        r, res, pc = pair.shape
        ch = msa.shape[-1]
        last = lambda weight: jnp.moveaxis(weight, 0, -1).reshape(-1, weight.shape[0])
        first = lambda weight: weight.reshape(-1, weight.shape[-1])
        ops = [msa.transpose(0, 2, 1), pair.reshape(r, side, res // side, pc), mask_full, res_mask[None],
               row_bias_w.T, last(row_qkvg_w), first(row_out_w), last(col_query_w), last(col_kv_w), last(col_gate_w), first(col_out_w),
               last(opm_proj_w), first(opm_out_w), start_bias_w.T, last(start_qkvg_w), first(start_out_w), end_bias_w.T, last(end_qkvg_w), first(end_out_w)]
        msa_out, pair_out = block_call(n, side, col_gate_w.shape[1:] + (start_bias_w.shape[-1],), ops)
        return msa_out.transpose(0, 2, 1), pair_out

    row_spec = P(('data', 'dap'), None, None)
    in_specs = (row_spec, row_spec, P('data', None), P('data')) + (P(),) * 15
    return jax.shard_map(block, mesh=mesh, in_specs=in_specs, out_specs=(row_spec, row_spec), check_vma=False)
```

```python
import functools
import math

import jax
import jax.numpy as jnp
from jax import lax
from jax.experimental import pallas as pl
from jax.experimental.pallas import tpu as pltpu
from jax.sharding import PartitionSpec as P

MESH = pl.DeviceIdType.MESH
F32 = jnp.float32
BF16 = jnp.bfloat16
NT = (((1,), (1,)), ((), ()))


def dot(a, b):
    return jnp.dot(a, b, preferred_element_type=F32)


def dot_nt(a, b):
    return lax.dot_general(a, b, NT, preferred_element_type=F32)


LOG2E = 1.4426950408889634
BLOCK = 16


def norm_cols(x):
    mean = jnp.mean(x, axis=0, keepdims=True)
    cen = x - mean
    var = jnp.mean(cen * cen, axis=0, keepdims=True)
    return (cen * lax.rsqrt(var + 1e-5)).astype(BF16)


def wide(ref, g):
    return jnp.concatenate([ref[g * BLOCK + u] for u in range(BLOCK)], axis=1)


def put(ref, g, value):
    res = ref.shape[-1]
    for u in range(BLOCK):
        ref[g * BLOCK + u] = value[:, u * res:(u + 1) * res]


def split_mask(hd):
    whole = jnp.float32(-1e4 * hd ** 0.5)
    high = whole.astype(BF16).astype(F32)
    mid = (whole - high).astype(BF16).astype(F32)
    return high, mid, whole - high - mid


def row_project(heads, hd, m_ref, mask_ref, wt_ref, q_buf, k_buf, v_buf, g_buf):
    seq, ch, res = m_ref.shape
    width = heads * hd
    terms = split_mask(hd)

    def step(g, _):
        proj = jnp.dot(wt_ref[...], norm_cols(wide(m_ref, g).astype(F32)), preferred_element_type=F32)
        put(q_buf, g, proj[:width].astype(BF16))
        put(v_buf, g, proj[2 * width:3 * width].astype(BF16))
        put(g_buf, g, proj[3 * width:].astype(BF16))
        for u in range(BLOCK):
            s = g * BLOCK + u
            off = 1.0 - mask_ref[pl.ds(s, 1), :]
            row = lax.broadcasted_iota(jnp.int32, (16, res), 0)
            extra = jnp.where(row == 0, terms[0], jnp.where(row == 1, terms[1], jnp.where(row == 2, terms[2], 0.0))) * off
            k_buf[s] = jnp.concatenate([proj[width:2 * width, u * res:(u + 1) * res], extra], axis=0).T.astype(BF16)
        return 0
    lax.fori_loop(0, seq // BLOCK, step, 0, unroll=4)


def row_attend(heads, hd, bias_ref, pick_ref, q_buf, k_buf, v_buf, att_buf, raw_buf, w_buf, den_buf):
    seq, width, res = q_buf.shape
    pairs = heads // 2
    scale = LOG2E * hd ** -0.5
    row = lax.broadcasted_iota(jnp.int32, (16, 2 * res), 0)
    ones = jnp.where(row < 3, 1.0, 0.0).astype(BF16)

    def logits(s, b, p):
        qt = q_buf[s]
        q2 = jnp.concatenate([qt, qt], axis=1)
        raw_buf[b, p] = jnp.dot(k_buf[s], jnp.concatenate([q2 * pick_ref[p], ones], axis=0), preferred_element_type=F32)

    def weigh(b, p):
        t = raw_buf[b, p] * scale + bias_ref[p]
        w = jnp.exp2(t - jnp.max(t, axis=0, keepdims=True))
        w_buf[b, p] = w.astype(BF16)
        den_buf[b, p] = jnp.broadcast_to(1.0 / jnp.sum(w, axis=0, keepdims=True), (8, 2 * res))

    def values(s, b, p):
        lo = 2 * p * hd
        o = jnp.dot(v_buf[s, lo:lo + 2 * hd], w_buf[b, p], preferred_element_type=F32) * den_buf[b, p, 0:1]
        att_buf[s, lo:lo + hd] = o[:hd, :res]
        att_buf[s, lo + hd:lo + 2 * hd] = o[hd:, res:]

    for p in range(pairs):
        logits(0, 0, p)
    for p in range(pairs):
        logits(1, 1, p)
        weigh(0, p)

    def step(t, _):
        for u in range(16):
            s = 16 * t + u
            for p in range(pairs):
                logits(jnp.minimum(s + 2, seq - 1), u % 2, p)
                weigh((u + 1) % 2, p)
                values(s, u % 2, p)
        return 0
    lax.fori_loop(0, seq // 16, step, 0)


def row_finish(m_ref, mask_ref, wo_ref, g_buf, att_buf, new_ref, ln_ref):
    seq, ch, res = m_ref.shape

    def step(g, total):
        y = (jax.nn.sigmoid(wide(g_buf, g).astype(F32)) * wide(att_buf, g)).astype(BF16)
        new = (wide(m_ref, g).astype(F32) + jnp.dot(wo_ref[...], y, preferred_element_type=F32)).astype(BF16)
        put(new_ref, g, new)
        ln = norm_cols(new.astype(F32))
        put(ln_ref, g, ln)
        for u in range(BLOCK):
            total += ln[:, u * res:(u + 1) * res].astype(F32) * mask_ref[pl.ds(g * BLOCK + u, 1), :]
        return total
    return lax.fori_loop(0, seq // BLOCK, step, jnp.zeros((ch, res), F32), unroll=2)


def col_project(ln_ref, wkv_ref, key_buf, val_buf):
    seq, ch, res = ln_ref.shape
    hd = key_buf.shape[1]

    def step(g, _):
        kv = jnp.dot(wkv_ref[...], wide(ln_ref, g), preferred_element_type=F32).astype(BF16).astype(F32)
        put(key_buf, g, kv[:hd])
        put(val_buf, g, kv[hd:])
        return 0
    lax.fori_loop(0, seq // BLOCK, step, 0, unroll=4)


def col_gates(ln_ref, wg_ref, gate_buf):
    seq, ch, res = ln_ref.shape

    def step(g, _):
        gate = jnp.dot(wg_ref[...], wide(ln_ref, g), preferred_element_type=F32).astype(BF16).astype(F32)
        put(gate_buf, g, jax.nn.sigmoid(gate))
        return 0
    lax.fori_loop(0, seq // BLOCK, step, 0, unroll=4)


def col_sums(query, mask_ref, key_buf, val_buf):
    seq, hd, res = val_buf.shape
    heads = query[0].shape[0]
    scale = hd ** -0.5

    def first(g, top):
        for u in range(BLOCK):
            s = g * BLOCK + u
            k = key_buf[s]
            logit = query[0] * k[0:1]
            for d in range(1, hd):
                logit += query[d] * k[d:d + 1]
            logit = logit * scale + (mask_ref[pl.ds(s, 1), :] - 1.0) * 1e4
            key_buf[s] = logit
            top = jnp.maximum(top, logit)
        return top
    top = lax.fori_loop(0, seq // BLOCK, first, jnp.full((heads, res), -jnp.inf, F32))

    def second(g, carry):
        den, acc = carry
        acc = list(acc)
        for u in range(BLOCK):
            s = g * BLOCK + u
            w = jnp.exp(key_buf[s] - top)
            den = den + w
            wb = w.astype(BF16).astype(F32)
            val = val_buf[s]
            for d in range(hd):
                acc[d] = acc[d] + wb * val[d:d + 1]
        return den, tuple(acc)
    zero = jnp.zeros((heads, res), F32)
    den, acc = lax.fori_loop(0, seq // BLOCK, second, (zero, (zero,) * hd))
    return acc, top, den


def col_finish(att, m_ref, mask_ref, wo_ref, wp_ref, out_ref, proj_ref):
    seq, ch, res = m_ref.shape

    def step(g, _):
        tiled = jnp.concatenate([att] * BLOCK, axis=1)
        y = (wide(proj_ref, g) * tiled).astype(BF16)
        new = (wide(m_ref, g).astype(F32) + jnp.dot(wo_ref[...], y, preferred_element_type=F32)).astype(BF16)
        put(out_ref, g, new)
        proj = jnp.dot(wp_ref[...], norm_cols(new.astype(F32)), preferred_element_type=F32).astype(BF16)
        for u in range(BLOCK):
            s = g * BLOCK + u
            proj_ref[s] = (proj[:, u * res:(u + 1) * res].astype(F32) * mask_ref[pl.ds(s, 1), :]).astype(proj_ref.dtype)
        return 0
    lax.fori_loop(0, seq // BLOCK, step, 0, unroll=4)


def remote(src, dst, send_sem, recv_sem, dev):
    return pltpu.make_async_remote_copy(src_ref=src, dst_ref=dst, send_sem=send_sem, recv_sem=recv_sem,
                                        device_id={'dap': dev}, device_id_type=MESH)


def vmem():
    return pl.BlockSpec(memory_space=pltpu.VMEM)


def position(me, side):
    return me // (2 * side), (me // 2) % side, me % 2


def rows_to_block(me, side, rows_ref, block_ref, send_sem, recv_sem):
    y, x, c = position(me, side)
    half = side // 2
    slot = (x % half) * 2 + c
    core = x // half
    for t in range(side):
        dst = y * 2 * side + t * 2 + core

        @pl.when(dst != me)
        def _():
            remote(rows_ref.at[:, t], block_ref.at[slot], send_sem.at[t], recv_sem.at[slot], dst).start()

        @pl.when(dst == me)
        def _():
            block_ref[slot] = rows_ref[:, t]


def rows_to_block_wait(me, side, rows_ref, block_ref, send_sem, recv_sem):
    y, x, c = position(me, side)
    half = side // 2
    core = x // half
    for t in range(side):
        dst = y * 2 * side + t * 2 + core
        src = y * 2 * side + (c * half + t // 2) * 2 + t % 2

        @pl.when(dst != me)
        def _():
            remote(rows_ref.at[:, t], block_ref.at[t], send_sem.at[t], recv_sem.at[t], dst).wait_send()

        @pl.when(src != me)
        def _():
            remote(rows_ref.at[:, 0], block_ref.at[t], send_sem.at[t], recv_sem.at[t], dst).wait_recv()


def norm_rows(x):
    mean = jnp.mean(x, axis=-1, keepdims=True)
    cen = x - mean
    var = jnp.mean(cen * cen, axis=-1, keepdims=True)
    return (cen * lax.rsqrt(var + 1e-5)).astype(BF16)


def triangle(z_ref, bias_ref, maskb, qkvg_ref, out_w_ref, heads):
    rows, res, ch = z_ref.shape
    width = qkvg_ref.shape[0] // 4
    hd = width // heads
    lane_head = lax.broadcasted_iota(jnp.int32, (res, width), 1) // hd
    picks = [(lane_head == h).astype(F32) for h in range(heads)]
    pick_bf = jnp.concatenate(picks, axis=0).astype(BF16)
    bias = bias_ref[...].reshape(heads * res, res) + maskb
    projs = [dot_nt(norm_rows(z_ref[i]), qkvg_ref[...]) for i in range(rows)]
    raws = []
    for i in range(rows):
        q = projs[i][:, :width].astype(BF16)
        k = projs[i][:, width:2 * width].astype(BF16)
        raws.append(lax.dot_general(jnp.concatenate([q] * heads, axis=0) * pick_bf, k, (((1,), (1,)), ((), ())), preferred_element_type=F32))
    outs = []
    for i in range(rows):
        t = raws[i] * hd ** -0.5 + bias
        w = jnp.exp(t - jnp.max(t, axis=-1, keepdims=True))
        den = 1.0 / jnp.sum(w, axis=-1, keepdims=True)
        v = projs[i][:, 2 * width:3 * width].astype(BF16)
        outs.append(jnp.dot(w.astype(BF16), v, preferred_element_type=F32) * den)
    for i in range(rows):
        att = outs[i][:res] * picks[0]
        for h in range(1, heads):
            att += outs[i][h * res:(h + 1) * res] * picks[h]
        gate = projs[i][:, 3 * width:].astype(BF16).astype(F32)
        y = (jax.nn.sigmoid(gate) * att).astype(BF16)
        z_ref[i] = (z_ref[i] + jnp.dot(y, out_w_ref[...], preferred_element_type=F32)).astype(BF16).astype(F32)


def bias_rows(z_f, wb_ref, heads):
    parts = [dot_nt(wb_ref[...], norm_rows(z_f[i]))[:heads] for i in range(z_f.shape[0])]
    return jnp.concatenate(parts, axis=0).astype(BF16)


def combine_sum(got):
    return jnp.sum(got[:, 0], axis=0)


def combine_softmax(got):
    acc, top, den = got[:, 0], got[:, 1], got[:, 2]
    scale = jnp.exp(top - jnp.max(top, axis=0, keepdims=True))
    return jnp.sum(acc * scale, axis=0) / jnp.sum(den * scale, axis=0)


def block_kernel(n, side, dims, n_ops, *refs):
    operands, (m_out, z_out), loaded, load_sem, rest = refs[:n_ops], refs[n_ops:n_ops + 2], refs[n_ops + 2:2 * n_ops + 2], refs[2 * n_ops + 2], refs[2 * n_ops + 3:]
    m_ref, z_ref, mask_ref, resm_ref, rb_ref, rw_ref, ro_ref, cq_ref, ckv_ref, cg_ref, co_ref, op_ref, ow_ref, sb_ref, sq_ref, so_ref, eb_ref, eq_ref, eo_ref = loaded
    (
                 smask, q_buf, k_buf, v_buf, g_buf, att_buf, raw_buf, w_buf, den_buf, rbias, pick, rbox, rflat, wt_row, wt_col,
                 part, cut, got1, mine, back, small, logit_buf, val_buf, a_f32, a_send, c_send, zblk, opm_f32, opmw_buf, count_buf, pairs_buf,
                 a_buf, c_buf, acc, got, terms, zsend, zrows, z_f, bias, msg, inbox, flat,
                 sa, ra, sb, rb, sc1, rc1, sc2, rc2, sd1, rd1, sd2, rd2,
                 s1, r1, s2, r2, s3, r3, s4, r4, s5, r5, s6, r6, s7, r7, s8, r8) = rest
    mh, md, heads = dims
    me = lax.axis_index('dap')
    y, x, c = position(me, side)
    half = side // 2
    seq, ch, res = m_ref.shape
    r, _, w, pc = z_ref.shape
    blk = a_buf.shape[2]
    width = mh * md
    e = op_ref.shape[0] // 2

    def dev(yy, xx, cc):
        return (yy * side + xx) * 2 + cc

    def ring(d):
        return min(d, side - d)

    steps = [(dy, dx, dc) for dy in range(side) for dx in range(side) for dc in range(2) if dy + dx + dc]
    steps.sort(key=lambda t: -(ring(t[0]) + ring(t[1])))
    peers = [((dy * side + dx) * 2 + dc, dev(lax.rem(y + dy, side), lax.rem(x + dx, side), lax.rem(c + dc, 2))) for dy, dx, dc in steps]

    def exchange_all(box, src_of, send_sem, recv_sem):
        copies = []
        for k, dst in peers:
            cp = remote(src_of(dst), box.at[me], send_sem.at[k], recv_sem.at[k], dst)
            cp.start()
            copies.append(cp)
        box[me] = src_of(me)[...]
        return copies

    barrier = pltpu.get_barrier_semaphore()
    for _, dst in peers:
        pl.semaphore_signal(barrier, inc=1, device_id={'dap': dst}, device_id_type=MESH)
    loads = [pltpu.make_async_copy(src, dst, load_sem.at[i]) for i, (src, dst) in enumerate(zip(operands, loaded))]
    urgent = [1, 4]
    for i in urgent:
        loads[i].start()
    for i in range(n_ops):
        if i not in urgent:
            loads[i].start()
    for i in urgent:
        loads[i].wait()

    for i in range(r):
        for t in range(side):
            z_f[i, t * w:(t + 1) * w, :] = z_ref[i, t].astype(F32)
    rmsg = rbox.at[n]
    rmsg[...] = bias_rows(z_f, rb_ref, mh)
    pl.semaphore_wait(barrier, n - 1)
    gathers = exchange_all(rbox, lambda p: rmsg, sa, ra)
    rows_to_block(me, side, z_ref, zblk, sb, rb)

    for i in range(n_ops):
        if i not in urgent:
            loads[i].wait()
    smask[...] = mask_ref[pl.ds(pl.multiple_of(me * seq, seq), seq), :].astype(F32)
    wt_row[...] = ro_ref[...].astype(F32).T.astype(BF16)
    wt_col[...] = co_ref[...].astype(F32).T.astype(BF16)
    row_id = lax.broadcasted_iota(jnp.int32, (width, 2 * res), 0) // md
    lane_id = lax.broadcasted_iota(jnp.int32, (width, 2 * res), 1) // res
    for p in range(mh // 2):
        pick[p] = jnp.where(row_id == 2 * p + lane_id, 1.0, 0.0).astype(BF16)
    row_project(mh, md, m_ref, smask, rw_ref, q_buf, k_buf, v_buf, g_buf)

    for cp in gathers:
        cp.wait()
    rflat[...] = rbox[:n].astype(F32).reshape(n * r * mh, res)
    for h in range(mh):
        rbias[h // 2, :, (h % 2) * res:(h % 2 + 1) * res] = rflat[pl.ds(h, res, stride=mh), :].T * LOG2E
    row_attend(mh, md, rbias, pick, q_buf, k_buf, v_buf, att_buf, raw_buf, w_buf, den_buf)
    new_buf, ln_buf, last_buf = q_buf, v_buf, g_buf
    part[0] = row_finish(m_ref, smask, wt_row, g_buf, att_buf, new_buf, ln_buf)

    def all_reduce(terms_n, combine, send1, recv1, send2, recv2, beside1, beside2):
        own = res // n
        for t in range(terms_n):
            turned = part[t].T
            for p in range(n):
                cut[p, t] = turned[p * own:(p + 1) * own]
        copies = []
        for k, dst in peers:
            cp = remote(cut.at[dst, :terms_n], got1.at[me, :terms_n], send1.at[k], recv1.at[k], dst)
            cp.start()
            copies.append(cp)
        got1[me, :terms_n] = cut[me, :terms_n]
        beside1()
        for cp in copies:
            cp.wait()
        total = combine(got1[...])
        slot_id = 0 if terms_n == 1 else 1
        mine[slot_id] = total
        back[slot_id, me] = total
        copies = []
        for k, dst in peers:
            cp = remote(mine.at[slot_id], back.at[slot_id, me], send2.at[k], recv2.at[k], dst)
            cp.start()
            copies.append(cp)
        beside2()
        for cp in copies:
            cp.wait()
        return jnp.concatenate([back[slot_id, p] for p in range(n)], axis=0).T

    def count_pairs():
        step = seq

        def add(t, total):
            rows = mask_ref[pl.ds(pl.multiple_of(t * step, step), step), :].astype(F32)
            return total + dot(rows.T.astype(BF16), rows.astype(BF16))
        pairs_buf[...] = lax.fori_loop(0, mask_ref.shape[0] // step, add, jnp.zeros((res, res), F32), unroll=8)
        size = (w // 2 * w, res)
        row = lax.broadcasted_iota(jnp.int32, size, 0)
        lane = lax.broadcasted_iota(jnp.int32, size, 1)
        pick_i = jnp.where(lane == y * w + c * (w // 2) + row // w, 1.0, 0.0).astype(BF16)
        whole = pairs_buf[...]
        high = jnp.floor(whole * (1.0 / 128.0))
        both = dot(pick_i, high.astype(BF16)) * 128.0 + dot(pick_i, (whole - high * 128.0).astype(BF16))
        one = jnp.sum(jnp.where(lane == x * w + row % w, both, 0.0), axis=1, keepdims=True)
        count_buf[...] = jnp.broadcast_to(1e-3 + one, size)
        opm_f32[...] = ow_ref[...].astype(F32)
        for f in range(e):
            rows_f = opm_f32[pl.ds(f, e, stride=e), :].astype(BF16)
            for i in range(128 // e):
                opmw_buf[(f * (128 // e) + i) * e:(f * (128 // e) + i + 1) * e, :] = rows_f

    proj = att_buf
    count = []

    def project():
        count.append(jnp.sum(mask_ref[...].astype(F32), axis=0, keepdims=True) + 1e-10)
        col_project(ln_buf, ckv_ref, logit_buf, val_buf)

    qsum = all_reduce(1, combine_sum, sc1, rc1, sc2, rc2, project, lambda: col_gates(ln_buf, cg_ref, proj))
    small[...] = dot(cq_ref[...], (qsum / count[0]).astype(BF16)).astype(BF16).astype(F32)
    query = [small[pl.ds(d, mh, stride=md), :] for d in range(md)]
    sums, top, den = col_sums(query, smask, logit_buf, val_buf)
    for d in range(md):
        part[0, pl.ds(d, mh, stride=md), :] = sums[d]
        part[1, pl.ds(d, mh, stride=md), :] = top
        part[2, pl.ds(d, mh, stride=md), :] = den
    attended = all_reduce(3, combine_softmax, sd1, rd1, sd2, rd2, count_pairs, lambda: None)
    col_finish(attended, new_buf, smask, wt_col, op_ref, last_buf, proj)
    store = pltpu.make_async_copy(last_buf, m_out, load_sem.at[len(loads)])
    store.start()

    planes = proj.reshape(seq * 2 * e, res)

    eye = jnp.where(lax.broadcasted_iota(jnp.int32, (res, res), 0) == lax.broadcasted_iota(jnp.int32, (res, res), 1), 1.0, 0.0).astype(BF16)

    def turned(t):
        return dot_nt(eye, planes[pl.ds(t, seq, stride=2 * e), :].astype(BF16))

    def turn_a(t, _):
        for u in range(4):
            a_f32[pl.ds(4 * t + u, res, stride=e), :] = turned(4 * t + u)
        return 0

    def turn_c(t, _):
        for u in range(4):
            f = 4 * t + u
            other = turned(e + f).astype(BF16)
            for b in range(side):
                c_send[b, pl.ds(pl.multiple_of(f * w, w), w), :] = other[b * w:(b + 1) * w]
        return 0
    def gather_bias(turned):
        for h in range(heads):
            plane = flat[pl.ds(h, res, stride=heads), :]
            bias[h] = plane.T if turned else plane

    places = {0: (0, 0), 1: (0, 1), side - 1: (1, 0), 2: (1, 1)}

    def slot(buf, k, l, rows=None):
        pair_id, part_id = places[l]
        return buf.at[k, pair_id, pl.ds(0, blk) if rows is None else rows, pl.ds(part_id * seq, seq)]

    order = [0, 1, side - 1, 2]
    assert side == len(order)
    xn, yn = [lax.rem(x + 1, side), lax.rem(x + side - 1, side)], [lax.rem(y + 1, side), lax.rem(y + side - 1, side)]
    back_by = [1, side - 1]
    halves = [pl.ds(0, blk // 2), pl.ds(blk // 2, blk // 2)]
    first, hop, passed = [{}, {}], {}, {}

    def send_first(which):
        for k in order[1:]:
            ty, tx = lax.rem(y + k, side), lax.rem(x + k, side)
            if which == 0:
                cp = remote(a_send.at[ty], slot(a_buf, k, 0), s1.at[0, k], r1.at[0, k], dev(ty, x, c))
            else:
                cp = remote(c_send.at[tx], slot(c_buf, 0, k), s1.at[1, k], r1.at[1, k], dev(y, tx, c))
            cp.start()
            first[which][k] = cp

    def spread(which, k):
        for d in range(2):
            if which == 0:
                cp = remote(a_send.at[y] if k == 0 else slot(a_buf, k, 0), slot(a_buf, k, back_by[d]), s2.at[0, k, d], r2.at[0, k, d], dev(y, xn[d], c))
            else:
                cp = remote(c_send.at[x] if k == 0 else slot(c_buf, 0, k), slot(c_buf, back_by[d], k), s2.at[1, k, d], r2.at[1, k, d], dev(yn[d], x, c))
            cp.start()
            hop[which, k, d] = cp

    def relay(k):
        for d in range(2):
            hop[0, k, d].wait_recv()
            f = remote(slot(a_buf, k, back_by[d], halves[d]), slot(a_buf, k, 2, halves[d]), s3.at[0, k, d], r3.at[0, k, d], dev(y, xn[d], c))
            f.start()
            hop[1, k, d].wait_recv()
            g = remote(slot(c_buf, back_by[d], k, halves[d]), slot(c_buf, 2, k, halves[d]), s3.at[1, k, d], r3.at[1, k, d], dev(yn[d], x, c))
            g.start()
            passed[k, d] = (f, g)

    def wait_passed(k):
        for d in range(2):
            for f in passed[k, d]:
                f.wait_recv()

    cols = blk // 2

    def product(chunk, dst_id, fresh=False):
        k, p = chunk
        base = jnp.where(dst_id == 0, 1 - c, c) * cols
        part_sum = dot_nt(c_buf[k, p], a_buf[k, p, pl.ds(pl.multiple_of(base, cols), cols), :])
        if fresh:
            acc[dst_id] = part_sum
        else:
            acc[dst_id] += part_sum

    def products(chunk, fresh=False):
        product(chunk, 0, fresh)
        product(chunk, 1, fresh)

    lax.fori_loop(0, e // 4, turn_a, 0, unroll=2)
    for b in range(side):
        a_send[b] = a_f32[b * blk:(b + 1) * blk].astype(BF16)
    send_first(0)
    spread(0, 0)
    lax.fori_loop(0, e // 4, turn_c, 0, unroll=2)
    send_first(1)
    spread(1, 0)
    a_buf[0, 0, :, :seq] = a_send[y]
    c_buf[0, 0, :, :seq] = c_send[x]
    rows_to_block_wait(me, side, z_ref, zblk, sb, rb)
    one, three, two = order[1:]
    first[0][one].wait_recv()
    first[1][one].wait_recv()
    spread(0, one)
    spread(1, one)
    relay(0)
    first[0][three].wait_recv()
    first[1][three].wait_recv()
    spread(0, three)
    spread(1, three)
    relay(one)
    products((0, 0), True)
    first[0][two].wait_recv()
    first[1][two].wait_recv()
    spread(0, two)
    spread(1, two)
    products((one, 0))
    relay(three)
    products((three, 0))
    wait_passed(0)
    products((0, 1))
    relay(two)
    wait_passed(one)
    products((two, 0))
    products((one, 1))
    wait_passed(three)
    products((three, 1))
    wait_passed(two)
    product((two, 1), 0)
    swap = remote(acc.at[0], got, s4, r4, dev(y, x, 1 - c))
    swap.start()
    product((two, 1), 1)
    for k in order[1:]:
        first[0][k].wait_send()
        first[1][k].wait_send()
    for cp in hop.values():
        cp.wait_send()
    for pair in passed.values():
        for f in pair:
            f.wait_send()
    swap.wait()

    per = 128 // e
    lane_i = lax.broadcasted_iota(jnp.int32, (w, 128), 1) // e
    keep = [(lane_i == i).astype(F32) for i in range(per)]

    def place(f, _):
        for g in range(cols // 128):
            rows = pl.ds(pl.multiple_of(f * w, w), w)
            both = acc[1, rows, g * 128:(g + 1) * 128] + got[rows, g * 128:(g + 1) * 128]
            for i in range(per):
                r0 = (g * per + i) * w
                terms[r0:r0 + w, pl.ds(pl.multiple_of(f * 128, 128), 128)] = (both * keep[i]).astype(BF16)
        return 0
    lax.fori_loop(0, blk // w, place, 0)
    update = dot(terms[...], opmw_buf[...]) / count_buf[...]
    fresh = (zblk[...].reshape(side * r * w, pc).astype(F32) + update).astype(BF16)
    zsend[...] = fresh.reshape(side, r, w, pc)

    nh = r * heads
    groups = (w // 2) * w // 128
    part_bias = dot_nt(sb_ref[...], norm_rows(fresh.astype(F32)))[:heads]
    msg[0, 0, :nh] = jnp.concatenate([part_bias[:, g * 128:(g + 1) * 128] for g in range(groups)], axis=0).astype(BF16)
    gathers = exchange_all(inbox.at[0, :, :nh], lambda p: msg.at[0, 0, :nh], s6, r6)
    my_core = x // half
    for t in range(side):
        dst = y * 2 * side + (c * half + t // 2) * 2 + t % 2

        @pl.when(dst != me)
        def _():
            remote(zsend.at[t], zrows.at[x], s5.at[t], r5.at[x], dst).start()

        @pl.when(dst == me)
        def _():
            zrows[x] = zsend[t]
    for t in range(side):
        dst = y * 2 * side + (c * half + t // 2) * 2 + t % 2
        src = y * 2 * side + t * 2 + my_core

        @pl.when(dst != me)
        def _():
            remote(zsend.at[t], zrows.at[x], s5.at[t], r5.at[x], dst).wait_send()

        @pl.when(src != me)
        def _():
            remote(zsend.at[t], zrows.at[t], s5.at[t], r5.at[t], dst).wait_recv()
    for t in range(side):
        z_f[:, t * w:(t + 1) * w, :] = zrows[t].astype(F32)

    for cp in gathers:
        cp.wait()
    flat[...] = inbox[0, :, :nh].astype(F32).reshape(n * nh, res)
    per_y = 2 * groups
    for yy in range(side):
        for h in range(heads):
            pieces = [flat[pl.ds((yy * side + xx) * per_y * heads + h, per_y, stride=heads), :] for xx in range(side)]
            for i in range(128 // w):
                bias[h, pl.ds(yy * w + i, per_y, stride=128 // w), :] = jnp.concatenate([piece[:, i * w:(i + 1) * w] for piece in pieces], axis=1)
    maskb = (resm_ref[...].astype(F32) - 1.0) * 1e4
    triangle(z_f, bias, maskb, sq_ref, so_ref, heads)

    rr = r * r

    def pack(slot_id):
        for p in range(n):
            msg[slot_id, p, :rr] = jnp.concatenate([z_f[i, p * r:(p + 1) * r, :] for i in range(r)], axis=0).astype(BF16)

    def unpack(slot_id):
        flat[...] = inbox[slot_id, :, :rr].astype(F32).reshape(n * rr, pc)
        for i in range(r):
            z_f[i] = flat[pl.ds(i, res, stride=r), :]

    pack(1)
    rows_b = bias_rows(z_f, eb_ref, heads)
    for p in range(n):
        msg[1, p, rr:] = rows_b
    for cp in exchange_all(inbox.at[1], lambda p: msg.at[1, p], s7, r7):
        cp.wait()
    flat[...] = inbox[1, :, rr:].astype(F32).reshape(n * nh, res)
    gather_bias(True)
    unpack(1)
    triangle(z_f, bias, maskb, eq_ref, eo_ref, heads)
    pack(2)
    for cp in exchange_all(inbox.at[2, :, :rr], lambda p: msg.at[2, p, :rr], s8, r8):
        cp.wait()
    unpack(2)
    z_out[...] = z_f[...].astype(BF16)
    store.wait()


def block_call(n, side, dims, ops):
    m, z = ops[0], ops[1]
    seq, ch, res = m.shape
    r, _, w, pc = z.shape
    mh, md, heads = dims
    width, e = mh * md, ops[11].shape[0] // 2
    blk = w * e
    vm, dma = pltpu.VMEM, pltpu.SemaphoreType.DMA
    assert r == heads and mh == md and res == 128 and seq == 128 and pc == 128
    own = res // n
    buf = vm((side, half_of(side), blk, 2 * seq), BF16)
    tall = vm((seq, width, res), BF16)
    box = vm((3, n, 2 * r * r, pc), BF16)
    scratch = [vm(op.shape, op.dtype) for op in ops] + [dma((len(ops) + 1,))]
    scratch += [vm((seq, res), F32), tall, vm((seq, res, width + 16), BF16), tall, tall, vm((seq, width, res), F32),
               vm((2, mh // 2, res, 2 * res), F32), vm((2, mh // 2, res, 2 * res), BF16), vm((2, mh // 2, 8, 2 * res), F32),
               vm((mh // 2, res, 2 * res), F32), vm((mh // 2, width, 2 * res), BF16), vm((n + 1, r * mh, res), BF16), vm((n * r * mh, res), F32),
               vm((ch, width), BF16), vm((ch, width), BF16),
               vm((3, width, res), F32), vm((n, 3, own, width), F32), vm((n, 3, own, width), F32), vm((2, own, width), F32), vm((2, n, own, width), F32),
               vm((width, res), F32), vm((seq, mh, res), F32), vm((seq, md, res), F32), vm((res * e, seq), F32),
               vm((side, blk, seq), BF16), vm((side, blk, seq), BF16), vm((side, r, w, pc), BF16), vm((e * e, pc), F32), vm((e * 128, pc), BF16),
               vm((w // 2 * w, pc), F32), vm((res, res), F32),
               buf, buf, vm((2, blk, blk // 2), F32), vm((blk, blk // 2), F32), vm((w // 2 * w, e * 128), BF16),
               vm((side, r, w, pc), BF16), vm((side, r, w, pc), BF16), vm((r, res, pc), F32),
               vm((heads, res, res), F32), box, box, vm((n * r * r, pc), F32),
               dma((n,)), dma((n,)), dma((side,)), dma((side,))] + [dma((n,))] * 8 + [
               dma((2, side)), dma((2, side)), dma((2, side, 2)), dma((2, side, 2)), dma((2, side, 2)), dma((2, side, 2)),
               dma, dma, dma((side,)), dma((side,))] + [dma((n,))] * 6
    return pl.pallas_call(
        functools.partial(block_kernel, n, side, dims, len(ops)),
        out_shape=[jax.ShapeDtypeStruct((seq, ch, res), BF16), jax.ShapeDtypeStruct((r, res, pc), BF16)],
        in_specs=[pl.BlockSpec(memory_space=pl.ANY)] * len(ops),
        out_specs=[pl.BlockSpec(memory_space=pl.ANY), vmem()], scratch_shapes=scratch,
        compiler_params=pltpu.CompilerParams(collective_id=0, has_side_effects=True, vmem_limit_bytes=63 * 1024 * 1024),
        name='evoformer_block')(*ops)


def half_of(side):
    return side // 2


def solution(mesh):
    n = mesh.shape['dap']
    side = math.isqrt(n // 2)
    assert 2 * side * side == n

    def block(msa, pair, mask_full, res_mask, row_bias_w, row_qkvg_w, row_out_w, col_query_w, col_kv_w, col_gate_w, col_out_w, opm_proj_w, opm_out_w, start_bias_w, start_qkvg_w, start_out_w, end_bias_w, end_qkvg_w, end_out_w):
        r, res, pc = pair.shape
        ch = msa.shape[-1]
        last = lambda weight: jnp.moveaxis(weight, 0, -1).reshape(-1, weight.shape[0])
        first = lambda weight: weight.reshape(-1, weight.shape[-1])
        ops = [msa.transpose(0, 2, 1), pair.reshape(r, side, res // side, pc), mask_full, res_mask[None],
               row_bias_w.T, last(row_qkvg_w), first(row_out_w), last(col_query_w), last(col_kv_w), last(col_gate_w), first(col_out_w),
               last(opm_proj_w), first(opm_out_w), start_bias_w.T, last(start_qkvg_w), first(start_out_w), end_bias_w.T, last(end_qkvg_w), first(end_out_w)]
        msa_out, pair_out = block_call(n, side, col_gate_w.shape[1:] + (start_bias_w.shape[-1],), ops)
        return msa_out.transpose(0, 2, 1), pair_out

    row_spec = P(('data', 'dap'), None, None)
    in_specs = (row_spec, row_spec, P('data', None), P('data')) + (P(),) * 15
    return jax.shard_map(block, mesh=mesh, in_specs=in_specs, out_specs=(row_spec, row_spec), check_vma=False)
```
